32 devices in a mesh: dp: 4 (over y, z), tp: 8 (over x, core).
Axes of the slice: x: 4, y: 2, z: 2, core: 2. Of those that a mesh axis runs over, the one named last changes fastest.
The devices are a block of a 4x4x8 slice.
Arguments:
- x_seq: bfloat16 [3, 512, 4096], P(None, 'dp'), parts along dimension 1
- cache_len: int32 [512], P('dp'), parts along dimension 0
- k_cache: bfloat16 [512, 8, 256, 128], P('dp', 'tp'), parts along dimension 0
- v_cache: bfloat16 [512, 8, 256, 128], P('dp', 'tp'), parts along dimension 0
- w_q: bfloat16 [4096, 4096], P(None, 'tp')
- w_k: bfloat16 [4096, 1024], P(None, 'tp')
- w_v: bfloat16 [4096, 1024], P(None, 'tp')
- w_o: bfloat16 [4096, 4096], P('tp')
- w_gate: bfloat16 [4096, 14336], P(None, 'tp')
- w_up: bfloat16 [4096, 14336], P(None, 'tp')
- w_down: bfloat16 [14336, 4096], P('tp')
- g_q: bfloat16 [4096], P('tp')
- g_k: bfloat16 [1024], P('tp')
- g_attn: bfloat16 [4096], replicated
- g_mlp: bfloat16 [4096], replicated
Outputs:
- output 1: bfloat16 [3, 512, 4096], P(None, 'dp'), parts along dimension 1
- output 2: bfloat16 [512, 8, 256, 128], P('dp', 'tp'), parts along dimension 0
- output 3: bfloat16 [512, 8, 256, 128], P('dp', 'tp'), parts along dimension 0
There are 4 independent parts. The reference program is written for one: setup_inputs(seed, part) draws one part's arguments, and reference() takes and returns one part's arrays. A program takes and returns all parts, laid end to end along the dimension named above; an argument that names none is the same for every part.
All inputs are finite; a program needn't handle non-finite values.
Results may differ from the reference program's by a relative error of at most 0.02.
Values are sent between devices in bfloat16 or wider.
A program may use at most 768 MiB of HBM per device.

```python
import math
import jax
import jax.numpy as jnp
from jax import lax

STEPS = 3
MIN_LEN = 128
D_MODEL = 4096
N_HEADS = 32
N_KV_HEADS = 8
HEAD_DIM = 128
FF_DIM = 14336
BATCH_ROWS = 128
MAX_SEQ = 256
ROPE_THETA = 500000.0
NORM_EPS = 1e-6


def draw_lengths(len_key):
    sub_keys = jax.random.split(len_key, 3)
    lengths = jax.random.randint(sub_keys[0], (BATCH_ROWS,), MIN_LEN, MAX_SEQ - STEPS + 1)
    long_row = jax.random.randint(sub_keys[1], (), 0, BATCH_ROWS)
    short_row = (long_row + 1 + jax.random.randint(sub_keys[2], (), 0, BATCH_ROWS - 1)) % BATCH_ROWS
    lengths = lengths.at[long_row].set(MAX_SEQ - STEPS).at[short_row].set(MIN_LEN)
    return lengths.astype(jnp.int32)


def normal_weight(w_key, rows_in, cols_out):
    return jax.random.normal(w_key, (rows_in, cols_out), jnp.float32) * rows_in ** -0.5


def head_scales(scale_key, n_heads):
    log_scale = jax.random.uniform(scale_key, (n_heads,), jnp.float32, math.log(0.3), math.log(3.0))
    return jnp.repeat(jnp.exp(log_scale), HEAD_DIM)


def setup_inputs(seed: int = 0, part: int = 0) -> dict:
    base_key = jax.random.key(seed)
    part_keys = jax.random.split(jax.random.fold_in(base_key, part), 4)
    w_keys = jax.random.split(jax.random.key(seed + 1), 13)
    q_width = N_HEADS * HEAD_DIM
    kv_width = N_KV_HEADS * HEAD_DIM
    cache_shape = (BATCH_ROWS, N_KV_HEADS, MAX_SEQ, HEAD_DIM)
    x_seq = jax.random.normal(part_keys[0], (STEPS, BATCH_ROWS, D_MODEL), jnp.float32)
    k_cache = jax.random.normal(part_keys[2], cache_shape, jnp.float32)
    v_cache = jax.random.normal(part_keys[3], cache_shape, jnp.float32)
    w_q = normal_weight(w_keys[0], D_MODEL, q_width) * head_scales(w_keys[1], N_HEADS)[None, :]
    w_k = normal_weight(w_keys[2], D_MODEL, kv_width) * head_scales(w_keys[3], N_KV_HEADS)[None, :]
    w_v = normal_weight(w_keys[4], D_MODEL, kv_width)
    w_o = normal_weight(w_keys[5], q_width, D_MODEL)
    w_gate = normal_weight(w_keys[6], D_MODEL, FF_DIM)
    w_up = normal_weight(w_keys[7], D_MODEL, FF_DIM)
    w_down = normal_weight(w_keys[8], FF_DIM, D_MODEL)
    g_q = jax.random.uniform(w_keys[9], (q_width,), jnp.float32, 0.5, 1.5)
    g_k = jax.random.uniform(w_keys[10], (kv_width,), jnp.float32, 0.5, 1.5)
    g_attn = jax.random.uniform(w_keys[11], (D_MODEL,), jnp.float32, 0.5, 1.5)
    g_mlp = jax.random.uniform(w_keys[12], (D_MODEL,), jnp.float32, 0.5, 1.5)
    return {'x_seq': x_seq.astype(jnp.bfloat16), 'cache_len': draw_lengths(part_keys[1]), 'k_cache': k_cache.astype(jnp.bfloat16), 'v_cache': v_cache.astype(jnp.bfloat16), 'w_q': w_q.astype(jnp.bfloat16), 'w_k': w_k.astype(jnp.bfloat16), 'w_v': w_v.astype(jnp.bfloat16), 'w_o': w_o.astype(jnp.bfloat16), 'w_gate': w_gate.astype(jnp.bfloat16), 'w_up': w_up.astype(jnp.bfloat16), 'w_down': w_down.astype(jnp.bfloat16), 'g_q': g_q.astype(jnp.bfloat16), 'g_k': g_k.astype(jnp.bfloat16), 'g_attn': g_attn.astype(jnp.bfloat16), 'g_mlp': g_mlp.astype(jnp.bfloat16)}


def rms_factor(sq_sum, full_width):
    return lax.rsqrt(sq_sum / full_width + NORM_EPS)


def rope_tables(positions):
    half_dim = HEAD_DIM // 2
    inv_freq = ROPE_THETA ** (-(jnp.arange(half_dim, dtype=jnp.float32) * (2.0 / HEAD_DIM)))
    angles = positions.astype(jnp.float32)[:, None] * inv_freq[None, :]
    return jnp.cos(angles), jnp.sin(angles)


def apply_rope(head_vals, cos_tab, sin_tab):
    half_dim = HEAD_DIM // 2
    lead_half = head_vals[..., :half_dim]
    tail_half = head_vals[..., half_dim:]
    cos_rows = cos_tab[:, None, :]
    sin_rows = sin_tab[:, None, :]
    return jnp.concatenate([lead_half * cos_rows - tail_half * sin_rows, tail_half * cos_rows + lead_half * sin_rows], axis=-1)


def reference(x_seq, cache_len, k_cache, v_cache, w_q, w_k, w_v, w_o, w_gate, w_up, w_down, g_q, g_k, g_attn, g_mlp):
    q_width = N_HEADS * HEAD_DIM
    kv_width = N_KV_HEADS * HEAD_DIM
    group_size = N_HEADS // N_KV_HEADS
    row_ids = jnp.arange(BATCH_ROWS)
    seq_ids = jnp.arange(MAX_SEQ)
    gain_q = g_q.astype(jnp.float32)
    gain_k = g_k.astype(jnp.float32)
    gain_a = g_attn.astype(jnp.float32)
    gain_m = g_mlp.astype(jnp.float32)

    def attend_row(row_in):
        q_row, k_row, v_row, last_pos = row_in
        q_grp = q_row.reshape(N_KV_HEADS, group_size, HEAD_DIM).astype(jnp.float32)
        scores = jnp.einsum('kgd,ksd->kgs', q_grp, k_row.astype(jnp.float32)) * HEAD_DIM ** -0.5
        scores = jnp.where(seq_ids <= last_pos, scores, -jnp.inf)
        row_max = jnp.max(scores, axis=-1, keepdims=True)
        exp_scores = jnp.exp(scores - row_max)
        row_sum = jnp.sum(exp_scores, axis=-1, keepdims=True)
        mixed_vals = jnp.einsum('kgs,ksd->kgd', exp_scores.astype(jnp.bfloat16).astype(jnp.float32), v_row.astype(jnp.float32))
        return (mixed_vals / row_sum).astype(jnp.bfloat16).reshape(q_width)

    def one_step(cache_pair, step_in):
        k_all, v_all = cache_pair
        x_tok, step_idx = step_in
        positions = cache_len + step_idx
        q_raw = jnp.dot(x_tok, w_q, preferred_element_type=jnp.float32).astype(jnp.bfloat16).astype(jnp.float32)
        k_raw = jnp.dot(x_tok, w_k, preferred_element_type=jnp.float32).astype(jnp.bfloat16).astype(jnp.float32)
        v_new = jnp.dot(x_tok, w_v, preferred_element_type=jnp.float32).astype(jnp.bfloat16).reshape(BATCH_ROWS, N_KV_HEADS, HEAD_DIM)
        q_normed = q_raw * rms_factor(jnp.sum(q_raw * q_raw, axis=-1, keepdims=True), q_width) * gain_q
        k_normed = k_raw * rms_factor(jnp.sum(k_raw * k_raw, axis=-1, keepdims=True), kv_width) * gain_k
        cos_tab, sin_tab = rope_tables(positions)
        q_rot = apply_rope(q_normed.reshape(BATCH_ROWS, N_HEADS, HEAD_DIM), cos_tab, sin_tab).astype(jnp.bfloat16)
        k_rot = apply_rope(k_normed.reshape(BATCH_ROWS, N_KV_HEADS, HEAD_DIM), cos_tab, sin_tab).astype(jnp.bfloat16)
        k_all = k_all.at[row_ids, :, positions, :].set(k_rot)
        v_all = v_all.at[row_ids, :, positions, :].set(v_new)
        attn_vals = lax.map(attend_row, (q_rot, k_all, v_all, positions))
        attn_sum = jnp.dot(attn_vals, w_o, preferred_element_type=jnp.float32).astype(jnp.bfloat16).astype(jnp.float32)
        hidden = (x_tok.astype(jnp.float32) + attn_sum * rms_factor(jnp.sum(attn_sum * attn_sum, axis=-1, keepdims=True), D_MODEL) * gain_a).astype(jnp.bfloat16)
        gate_pre = jnp.dot(hidden, w_gate, preferred_element_type=jnp.float32)
        up_pre = jnp.dot(hidden, w_up, preferred_element_type=jnp.float32)
        act_vals = (jax.nn.silu(gate_pre) * up_pre).astype(jnp.bfloat16)
        mlp_sum = jnp.dot(act_vals, w_down, preferred_element_type=jnp.float32).astype(jnp.bfloat16).astype(jnp.float32)
        y_tok = (hidden.astype(jnp.float32) + mlp_sum * rms_factor(jnp.sum(mlp_sum * mlp_sum, axis=-1, keepdims=True), D_MODEL) * gain_m).astype(jnp.bfloat16)
        return (k_all, v_all), y_tok

    (k_final, v_final), y_seq = lax.scan(one_step, (k_cache, v_cache), (x_seq, jnp.arange(STEPS, dtype=jnp.int32)))
    return (y_seq, k_final, v_final)
```

```python
import jax
import jax.numpy as jnp
from jax import lax
from jax.sharding import PartitionSpec as P

ROPE_THETA = 500000.0
NORM_EPS = 1e-6


def rms_factor(sq_sum, full_width):
    return lax.rsqrt(sq_sum / full_width + NORM_EPS)


def rope_tables(positions, head_dim):
    half_dim = head_dim // 2
    inv_freq = ROPE_THETA ** (-(jnp.arange(half_dim, dtype=jnp.float32) * (2.0 / head_dim)))
    angles = positions.astype(jnp.float32)[:, None] * inv_freq[None, :]
    return jnp.cos(angles), jnp.sin(angles)


def apply_rope(head_vals, cos_tab, sin_tab):
    half_dim = head_vals.shape[-1] // 2
    lead_half = head_vals[..., :half_dim]
    tail_half = head_vals[..., half_dim:]
    cos_rows = cos_tab[:, None, :]
    sin_rows = sin_tab[:, None, :]
    return jnp.concatenate([lead_half * cos_rows - tail_half * sin_rows, tail_half * cos_rows + lead_half * sin_rows], axis=-1)


def group_psum(part_val):
    return lax.psum(part_val, 'tp')


def layer_steps(x_seq, cache_len, k_cache, v_cache, w_q, w_k, w_v, w_o, w_gate, w_up, w_down, g_q, g_k, g_attn, g_mlp, q_width, kv_width, group_sum):
    num_steps, n_rows, d_model = x_seq.shape
    kv_loc = k_cache.shape[1]
    head_dim = k_cache.shape[-1]
    seq_max = k_cache.shape[2]
    q_loc = w_q.shape[1] // head_dim
    group_size = q_loc // kv_loc
    gain_q = g_q.astype(jnp.float32)
    gain_k = g_k.astype(jnp.float32)
    gain_a = g_attn.astype(jnp.float32)
    gain_m = g_mlp.astype(jnp.float32)
    x_all = x_seq.reshape(num_steps * n_rows, d_model)
    positions = (cache_len[None, :] + jnp.arange(num_steps, dtype=cache_len.dtype)[:, None]).reshape(-1)
    q_raw = jnp.dot(x_all, w_q, preferred_element_type=jnp.float32).astype(jnp.bfloat16).astype(jnp.float32)
    k_raw = jnp.dot(x_all, w_k, preferred_element_type=jnp.float32).astype(jnp.bfloat16).astype(jnp.float32)
    v_new = jnp.dot(x_all, w_v, preferred_element_type=jnp.float32).astype(jnp.bfloat16)
    sums = group_sum(jnp.concatenate([jnp.sum(q_raw * q_raw, axis=-1, keepdims=True), jnp.sum(k_raw * k_raw, axis=-1, keepdims=True)], axis=1))
    cos_tab, sin_tab = rope_tables(positions, head_dim)
    q_normed = (q_raw * rms_factor(sums[:, :1], q_width) * gain_q).reshape(-1, q_loc, head_dim)
    k_normed = (k_raw * rms_factor(sums[:, 1:], kv_width) * gain_k).reshape(-1, kv_loc, head_dim)
    q_rot = apply_rope(q_normed, cos_tab, sin_tab).astype(jnp.bfloat16)
    k_rot = apply_rope(k_normed, cos_tab, sin_tab).astype(jnp.bfloat16)
    q_rot = q_rot.reshape(num_steps, n_rows, kv_loc, group_size, head_dim).transpose(1, 2, 0, 3, 4).reshape(n_rows, kv_loc, num_steps * group_size, head_dim)
    new_k = k_rot.reshape(num_steps, n_rows, kv_loc, head_dim)
    new_v = v_new.reshape(num_steps, n_rows, kv_loc, head_dim)
    offsets = jnp.arange(seq_max, dtype=jnp.int32)[None, None, :, None] - cache_len[:, None, None, None]
    k_out = k_cache
    v_out = v_cache
    for step_idx in range(num_steps):
        k_out = jnp.where(offsets == step_idx, new_k[step_idx][:, :, None, :], k_out)
        v_out = jnp.where(offsets == step_idx, new_v[step_idx][:, :, None, :], v_out)
    scores = jnp.einsum('bkqd,bksd->bkqs', q_rot, k_out, preferred_element_type=jnp.float32) * head_dim ** -0.5
    last = cache_len[:, None] + jnp.repeat(jnp.arange(num_steps, dtype=jnp.int32), group_size)[None, :]
    valid = jnp.arange(seq_max, dtype=jnp.int32)[None, None, :] <= last[:, :, None]
    scores = jnp.where(valid[:, None], scores, -jnp.inf)
    exps = jnp.exp(scores - jnp.max(scores, axis=-1, keepdims=True))
    mixed = jnp.einsum('bkqs,bksd->bkqd', exps.astype(jnp.bfloat16), v_out, preferred_element_type=jnp.float32)
    attn = (mixed / jnp.sum(exps, axis=-1, keepdims=True)).astype(jnp.bfloat16)
    attn = attn.reshape(n_rows, kv_loc, num_steps, group_size, head_dim).transpose(2, 0, 1, 3, 4).reshape(num_steps * n_rows, q_loc * head_dim)
    attn_sum = group_sum(jnp.dot(attn, w_o, preferred_element_type=jnp.float32).astype(jnp.bfloat16)).astype(jnp.float32)
    hidden = (x_all.astype(jnp.float32) + attn_sum * rms_factor(jnp.sum(attn_sum * attn_sum, axis=-1, keepdims=True), d_model) * gain_a).astype(jnp.bfloat16)
    gate_pre = jnp.dot(hidden, w_gate, preferred_element_type=jnp.float32)
    up_pre = jnp.dot(hidden, w_up, preferred_element_type=jnp.float32)
    act = (jax.nn.silu(gate_pre) * up_pre).astype(jnp.bfloat16)
    mlp_sum = group_sum(jnp.dot(act, w_down, preferred_element_type=jnp.float32).astype(jnp.bfloat16)).astype(jnp.float32)
    y = (hidden.astype(jnp.float32) + mlp_sum * rms_factor(jnp.sum(mlp_sum * mlp_sum, axis=-1, keepdims=True), d_model) * gain_m).astype(jnp.bfloat16)
    return y.reshape(num_steps, n_rows, d_model), k_out, v_out


def solution(mesh):
    tp_size = mesh.shape['tp']

    def local_run(x_seq, cache_len, k_cache, v_cache, w_q, w_k, w_v, w_o, w_gate, w_up, w_down, g_q, g_k, g_attn, g_mlp):
        return layer_steps(x_seq, cache_len, k_cache, v_cache, w_q, w_k, w_v, w_o, w_gate, w_up, w_down, g_q, g_k, g_attn, g_mlp, w_q.shape[1] * tp_size, w_k.shape[1] * tp_size, group_psum)

    data_spec = P(None, 'dp', None)
    cache_spec = P('dp', 'tp', None, None)
    col_spec = P(None, 'tp')
    row_spec = P('tp', None)
    arg_specs = (data_spec, P('dp'), cache_spec, cache_spec, col_spec, col_spec, col_spec, row_spec, col_spec, col_spec, row_spec, P('tp'), P('tp'), P(None), P(None))
    out_specs = (data_spec, cache_spec, cache_spec)
    return jax.shard_map(local_run, mesh=mesh, in_specs=arg_specs, out_specs=out_specs, check_vma=False)
```

```python
import functools

import jax
import jax.numpy as jnp
import numpy as np
from jax import lax
from jax.experimental import pallas as pl
from jax.experimental.pallas import tpu as pltpu
from jax.sharding import PartitionSpec as P

ROPE_THETA = 500000.0
NORM_EPS = 1e-6
F32 = jnp.float32
BF16 = jnp.bfloat16
MESH = pl.DeviceIdType.MESH
VMEM_SPEC = pl.BlockSpec(memory_space=pltpu.VMEM)
ANY_SPEC = pl.BlockSpec(memory_space=pl.ANY)
SMEM_SPEC = pl.BlockSpec(memory_space=pltpu.SMEM)
VMEM_LIMIT = 67043328
SLOT_ROWS = 16


def matmul(lhs, rhs):
    return jnp.dot(lhs, rhs, preferred_element_type=F32)


def qkv_kernel(tp, q_width, kv_width, x_hbm, len_ref, freq_ref, wq_hbm, wk_hbm, wv_hbm, gq_ref, gk_ref,
               q_out, kn_out, vn_out,
               x_buf, wq_buf, wk_buf, wv_buf, q_raw, q_rows, part, inbox, turn, in_sem, send_sem, recv_sem):
    steps, rows, _ = x_hbm.shape
    hd = wk_hbm.shape[1]
    heads = wq_hbm.shape[1] // hd
    pad = q_out.shape[1]
    me = lax.axis_index("tp")
    x_in = [pltpu.make_async_copy(x_hbm.at[t], x_buf.at[pl.ds(t * rows, rows), :], in_sem.at[t]) for t in range(steps)]
    for copy in x_in:
        copy.start()
    half = heads * hd // 2
    wk_in = pltpu.make_async_copy(wk_hbm, wk_buf, in_sem.at[3])
    wq_in = [pltpu.make_async_copy(wq_hbm.at[:, pl.ds(j * half, half)], wq_buf.at[:, pl.ds(j * half, half)], in_sem.at[4 + j]) for j in range(2)]
    wv_in = pltpu.make_async_copy(wv_hbm, wv_buf, in_sem.at[6])
    for copy in (wk_in, wq_in[0], wq_in[1], wv_in):
        copy.start()

    barrier = pltpu.get_barrier_semaphore()
    for j in range(1, tp):
        pl.semaphore_signal(barrier, inc=1, device_id={"tp": lax.rem(me + j, tp)}, device_id_type=MESH)

    lens = jnp.transpose(jnp.broadcast_to(len_ref[...].astype(F32), (rows, rows)))[:, :hd]
    lane = lax.broadcasted_iota(jnp.int32, (rows, hd), 1)
    sign = jnp.where(lane < hd // 2, -1.0, 1.0).astype(F32)
    tables = []
    for t in range(steps):
        angle = (lens + float(t)) * freq_ref[...]
        tables.append((jnp.cos(angle), jnp.sin(angle) * sign))

    q_rows[...] = jnp.zeros_like(q_rows)
    for copy in x_in:
        copy.wait()
    wk_in.wait()
    k_raw = matmul(x_buf[...], wk_buf[...]).astype(BF16).astype(F32)
    k_sq = jnp.sum(k_raw * k_raw, axis=1, keepdims=True)
    q_sq = None
    for j in range(2):
        wq_in[j].wait()
        val = matmul(x_buf[...], wq_buf[:, j * half:(j + 1) * half]).astype(BF16).astype(F32)
        q_raw[:, j * half:(j + 1) * half] = val
        sq = jnp.sum(val * val, axis=1, keepdims=True)
        q_sq = sq if q_sq is None else q_sq + sq
    packed = jnp.zeros((rows, rows), F32)
    col = lax.broadcasted_iota(jnp.int32, (rows, rows), 1)
    for t in range(steps):
        packed = jnp.where(col == t, q_sq[t * rows:(t + 1) * rows], packed)
        packed = jnp.where(col == steps + t, k_sq[t * rows:(t + 1) * rows], packed)
    part[...] = jnp.transpose(packed)[:part.shape[0]]
    pl.semaphore_wait(barrier, tp - 1)
    copies = []
    for j in range(1, tp):
        copy = pltpu.make_async_remote_copy(
            src_ref=part, dst_ref=inbox.at[j - 1], send_sem=send_sem.at[j - 1], recv_sem=recv_sem.at[j - 1],
            device_id={"tp": lax.rem(me + j, tp)}, device_id_type=MESH)
        copy.start()
        copies.append(copy)
    wv_in.wait()
    vn_out[...] = matmul(x_buf[...], wv_buf[...]).astype(BF16).astype(F32).reshape(steps, rows, hd)
    total = part[...]
    for j in range(1, tp):
        copies[j - 1].wait()
        total = total + inbox[j - 1]
    turn[...] = jnp.zeros_like(turn)
    turn[0:part.shape[0], :] = total
    sums = jnp.transpose(turn[...])
    gain_k = gk_ref[...].astype(F32)
    for t in range(steps):
        cos_tab, sin_tab = tables[t]
        q_fac = lax.rsqrt(sums[:, t:t + 1] / q_width + NORM_EPS)
        k_fac = lax.rsqrt(sums[:, steps + t:steps + t + 1] / kv_width + NORM_EPS)
        val = k_raw[t * rows:(t + 1) * rows] * k_fac * gain_k
        val = val * cos_tab + pltpu.roll(val, hd // 2, axis=1) * sin_tab
        kn_out[t] = val.astype(BF16).astype(F32)
        for g in range(heads):
            val = q_raw[t * rows:(t + 1) * rows, g * hd:(g + 1) * hd] * q_fac * gq_ref[:, g * hd:(g + 1) * hd].astype(F32)
            val = val * cos_tab + pltpu.roll(val, hd // 2, axis=1) * sin_tab
            q_rows[pl.ds(t * heads + g, rows, stride=pad), :] = val
    q_out[...] = q_rows[...].reshape(rows, pad, hd).astype(BF16)


def run_qkv(tp, x_seq, cache_len, w_q, w_k, w_v, g_q, g_k):
    steps, rows, d_model = x_seq.shape
    hd = w_k.shape[1]
    width = w_q.shape[1]
    heads = width // hd
    pad = 16
    inv_freq = (ROPE_THETA ** (-(np.arange(hd // 2, dtype=np.float64) * (2.0 / hd)))).astype(np.float32)
    freq = jnp.asarray(np.concatenate([inv_freq, inv_freq])[None, :])
    return pl.pallas_call(
        functools.partial(qkv_kernel, tp, width * tp, hd * tp),
        out_shape=(jax.ShapeDtypeStruct((rows, pad, hd), BF16),
                   jax.ShapeDtypeStruct((steps, rows, hd), F32),
                   jax.ShapeDtypeStruct((steps, rows, hd), F32)),
        in_specs=[ANY_SPEC, VMEM_SPEC, VMEM_SPEC, ANY_SPEC, ANY_SPEC, ANY_SPEC, VMEM_SPEC, VMEM_SPEC],
        out_specs=(VMEM_SPEC, VMEM_SPEC, VMEM_SPEC),
        scratch_shapes=[
            pltpu.VMEM((steps * rows, d_model), BF16),
            pltpu.VMEM((d_model, width), BF16),
            pltpu.VMEM((d_model, hd), BF16),
            pltpu.VMEM((d_model, hd), BF16),
            pltpu.VMEM((steps * rows, width), F32),
            pltpu.VMEM((rows * pad, hd), F32),
            pltpu.VMEM((8, rows), F32),
            pltpu.VMEM((tp - 1, 8, rows), F32),
            pltpu.VMEM((rows, rows), F32),
            pltpu.SemaphoreType.DMA((7,)),
            pltpu.SemaphoreType.DMA((tp - 1,)),
            pltpu.SemaphoreType.DMA((tp - 1,)),
        ],
        compiler_params=pltpu.CompilerParams(collective_id=0, has_side_effects=True, vmem_limit_bytes=VMEM_LIMIT),
        name="qkv",
    )(x_seq, cache_len.reshape(1, rows), freq, w_q, w_k, w_v, g_q.reshape(1, width), g_k.reshape(1, hd))


SEQ_BLOCK = 8
PATCH_ROWS = 32


def attention_kernel(steps, heads, len_ref, q_ref, kn_ref, vn_ref, k_hbm, v_hbm, o_ref, k_out, v_out,
                     k_buf, v_buf, mixed, in_sem, out_sem):
    rows, seq_max, hd = k_hbm.shape
    pad = q_ref.shape[1]
    blocks = rows // SEQ_BLOCK

    def moves(blk, inward):
        sl = pl.ds(blk * SEQ_BLOCK, SEQ_BLOCK)
        if inward:
            return (pltpu.make_async_copy(k_hbm.at[sl], k_buf.at[sl], in_sem.at[0, blk]),
                    pltpu.make_async_copy(v_hbm.at[sl], v_buf.at[sl], in_sem.at[1, blk]))
        return (pltpu.make_async_copy(k_buf.at[sl], k_out.at[sl], out_sem.at[0, blk]),
                pltpu.make_async_copy(v_buf.at[sl], v_out.at[sl], out_sem.at[1, blk]))

    def start_in(blk, carry):
        for copy in moves(blk, True):
            copy.start()
        return carry

    lax.fori_loop(0, blocks, start_in, 0)
    scale = hd ** -0.5
    win_row = lax.broadcasted_iota(jnp.int32, (PATCH_ROWS, hd), 0)
    key_col = lax.broadcasted_iota(jnp.int32, (pad, seq_max), 1)
    step_row = lax.broadcasted_iota(jnp.int32, (pad, seq_max), 0) // heads
    key_off = key_col - step_row

    def body(blk, carry):
        for copy in moves(blk, True):
            copy.wait()
        lens = []
        for i in range(SEQ_BLOCK):
            b = blk * SEQ_BLOCK + i
            length = len_ref[b]
            base = pl.multiple_of(jnp.minimum((length // 16) * 16, seq_max - PATCH_ROWS), 16)
            for buf, new_ref in ((k_buf, kn_ref), (v_buf, vn_ref)):
                win = buf[b, pl.ds(base, PATCH_ROWS), :].astype(F32)
                for t in range(steps):
                    win = jnp.where(win_row == length + t - base, new_ref[t, pl.ds(b, 1), :], win)
                buf[b, pl.ds(base, PATCH_ROWS), :] = win.astype(BF16)
            lens.append(length)
        scores = []
        for i in range(SEQ_BLOCK):
            b = blk * SEQ_BLOCK + i
            s = lax.dot_general(q_ref[b], k_buf[b], (((1,), (1,)), ((), ())), preferred_element_type=F32) * scale
            scores.append(jnp.where(key_off <= lens[i], s, -jnp.inf))
        exps = []
        for i in range(SEQ_BLOCK):
            e = jnp.exp(scores[i] - jnp.max(scores[i], axis=1, keepdims=True))
            exps.append((e.astype(BF16), jnp.sum(e, axis=1, keepdims=True)))
        for i in range(SEQ_BLOCK):
            b = blk * SEQ_BLOCK + i
            out = matmul(exps[i][0], v_buf[b]) / exps[i][1]
            mixed[pl.ds(pl.multiple_of(b * pad, pad), pad), :] = out
        for copy in moves(blk, False):
            copy.start()
        return carry

    lax.fori_loop(0, blocks, body, 0)
    for t in range(steps):
        for g in range(heads):
            o_ref[t, :, g * hd:(g + 1) * hd] = mixed[pl.ds(t * heads + g, rows, stride=pad), :].astype(BF16)

    def finish(blk, carry):
        for copy in moves(blk, False):
            copy.wait()
        return carry

    lax.fori_loop(0, blocks, finish, 0)


def run_attention(heads, cache_len, q_rows, k_new, v_new, k_cache, v_cache):
    rows, _, seq_max, hd = k_cache.shape
    steps = k_new.shape[0]
    pad = q_rows.shape[1]
    flat = jax.ShapeDtypeStruct((rows, seq_max, hd), BF16)
    out, k_out, v_out = pl.pallas_call(
        functools.partial(attention_kernel, steps, heads),
        out_shape=(jax.ShapeDtypeStruct((steps, rows, heads * hd), BF16), flat, flat),
        in_specs=[SMEM_SPEC, VMEM_SPEC, VMEM_SPEC, VMEM_SPEC, ANY_SPEC, ANY_SPEC],
        out_specs=(VMEM_SPEC, ANY_SPEC, ANY_SPEC),
        scratch_shapes=[
            pltpu.VMEM((rows, seq_max, hd), BF16),
            pltpu.VMEM((rows, seq_max, hd), BF16),
            pltpu.VMEM((rows * pad, hd), F32),
            pltpu.SemaphoreType.DMA((2, rows // SEQ_BLOCK)),
            pltpu.SemaphoreType.DMA((2, rows // SEQ_BLOCK)),
        ],
        compiler_params=pltpu.CompilerParams(vmem_limit_bytes=VMEM_LIMIT),
        name="attention",
    )(cache_len, q_rows, k_new, v_new, k_cache.reshape(rows, seq_max, hd), v_cache.reshape(rows, seq_max, hd))
    return out, k_out.reshape(k_cache.shape), v_out.reshape(v_cache.shape)


COPIES = ("pair_l", "pair_r", "relay_r", "relay_l", "near_r", "near_l", "far_r", "far_l",
          "own_r", "own_l", "own_s", "pass_r", "pass_l", "sib_l", "sib_r", "sib_fl", "sib_fr")
GATE_TILE = 256
DOWN_TILE = 512


def mlp_kernel(chips, x_hbm, o_ref, wo_hbm, w1_hbm, w3_hbm, w2_hbm, ga_ref, gm_ref, y_out,
               wo, w1, w3, w2, x_own, part, pair_in, relay_in, near_in, hid, act, w_sem, x_sem, y_sem, send_sem, recv_sem):
    steps, rows, d_model = x_hbm.shape
    ff = w1_hbm.shape[1]
    half = d_model // 2
    me = lax.axis_index("tp")
    chip, core = me // 2, lax.rem(me, 2)
    nxt, prv, opp = lax.rem(chip + 1, chips), lax.rem(chip + chips - 1, chips), lax.rem(chip + 2, chips)
    right, left, sib = nxt * 2 + core, prv * 2 + core, chip * 2 + 1 - core
    lo, hi = pl.ds(0, half), pl.ds(half, half)
    n_gate, n_down = ff // GATE_TILE, d_model // DOWN_TILE

    def cols(hbm, buf, j, width, sem):
        return pltpu.make_async_copy(hbm.at[:, pl.ds(j * width, width)], buf.at[:, pl.ds(j * width, width)], w_sem.at[sem])

    wo_in = [cols(wo_hbm, wo, j, half, j) for j in range(2)]
    w1_in = [cols(w1_hbm, w1, j, GATE_TILE, 2 + j) for j in range(n_gate)]
    w3_in = [cols(w3_hbm, w3, j, GATE_TILE, 2 + n_gate + j) for j in range(n_gate)]
    w2_in = [cols(w2_hbm, w2, j, DOWN_TILE, 2 + 2 * n_gate + j) for j in range(n_down)]

    def slot(c, k):
        return pl.ds(pl.multiple_of((c * 2 + k) * SLOT_ROWS, SLOT_ROWS), SLOT_ROWS)

    x_in = [pltpu.make_async_copy(x_hbm.at[t, slot(chip, core), :], x_own.at[t], x_sem.at[t]) for t in range(steps)]
    for copy in wo_in + x_in:
        copy.start()
    for j in range(n_gate):
        w1_in[j].start()
        w3_in[j].start()
    for copy in w2_in:
        copy.start()

    barrier = pltpu.get_barrier_semaphore()
    for other in (right, left, sib):
        pl.semaphore_signal(barrier, inc=1, device_id={"tp": other}, device_id_type=MESH)
    pl.semaphore_wait(barrier, 3)

    def remote(ph, t, name, src, dst, device):
        j = COPIES.index(name)
        return pltpu.make_async_remote_copy(
            src_ref=src, dst_ref=dst, send_sem=send_sem.at[ph, t, j], recv_sem=recv_sem.at[ph, t, j],
            device_id={"tp": device}, device_id_type=MESH)

    def copy(ph, t, name):
        own, other = part.at[t, :, core], part.at[t, :, 1 - core]
        if name == "pair_l":
            return remote(ph, t, name, other.at[:, :, lo], pair_in.at[t, :, :, lo], sib)
        if name == "pair_r":
            return remote(ph, t, name, other.at[:, :, hi], pair_in.at[t, :, :, hi], sib)
        if name == "relay_r":
            return remote(ph, t, name, own.at[opp, :, lo], relay_in.at[t, 0], right)
        if name == "relay_l":
            return remote(ph, t, name, own.at[opp, :, hi], relay_in.at[t, 1], left)
        if name == "near_r":
            return remote(ph, t, name, own.at[nxt, :, hi], near_in.at[t, 0, :, hi], right)
        if name == "near_l":
            return remote(ph, t, name, own.at[prv, :, lo], near_in.at[t, 1, :, lo], left)
        if name == "far_r":
            return remote(ph, t, name, own.at[nxt, :, lo], near_in.at[t, 0, :, lo], right)
        if name == "far_l":
            return remote(ph, t, name, own.at[prv, :, hi], near_in.at[t, 1, :, hi], left)

        def block(c, c_cols, device):
            ref = hid.at[t, slot(c, core), c_cols]
            return remote(ph, t, name, ref, ref, device)

        full = pl.ds(0, d_model)
        if name == "own_r":
            return block(chip, full, right)
        if name == "own_l":
            return block(chip, full, left)
        if name == "own_s":
            return block(chip, full, sib)
        if name == "pass_r":
            return block(prv, lo, right)
        if name == "pass_l":
            return block(nxt, hi, left)
        if name == "sib_l":
            return block(prv, full, sib)
        if name == "sib_r":
            return block(nxt, full, sib)
        if name == "sib_fl":
            return block(opp, lo, sib)
        return block(opp, hi, sib)

    def send(ph, t, *names):
        for name in names:
            copy(ph, t, name).start()

    def recv(ph, t, *names):
        for name in names:
            copy(ph, t, name).wait_recv()

    def sent(ph, t, names):
        for name in names:
            copy(ph, t, name).wait_send()

    def proj(t):
        for j, name in enumerate(("pair_l", "pair_r")):
            if t == 0:
                wo_in[j].wait()
            for n in range(j * half, (j + 1) * half, DOWN_TILE):
                val = matmul(o_ref[t], wo[:, n:n + DOWN_TILE]).astype(BF16)
                part[t, :, :, :, n:n + DOWN_TILE] = val.reshape(chips, 2, SLOT_ROWS, DOWN_TILE)
            send(0, t, name)

    def pair_add(ph, t):
        recv(ph, t, "pair_l", "pair_r")
        for c in range(chips):
            part[t, c, core] = (part[t, c, core].astype(F32) + pair_in[t, c].astype(F32)).astype(BF16)
        send(ph, t, "relay_r", "relay_l", "near_r", "near_l")

    def relay_add(ph, t):
        recv(ph, t, "relay_r")
        part[t, nxt, core, :, :half] = (part[t, nxt, core, :, :half].astype(F32) + relay_in[t, 0].astype(F32)).astype(BF16)
        send(ph, t, "far_r")
        recv(ph, t, "relay_l")
        part[t, prv, core, :, half:] = (part[t, prv, core, :, half:].astype(F32) + relay_in[t, 1].astype(F32)).astype(BF16)
        send(ph, t, "far_l")

    def norm_send(ph, t):
        recv(ph, t, "near_r", "near_l", "far_r", "far_l")
        total = part[t, chip, core].astype(F32) + near_in[t, 0].astype(F32) + near_in[t, 1].astype(F32)
        total = total.astype(BF16).astype(F32)
        fac = lax.rsqrt(jnp.sum(total * total, axis=1, keepdims=True) / d_model + NORM_EPS)
        if ph == 0:
            x_in[t].wait()
            base, gain = x_own[t], ga_ref[...]
        else:
            base, gain = hid[t, slot(chip, core), :], gm_ref[...]
        hid[t, slot(chip, core), :] = (base.astype(F32) + total * fac * gain.astype(F32)).astype(BF16)
        send(ph, t, "own_r", "own_l", "own_s")

    def pass_on(ph, t):
        recv(ph, t, "own_r")
        send(ph, t, "pass_r", "sib_l")
        recv(ph, t, "own_l")
        send(ph, t, "pass_l", "sib_r")

    def pass_sib(ph, t):
        recv(ph, t, "pass_r")
        send(ph, t, "sib_fl")
        recv(ph, t, "pass_l")
        send(ph, t, "sib_fr")

    def gathered(ph, t):
        recv(ph, t, "own_s", "sib_l", "sib_r", "sib_fl", "sib_fr")

    def mlp(t, hooks):
        def run_hooks(key):
            for fn, ph, s in hooks.get(key, ()):
                fn(ph, s)

        for j in range(n_gate):
            if t == 0:
                w1_in[j].wait()
                w3_in[j].wait()
            sl = slice(j * GATE_TILE, (j + 1) * GATE_TILE)
            gate = matmul(hid[t], w1[:, sl])
            up = matmul(hid[t], w3[:, sl])
            act[:, sl] = (gate / (1.0 + jnp.exp(-gate)) * up).astype(BF16)
            run_hooks("g%d" % j)
        sent(0, t, COPIES)
        for j in range(n_down):
            if t == 0:
                w2_in[j].wait()
            sl = slice(j * DOWN_TILE, (j + 1) * DOWN_TILE)
            val = matmul(act[...], w2[:, sl]).astype(BF16)
            part[t, :, :, :, sl] = val.reshape(chips, 2, SLOT_ROWS, DOWN_TILE)
            if j == n_down // 2 - 1:
                send(1, t, "pair_l")
            if j == n_down - 1:
                send(1, t, "pair_r")
            run_hooks("d%d" % j)

    def write_y(ph, t):
        gathered(ph, t)
        pltpu.make_async_copy(hid.at[t], y_out.at[t], y_sem.at[t]).start()

    proj(0)
    proj(1)
    pair_add(0, 0)
    proj(2)
    pair_add(0, 1)
    relay_add(0, 0)
    pair_add(0, 2)
    relay_add(0, 1)
    norm_send(0, 0)
    relay_add(0, 2)
    norm_send(0, 1)
    pass_on(0, 0)
    norm_send(0, 2)
    pass_sib(0, 0)
    gathered(0, 0)
    mlp(0, {"g0": [(pass_on, 0, 1)], "g3": [(pass_sib, 0, 1)], "g5": [(pass_on, 0, 2)],
            "d3": [(pass_sib, 0, 2)], "d7": [(gathered, 0, 1)]})
    mlp(1, {"g2": [(pair_add, 1, 0)], "g6": [(relay_add, 1, 0)], "d7": [(norm_send, 1, 0), (gathered, 0, 2)]})
    mlp(2, {"g2": [(pair_add, 1, 1)], "g6": [(relay_add, 1, 1)], "d1": [(pass_on, 1, 0)], "d6": [(norm_send, 1, 1)],
            "d7": [(pass_sib, 1, 0)]})
    pair_add(1, 2)
    write_y(1, 0)
    pass_on(1, 1)
    relay_add(1, 2)
    pass_sib(1, 1)
    norm_send(1, 2)
    write_y(1, 1)
    pass_on(1, 2)
    pass_sib(1, 2)
    write_y(1, 2)
    for t in range(steps):
        sent(1, t, COPIES)
        pltpu.make_async_copy(hid.at[t], y_out.at[t], y_sem.at[t]).wait()


def run_mlp(tp, x_seq, attn, w_o, w_gate, w_up, w_down, g_attn, g_mlp):
    steps, rows, d_model = x_seq.shape
    ff = w_gate.shape[1]
    chips = tp // 2
    half = d_model // 2
    n_sem = 2 + 2 * (ff // GATE_TILE) + d_model // DOWN_TILE
    return pl.pallas_call(
        functools.partial(mlp_kernel, chips),
        out_shape=jax.ShapeDtypeStruct((steps, rows, d_model), BF16),
        in_specs=[ANY_SPEC, VMEM_SPEC, ANY_SPEC, ANY_SPEC, ANY_SPEC, ANY_SPEC, VMEM_SPEC, VMEM_SPEC],
        out_specs=ANY_SPEC,
        scratch_shapes=[
            pltpu.VMEM(w_o.shape, BF16),
            pltpu.VMEM(w_gate.shape, BF16),
            pltpu.VMEM(w_up.shape, BF16),
            pltpu.VMEM(w_down.shape, BF16),
            pltpu.VMEM((steps, SLOT_ROWS, d_model), BF16),
            pltpu.VMEM((steps, chips, 2, SLOT_ROWS, d_model), BF16),
            pltpu.VMEM((steps, chips, SLOT_ROWS, d_model), BF16),
            pltpu.VMEM((steps, 2, SLOT_ROWS, half), BF16),
            pltpu.VMEM((steps, 2, SLOT_ROWS, d_model), BF16),
            pltpu.VMEM((steps, rows, d_model), BF16),
            pltpu.VMEM((rows, ff), BF16),
            pltpu.SemaphoreType.DMA((n_sem,)),
            pltpu.SemaphoreType.DMA((steps,)),
            pltpu.SemaphoreType.DMA((steps,)),
            pltpu.SemaphoreType.DMA((2, steps, len(COPIES))),
            pltpu.SemaphoreType.DMA((2, steps, len(COPIES))),
        ],
        compiler_params=pltpu.CompilerParams(collective_id=1, has_side_effects=True, vmem_limit_bytes=VMEM_LIMIT),
        name="mlp",
    )(x_seq, attn, w_o, w_gate, w_up, w_down, g_attn.reshape(1, d_model), g_mlp.reshape(1, d_model))


def solution(mesh):
    tp = mesh.shape['tp']

    def local_run(x_seq, cache_len, k_cache, v_cache, w_q, w_k, w_v, w_o, w_gate, w_up, w_down, g_q, g_k, g_attn, g_mlp):
        heads = w_q.shape[1] // w_k.shape[1]
        q_rows, k_new, v_new = run_qkv(tp, x_seq, cache_len, w_q, w_k, w_v, g_q, g_k)
        attn, k_out, v_out = run_attention(heads, cache_len, q_rows, k_new, v_new, k_cache, v_cache)
        y_seq = run_mlp(tp, x_seq, attn, w_o, w_gate, w_up, w_down, g_attn, g_mlp)
        return y_seq, k_out, v_out

    data_spec = P(None, 'dp', None)
    cache_spec = P('dp', 'tp', None, None)
    col_spec = P(None, 'tp')
    row_spec = P('tp', None)
    arg_specs = (data_spec, P('dp'), cache_spec, cache_spec, col_spec, col_spec, col_spec, row_spec, col_spec, col_spec, row_spec, P('tp'), P('tp'), P(None), P(None))
    out_specs = (data_spec, cache_spec, cache_spec)
    return jax.shard_map(local_run, mesh=mesh, in_specs=arg_specs, out_specs=out_specs, check_vma=False)
```

```python
import functools

import jax
import jax.numpy as jnp
import numpy as np
from jax import lax
from jax.experimental import pallas as pl
from jax.experimental.pallas import tpu as pltpu
from jax.sharding import PartitionSpec as P

ROPE_THETA = 500000.0
NORM_EPS = 1e-6
F32 = jnp.float32
BF16 = jnp.bfloat16
MESH = pl.DeviceIdType.MESH
VMEM_SPEC = pl.BlockSpec(memory_space=pltpu.VMEM)
ANY_SPEC = pl.BlockSpec(memory_space=pl.ANY)
SMEM_SPEC = pl.BlockSpec(memory_space=pltpu.SMEM)
VMEM_LIMIT = 67043328
SLOT_ROWS = 16


def matmul(lhs, rhs):
    return jnp.dot(lhs, rhs, preferred_element_type=F32)


def qkv_kernel(tp, q_width, kv_width, x_hbm, len_hbm, freq_hbm, wq_hbm, wk_hbm, wv_hbm, gq_hbm, gk_hbm,
               q_hbm, kn_hbm, vn_hbm,
               len_ref, freq_ref, gq_ref, gk_ref, q_out, kn_out, vn_out, small_sem, out_sem, x_buf, wq_buf, wk_buf, wv_buf, q_raw, q_rows, part, inbox, turn, in_sem, send_sem, recv_sem):
    steps, rows, _ = x_hbm.shape
    hd = wk_hbm.shape[1]
    heads = wq_hbm.shape[1] // hd
    pad = q_hbm.shape[1]
    me = lax.axis_index("tp")
    x_in = [pltpu.make_async_copy(x_hbm.at[t], x_buf.at[pl.ds(t * rows, rows), :], in_sem.at[t]) for t in range(steps)]
    for copy in x_in:
        copy.start()
    half = heads * hd // 2
    wk_in = pltpu.make_async_copy(wk_hbm, wk_buf, in_sem.at[3])
    wq_in = [pltpu.make_async_copy(wq_hbm.at[:, pl.ds(j * half, half)], wq_buf.at[:, pl.ds(j * half, half)], in_sem.at[4 + j]) for j in range(2)]
    wv_in = pltpu.make_async_copy(wv_hbm, wv_buf, in_sem.at[6])
    small_in = [pltpu.make_async_copy(src, dst, small_sem.at[i]) for i, (src, dst) in enumerate(
        ((len_hbm, len_ref), (freq_hbm, freq_ref), (gq_hbm, gq_ref), (gk_hbm, gk_ref)))]
    outs = [pltpu.make_async_copy(src, dst, out_sem.at[i]) for i, (src, dst) in enumerate(
        ((q_out, q_hbm), (kn_out, kn_hbm), (vn_out, vn_hbm)))]
    for copy in small_in + [wk_in, wq_in[0], wq_in[1], wv_in]:
        copy.start()

    barrier = pltpu.get_barrier_semaphore()
    for j in range(1, tp):
        pl.semaphore_signal(barrier, inc=1, device_id={"tp": lax.rem(me + j, tp)}, device_id_type=MESH)

    for copy in small_in:
        copy.wait()
    lens = jnp.transpose(jnp.broadcast_to(len_ref[...].astype(F32), (rows, rows)))[:, :hd]
    lane = lax.broadcasted_iota(jnp.int32, (rows, hd), 1)
    sign = jnp.where(lane < hd // 2, -1.0, 1.0).astype(F32)
    tables = []
    for t in range(steps):
        angle = (lens + float(t)) * freq_ref[...]
        tables.append((jnp.cos(angle), jnp.sin(angle) * sign))

    q_rows[...] = jnp.zeros_like(q_rows)
    for copy in x_in:
        copy.wait()
    wk_in.wait()
    k_raw = matmul(x_buf[...], wk_buf[...]).astype(BF16).astype(F32)
    k_sq = jnp.sum(k_raw * k_raw, axis=1, keepdims=True)
    q_sq = None
    for j in range(2):
        wq_in[j].wait()
        val = matmul(x_buf[...], wq_buf[:, j * half:(j + 1) * half]).astype(BF16).astype(F32)
        q_raw[:, j * half:(j + 1) * half] = val
        sq = jnp.sum(val * val, axis=1, keepdims=True)
        q_sq = sq if q_sq is None else q_sq + sq
    packed = jnp.zeros((rows, rows), F32)
    col = lax.broadcasted_iota(jnp.int32, (rows, rows), 1)
    for t in range(steps):
        packed = jnp.where(col == t, q_sq[t * rows:(t + 1) * rows], packed)
        packed = jnp.where(col == steps + t, k_sq[t * rows:(t + 1) * rows], packed)
    part[...] = jnp.transpose(packed)[:part.shape[0]]
    pl.semaphore_wait(barrier, tp - 1)
    copies = []
    for j in range(1, tp):
        copy = pltpu.make_async_remote_copy(
            src_ref=part, dst_ref=inbox.at[j - 1], send_sem=send_sem.at[j - 1], recv_sem=recv_sem.at[j - 1],
            device_id={"tp": lax.rem(me + j, tp)}, device_id_type=MESH)
        copy.start()
        copies.append(copy)
    wv_in.wait()
    vn_out[...] = matmul(x_buf[...], wv_buf[...]).astype(BF16).astype(F32).reshape(steps, rows, hd)
    outs[2].start()
    total = part[...]
    for j in range(1, tp):
        copies[j - 1].wait()
        total = total + inbox[j - 1]
    turn[...] = jnp.zeros_like(turn)
    turn[0:part.shape[0], :] = total
    sums = jnp.transpose(turn[...])
    gain_k = gk_ref[...].astype(F32)
    gain_q = gq_ref[...].astype(F32)
    for t in range(steps):
        cos_tab, sin_tab = tables[t]
        q_fac = lax.rsqrt(sums[:, t:t + 1] / q_width + NORM_EPS)
        k_fac = lax.rsqrt(sums[:, steps + t:steps + t + 1] / kv_width + NORM_EPS)
        val = k_raw[t * rows:(t + 1) * rows] * k_fac * gain_k
        val = val * cos_tab + pltpu.roll(val, hd // 2, axis=1) * sin_tab
        kn_out[t] = val.astype(BF16).astype(F32)
        for g in range(heads):
            val = q_raw[t * rows:(t + 1) * rows, g * hd:(g + 1) * hd] * q_fac * gain_q[g:g + 1, :]
            val = val * cos_tab + pltpu.roll(val, hd // 2, axis=1) * sin_tab
            q_rows[pl.ds(t * heads + g, rows, stride=pad), :] = val
    outs[1].start()
    q_out[...] = q_rows[...].reshape(rows, pad, hd).astype(BF16)
    outs[0].start()
    for copy in outs:
        copy.wait()


def run_qkv(tp, x_seq, cache_len, w_q, w_k, w_v, g_q, g_k):
    steps, rows, d_model = x_seq.shape
    hd = w_k.shape[1]
    width = w_q.shape[1]
    heads = width // hd
    pad = 16
    inv_freq = (ROPE_THETA ** (-(np.arange(hd // 2, dtype=np.float64) * (2.0 / hd)))).astype(np.float32)
    freq = jnp.asarray(np.concatenate([inv_freq, inv_freq])[None, :])
    return pl.pallas_call(
        functools.partial(qkv_kernel, tp, width * tp, hd * tp),
        out_shape=(jax.ShapeDtypeStruct((rows, pad, hd), BF16),
                   jax.ShapeDtypeStruct((steps, rows, hd), F32),
                   jax.ShapeDtypeStruct((steps, rows, hd), F32)),
        in_specs=[ANY_SPEC] * 8,
        out_specs=(ANY_SPEC, ANY_SPEC, ANY_SPEC),
        scratch_shapes=[
            pltpu.VMEM((1, rows), jnp.int32),
            pltpu.VMEM((1, hd), F32),
            pltpu.VMEM((heads, hd), BF16),
            pltpu.VMEM((1, hd), BF16),
            pltpu.VMEM((rows, pad, hd), BF16),
            pltpu.VMEM((steps, rows, hd), F32),
            pltpu.VMEM((steps, rows, hd), F32),
            pltpu.SemaphoreType.DMA((4,)),
            pltpu.SemaphoreType.DMA((3,)),
            pltpu.VMEM((steps * rows, d_model), BF16),
            pltpu.VMEM((d_model, width), BF16),
            pltpu.VMEM((d_model, hd), BF16),
            pltpu.VMEM((d_model, hd), BF16),
            pltpu.VMEM((steps * rows, width), F32),
            pltpu.VMEM((rows * pad, hd), F32),
            pltpu.VMEM((8, rows), F32),
            pltpu.VMEM((tp - 1, 8, rows), F32),
            pltpu.VMEM((rows, rows), F32),
            pltpu.SemaphoreType.DMA((7,)),
            pltpu.SemaphoreType.DMA((tp - 1,)),
            pltpu.SemaphoreType.DMA((tp - 1,)),
        ],
        compiler_params=pltpu.CompilerParams(collective_id=0, has_side_effects=True, vmem_limit_bytes=VMEM_LIMIT),
        name="qkv",
    )(x_seq, cache_len.reshape(1, rows), freq, w_q, w_k, w_v, g_q.reshape(heads, hd), g_k.reshape(1, hd))


SEQ_BLOCK = 8
PATCH_ROWS = 32


def attention_kernel(steps, heads, len_ref, q_hbm, kn_hbm, vn_hbm, k_hbm, v_hbm, o_hbm, k_out, v_out,
                     q_ref, kn_ref, vn_ref, o_ref, small_sem, k_buf, v_buf, mixed, in_sem, out_sem):
    rows, seq_max, hd = k_hbm.shape
    pad = q_hbm.shape[1]
    blocks = rows // SEQ_BLOCK

    def moves(blk, inward):
        sl = pl.ds(blk * SEQ_BLOCK, SEQ_BLOCK)
        if inward:
            return (pltpu.make_async_copy(k_hbm.at[sl], k_buf.at[sl], in_sem.at[0, blk]),
                    pltpu.make_async_copy(v_hbm.at[sl], v_buf.at[sl], in_sem.at[1, blk]))
        return (pltpu.make_async_copy(k_buf.at[sl], k_out.at[sl], out_sem.at[0, blk]),
                pltpu.make_async_copy(v_buf.at[sl], v_out.at[sl], out_sem.at[1, blk]))

    def start_in(blk, carry):
        for copy in moves(blk, True):
            copy.start()
        return carry

    small_in = [pltpu.make_async_copy(src, dst, small_sem.at[i]) for i, (src, dst) in enumerate(
        ((q_hbm, q_ref), (kn_hbm, kn_ref), (vn_hbm, vn_ref)))]
    o_store = pltpu.make_async_copy(o_ref, o_hbm, small_sem.at[3])
    start_in(0, 0)
    for copy in small_in:
        copy.start()
    lax.fori_loop(1, blocks, start_in, 0)
    scale = hd ** -0.5
    win_row = lax.broadcasted_iota(jnp.int32, (PATCH_ROWS, hd), 0)
    key_col = lax.broadcasted_iota(jnp.int32, (pad, seq_max), 1)
    step_row = lax.broadcasted_iota(jnp.int32, (pad, seq_max), 0) // heads
    key_off = key_col - step_row

    def body(blk, carry):
        for copy in moves(blk, True):
            copy.wait()
        lens = []
        for i in range(SEQ_BLOCK):
            b = blk * SEQ_BLOCK + i
            length = len_ref[b]
            base = pl.multiple_of(jnp.minimum((length // 16) * 16, seq_max - PATCH_ROWS), 16)
            for buf, new_ref in ((k_buf, kn_ref), (v_buf, vn_ref)):
                win = buf[b, pl.ds(base, PATCH_ROWS), :].astype(F32)
                for t in range(steps):
                    win = jnp.where(win_row == length + t - base, new_ref[t, pl.ds(b, 1), :], win)
                buf[b, pl.ds(base, PATCH_ROWS), :] = win.astype(BF16)
            lens.append(length)
        scores = []
        for i in range(SEQ_BLOCK):
            b = blk * SEQ_BLOCK + i
            s = lax.dot_general(q_ref[b], k_buf[b], (((1,), (1,)), ((), ())), preferred_element_type=F32) * scale
            scores.append(jnp.where(key_off <= lens[i], s, -jnp.inf))
        exps = []
        for i in range(SEQ_BLOCK):
            e = jnp.exp(scores[i] - jnp.max(scores[i], axis=1, keepdims=True))
            exps.append((e.astype(BF16), jnp.sum(e, axis=1, keepdims=True)))
        for i in range(SEQ_BLOCK):
            b = blk * SEQ_BLOCK + i
            out = matmul(exps[i][0], v_buf[b]) / exps[i][1]
            mixed[pl.ds(pl.multiple_of(b * pad, pad), pad), :] = out
        for copy in moves(blk, False):
            copy.start()
        return carry

    for copy in small_in:
        copy.wait()
    lax.fori_loop(0, blocks, body, 0)
    for t in range(steps):
        for g in range(heads):
            o_ref[t, :, g * hd:(g + 1) * hd] = mixed[pl.ds(t * heads + g, rows, stride=pad), :].astype(BF16)

    o_store.start()

    def finish(blk, carry):
        for copy in moves(blk, False):
            copy.wait()
        return carry

    lax.fori_loop(0, blocks, finish, 0)
    o_store.wait()


def run_attention(heads, cache_len, q_rows, k_new, v_new, k_cache, v_cache):
    rows, _, seq_max, hd = k_cache.shape
    steps = k_new.shape[0]
    pad = q_rows.shape[1]
    flat = jax.ShapeDtypeStruct((rows, seq_max, hd), BF16)
    out, k_out, v_out = pl.pallas_call(
        functools.partial(attention_kernel, steps, heads),
        out_shape=(jax.ShapeDtypeStruct((steps, rows, heads * hd), BF16), flat, flat),
        in_specs=[SMEM_SPEC] + [ANY_SPEC] * 5,
        out_specs=(ANY_SPEC, ANY_SPEC, ANY_SPEC),
        scratch_shapes=[
            pltpu.VMEM(q_rows.shape, BF16),
            pltpu.VMEM(k_new.shape, F32),
            pltpu.VMEM(v_new.shape, F32),
            pltpu.VMEM((steps, rows, heads * hd), BF16),
            pltpu.SemaphoreType.DMA((4,)),
            pltpu.VMEM((rows, seq_max, hd), BF16),
            pltpu.VMEM((rows, seq_max, hd), BF16),
            pltpu.VMEM((rows * pad, hd), F32),
            pltpu.SemaphoreType.DMA((2, rows // SEQ_BLOCK)),
            pltpu.SemaphoreType.DMA((2, rows // SEQ_BLOCK)),
        ],
        compiler_params=pltpu.CompilerParams(vmem_limit_bytes=VMEM_LIMIT),
        name="attention",
    )(cache_len, q_rows, k_new, v_new, k_cache.reshape(rows, seq_max, hd), v_cache.reshape(rows, seq_max, hd))
    return out, k_out.reshape(k_cache.shape), v_out.reshape(v_cache.shape)


QUARTERS = 4
LEFT_PIECES = tuple(range(QUARTERS // 2))
RIGHT_PIECES = tuple(range(QUARTERS // 2, QUARTERS))
PIECED = ("pair", "relay", "near", "far", "own_r", "own_l", "pass")
WHOLE = ("own_s", "sib_r", "sib_l", "sib_fr", "sib_fl")
COPIES = tuple((kind, q) for kind in PIECED for q in range(QUARTERS)) + tuple((kind, 0) for kind in WHOLE)
GATE_TILE = 256
DOWN_TILE = 512
TASKS = ("proj", "pair", "relay", "norm", "pass", "sib", "sibf", "gather", "gate", "down")
ORDER = (
    0, 1, 3, 100, 2, 101, 13, 23, 103, 10, 102, 11, 113, 12, 111, 110, 201, 200, 112, 203, 20, 22, 202, 123,
    120, 210, 213, 212, 122, 21, 211, 300, 121, 400, 402, 403, 401, 310, 501, 220, 221, 223, 500, 600, 601, 222, 700, 410,
    800, 801, 413, 411, 412, 802, 803, 511, 320, 804, 805, 806, 900, 901, 610, 510, 902, 903, 611, 904, 420, 905, 422, 150,
    906, 421, 423, 907, 710, 810, 151, 811, 812, 153, 152, 813, 814, 815, 621, 816, 620, 251, 910, 911, 912, 521, 253, 520,
    913, 250, 914, 252, 160, 915, 916, 917, 720, 820, 161, 821, 822, 163, 823, 350, 260, 162, 824, 825, 826, 920, 921, 922,
    263, 923, 924, 925, 170, 926, 171, 927, 172, 261, 173, 262, 453, 451, 270, 452, 450, 551, 550, 271, 272, 273, 360, 370,
    460, 461, 462, 463, 650, 472, 560, 470, 561, 473, 471, 651, 570, 750, 660, 571, 661, 671, 670, 760, 770,
)


def mlp_kernel(chips, x_hbm, o_hbm, wo_hbm, w1_hbm, w3_hbm, w2_hbm, ga_hbm, gm_hbm, y_out,
               o_ref, ga_ref, gm_ref, small_sem, wo, w1, w3, w2, x_own, gains, part, pair_in, relay_in, near_in, hid, act, w_sem, x_sem, y_sem, send_sem, recv_sem):
    steps, rows, d_model = x_hbm.shape
    ff = w1_hbm.shape[1]
    piece = d_model // QUARTERS
    me = lax.axis_index("tp")
    chip, core = me // 2, lax.rem(me, 2)
    nxt, prv, opp = lax.rem(chip + 1, chips), lax.rem(chip + chips - 1, chips), lax.rem(chip + 2, chips)
    right, left, sib = nxt * 2 + core, prv * 2 + core, chip * 2 + 1 - core
    n_gate, n_down = ff // GATE_TILE, d_model // DOWN_TILE

    def cols(hbm, buf, j, width, sem):
        return pltpu.make_async_copy(hbm.at[:, pl.ds(j * width, width)], buf.at[:, pl.ds(j * width, width)], w_sem.at[sem])

    wo_in = [cols(wo_hbm, wo, j, piece, j) for j in range(QUARTERS)]
    w1_in = [cols(w1_hbm, w1, j, GATE_TILE, QUARTERS + j) for j in range(n_gate)]
    w3_in = [cols(w3_hbm, w3, j, GATE_TILE, QUARTERS + n_gate + j) for j in range(n_gate)]
    w2_in = [cols(w2_hbm, w2, j, DOWN_TILE, QUARTERS + 2 * n_gate + j) for j in range(n_down)]

    def slot(c, k):
        return pl.ds(pl.multiple_of((c * 2 + k) * SLOT_ROWS, SLOT_ROWS), SLOT_ROWS)

    x_in = [pltpu.make_async_copy(x_hbm.at[t, slot(chip, core), :], x_own.at[t], x_sem.at[t]) for t in range(steps)]
    small_in = [pltpu.make_async_copy(src, dst, small_sem.at[i]) for i, (src, dst) in enumerate(
        ((o_hbm, o_ref), (ga_hbm, ga_ref), (gm_hbm, gm_ref)))]
    for copy in small_in + wo_in + x_in:
        copy.start()
    for j in range(n_gate):
        w1_in[j].start()
        w3_in[j].start()
    for copy in w2_in:
        copy.start()

    barrier = pltpu.get_barrier_semaphore()
    for other in (right, left, sib):
        pl.semaphore_signal(barrier, inc=1, device_id={"tp": other}, device_id_type=MESH)
    for copy in small_in:
        copy.wait()
    for i, ref in enumerate((ga_ref, gm_ref)):
        vals = ref[...].astype(F32)
        for j in range(vals.shape[0]):
            gains[i, :, j * vals.shape[1]:(j + 1) * vals.shape[1]] = vals[j:j + 1, :]
    pl.semaphore_wait(barrier, 3)

    def quarter(q, count=1):
        return pl.ds(q * piece, count * piece)

    def endpoints(t, kind, q):
        own, other = part.at[t, :, core], part.at[t, :, 1 - core]
        to_right = q in LEFT_PIECES
        c = quarter(q)
        if kind == "pair":
            return other.at[:, :, c], pair_in.at[t, :, :, c], sib
        if kind == "relay":
            return own.at[opp, :, c], relay_in.at[t, :, c], right if to_right else left
        if kind == "near":
            if to_right:
                return own.at[prv, :, c], near_in.at[t, 1, :, c], left
            return own.at[nxt, :, c], near_in.at[t, 0, :, c], right
        if kind == "far":
            if to_right:
                return own.at[nxt, :, c], near_in.at[t, 0, :, c], right
            return own.at[prv, :, c], near_in.at[t, 1, :, c], left
        if kind == "own_r":
            block, device = hid.at[t, slot(chip, core), c], right
        elif kind == "own_l":
            block, device = hid.at[t, slot(chip, core), c], left
        elif kind == "pass":
            block, device = (hid.at[t, slot(prv, core), c], right) if to_right else (hid.at[t, slot(nxt, core), c], left)
        elif kind == "own_s":
            block, device = hid.at[t, slot(chip, core), :], sib
        elif kind == "sib_r":
            block, device = hid.at[t, slot(prv, core), :], sib
        elif kind == "sib_l":
            block, device = hid.at[t, slot(nxt, core), :], sib
        elif kind == "sib_fr":
            block, device = hid.at[t, slot(opp, core), quarter(0, QUARTERS // 2)], sib
        else:
            block, device = hid.at[t, slot(opp, core), quarter(QUARTERS // 2, QUARTERS // 2)], sib
        return block, block, device

    def copy(ph, t, kind, q=0):
        src, dst, device = endpoints(t, kind, q)
        j = COPIES.index((kind, q))
        return pltpu.make_async_remote_copy(
            src_ref=src, dst_ref=dst, send_sem=send_sem.at[ph, t, j], recv_sem=recv_sem.at[ph, t, j],
            device_id={"tp": device}, device_id_type=MESH)

    def sent(ph, t):
        for kind, q in COPIES:
            copy(ph, t, kind, q).wait_send()

    def proj(ph, t, q):
        if t == 0:
            wo_in[q].wait()
        for n in range(q * piece, (q + 1) * piece, DOWN_TILE):
            val = matmul(o_ref[t], wo[:, n:n + DOWN_TILE]).astype(BF16)
            part[t, :, :, :, n:n + DOWN_TILE] = val.reshape(chips, 2, SLOT_ROWS, DOWN_TILE)
        copy(0, t, "pair", q).start()

    def pair_add(ph, t, q):
        copy(ph, t, "pair", q).wait_recv()
        c = slice(q * piece, (q + 1) * piece)
        for n in (opp, prv, nxt, chip):
            part[t, n, core, :, c] = (part[t, n, core, :, c].astype(F32) + pair_in[t, n, :, c].astype(F32)).astype(BF16)
        copy(ph, t, "relay", q).start()
        copy(ph, t, "near", q).start()

    def relay_add(ph, t, q):
        copy(ph, t, "relay", q).wait_recv()
        c = slice(q * piece, (q + 1) * piece)
        n = nxt if q in LEFT_PIECES else prv
        part[t, n, core, :, c] = (part[t, n, core, :, c].astype(F32) + relay_in[t, :, c].astype(F32)).astype(BF16)
        copy(ph, t, "far", q).start()

    def norm(ph, t, _):
        for q in range(QUARTERS):
            copy(ph, t, "near", q).wait_recv()
            copy(ph, t, "far", q).wait_recv()
        total = part[t, chip, core].astype(F32) + near_in[t, 0].astype(F32) + near_in[t, 1].astype(F32)
        total = total.astype(BF16).astype(F32)
        fac = lax.rsqrt(jnp.sum(total * total, axis=1, keepdims=True) / d_model + NORM_EPS)
        if ph == 0:
            x_in[t].wait()
            base = x_own[t]
        else:
            base = hid[t, slot(chip, core), :]
        hid[t, slot(chip, core), :] = (base.astype(F32) + total * fac * gains[ph]).astype(BF16)
        for first, second in ((LEFT_PIECES, RIGHT_PIECES), (RIGHT_PIECES, LEFT_PIECES)):
            for i, j in zip(first, second):
                copy(ph, t, "own_r", i).start()
                copy(ph, t, "own_l", j).start()
        copy(ph, t, "own_s").start()

    def pass_on(ph, t, q):
        copy(ph, t, "own_r" if q in LEFT_PIECES else "own_l", q).wait_recv()
        copy(ph, t, "pass", q).start()

    def pass_sib(ph, t, side):
        for q in (RIGHT_PIECES, LEFT_PIECES)[side]:
            copy(ph, t, ("own_r", "own_l")[side], q).wait_recv()
        copy(ph, t, ("sib_r", "sib_l")[side]).start()

    def far_sib(ph, t, side):
        for q in (LEFT_PIECES, RIGHT_PIECES)[side]:
            copy(ph, t, "pass", q).wait_recv()
        copy(ph, t, ("sib_fr", "sib_fl")[side]).start()

    def gather(ph, t, _):
        for kind in WHOLE:
            copy(ph, t, kind).wait_recv()
        if ph == 1:
            pltpu.make_async_copy(hid.at[t], y_out.at[t], y_sem.at[t]).start()

    def gate_up(ph, t, j):
        if t == 0:
            w1_in[j].wait()
            w3_in[j].wait()
        sl = slice(j * GATE_TILE, (j + 1) * GATE_TILE)
        gate = matmul(hid[t], w1[:, sl])
        up = matmul(hid[t], w3[:, sl])
        act[:, sl] = (gate / (1.0 + jnp.exp(-gate)) * up).astype(BF16)

    def down(ph, t, j):
        if j == 0:
            sent(0, t)
        if t == 0:
            w2_in[j].wait()
        sl = slice(j * DOWN_TILE, (j + 1) * DOWN_TILE)
        val = matmul(act[...], w2[:, sl]).astype(BF16)
        part[t, :, :, :, sl] = val.reshape(chips, 2, SLOT_ROWS, DOWN_TILE)
        if (j + 1) * DOWN_TILE % piece == 0:
            copy(1, t, "pair", (j + 1) * DOWN_TILE // piece - 1).start()

    run = (proj, pair_add, relay_add, norm, pass_on, pass_sib, far_sib, gather, gate_up, down)
    for code in ORDER:
        run[code // 100](code // 50 % 2, code % 50 // 10, code % 10)
    for t in range(steps):
        sent(1, t)
        pltpu.make_async_copy(hid.at[t], y_out.at[t], y_sem.at[t]).wait()


def run_mlp(tp, x_seq, attn, w_o, w_gate, w_up, w_down, g_attn, g_mlp):
    steps, rows, d_model = x_seq.shape
    ff = w_gate.shape[1]
    chips = tp // 2
    n_sem = QUARTERS + 2 * (ff // GATE_TILE) + d_model // DOWN_TILE
    return pl.pallas_call(
        functools.partial(mlp_kernel, chips),
        out_shape=jax.ShapeDtypeStruct((steps, rows, d_model), BF16),
        in_specs=[ANY_SPEC] * 8,
        out_specs=ANY_SPEC,
        scratch_shapes=[
            pltpu.VMEM(attn.shape, BF16),
            pltpu.VMEM((d_model // 128, 128), BF16),
            pltpu.VMEM((d_model // 128, 128), BF16),
            pltpu.SemaphoreType.DMA((3,)),
            pltpu.VMEM(w_o.shape, BF16),
            pltpu.VMEM(w_gate.shape, BF16),
            pltpu.VMEM(w_up.shape, BF16),
            pltpu.VMEM(w_down.shape, BF16),
            pltpu.VMEM((steps, SLOT_ROWS, d_model), BF16),
            pltpu.VMEM((2, 1, d_model), F32),
            pltpu.VMEM((steps, chips, 2, SLOT_ROWS, d_model), BF16),
            pltpu.VMEM((steps, chips, SLOT_ROWS, d_model), BF16),
            pltpu.VMEM((steps, SLOT_ROWS, d_model), BF16),
            pltpu.VMEM((steps, 2, SLOT_ROWS, d_model), BF16),
            pltpu.VMEM((steps, rows, d_model), BF16),
            pltpu.VMEM((rows, ff), BF16),
            pltpu.SemaphoreType.DMA((n_sem,)),
            pltpu.SemaphoreType.DMA((steps,)),
            pltpu.SemaphoreType.DMA((steps,)),
            pltpu.SemaphoreType.DMA((2, steps, len(COPIES))),
            pltpu.SemaphoreType.DMA((2, steps, len(COPIES))),
        ],
        compiler_params=pltpu.CompilerParams(collective_id=1, has_side_effects=True, vmem_limit_bytes=VMEM_LIMIT),
        name="mlp",
    )(x_seq, attn, w_o, w_gate, w_up, w_down, g_attn.reshape(-1, 128), g_mlp.reshape(-1, 128))


COPY_ROWS = 64


def store_kernel(src, dst, buf, in_sem, out_sem):
    rows = src.shape[0]
    n = rows // COPY_ROWS
    sl = [pl.ds(i * COPY_ROWS, COPY_ROWS) for i in range(n)]
    ins = [pltpu.make_async_copy(src.at[sl[i]], buf.at[sl[i]], in_sem.at[i]) for i in range(n)]
    outs = [pltpu.make_async_copy(buf.at[sl[i]], dst.at[sl[i]], out_sem.at[i]) for i in range(n)]
    for i in range(n):
        ins[i].start()
    for i in range(n):
        ins[i].wait()
        outs[i].start()
    for i in range(n):
        outs[i].wait()


def run_store(y_seq):
    steps, rows, d_model = y_seq.shape
    total = steps * rows
    return pl.pallas_call(
        store_kernel,
        out_shape=jax.ShapeDtypeStruct((total, d_model), BF16),
        in_specs=[ANY_SPEC],
        out_specs=ANY_SPEC,
        scratch_shapes=[
            pltpu.VMEM((total, d_model), BF16),
            pltpu.SemaphoreType.DMA((total // COPY_ROWS,)),
            pltpu.SemaphoreType.DMA((total // COPY_ROWS,)),
        ],
        compiler_params=pltpu.CompilerParams(vmem_limit_bytes=VMEM_LIMIT),
        name="store",
    )(y_seq.reshape(total, d_model)).reshape(y_seq.shape)


def solution(mesh):
    tp = mesh.shape['tp']

    def local_run(x_seq, cache_len, k_cache, v_cache, w_q, w_k, w_v, w_o, w_gate, w_up, w_down, g_q, g_k, g_attn, g_mlp):
        heads = w_q.shape[1] // w_k.shape[1]
        q_rows, k_new, v_new = run_qkv(tp, x_seq, cache_len, w_q, w_k, w_v, g_q, g_k)
        attn, k_out, v_out = run_attention(heads, cache_len, q_rows, k_new, v_new, k_cache, v_cache)
        y_seq = run_mlp(tp, x_seq, attn, w_o, w_gate, w_up, w_down, g_attn, g_mlp)
        return run_store(y_seq), k_out, v_out

    data_spec = P(None, 'dp', None)
    cache_spec = P('dp', 'tp', None, None)
    col_spec = P(None, 'tp')
    row_spec = P('tp', None)
    arg_specs = (data_spec, P('dp'), cache_spec, cache_spec, col_spec, col_spec, col_spec, row_spec, col_spec, col_spec, row_spec, P('tp'), P('tp'), P(None), P(None))
    out_specs = (data_spec, cache_spec, cache_spec)
    return jax.shard_map(local_run, mesh=mesh, in_specs=arg_specs, out_specs=out_specs, check_vma=False)
```

```python
import functools

import jax
import jax.numpy as jnp
import numpy as np
from jax import lax
from jax.experimental import pallas as pl
from jax.experimental.pallas import tpu as pltpu
from jax.sharding import PartitionSpec as P

ROPE_THETA = 500000.0
NORM_EPS = 1e-6
F32 = jnp.float32
BF16 = jnp.bfloat16
MESH = pl.DeviceIdType.MESH
VMEM_SPEC = pl.BlockSpec(memory_space=pltpu.VMEM)
ANY_SPEC = pl.BlockSpec(memory_space=pl.ANY)
SMEM_SPEC = pl.BlockSpec(memory_space=pltpu.SMEM)
VMEM_LIMIT = 67043328
SLOT_ROWS = 16


def matmul(lhs, rhs):
    return jnp.dot(lhs, rhs, preferred_element_type=F32)


def qkv_kernel(tp, q_width, kv_width, x_hbm, len_hbm, freq_hbm, wq_hbm, wk_hbm, wv_hbm, gq_hbm, gk_hbm,
               q_hbm, kn_hbm, vn_hbm,
               len_ref, freq_ref, gq_ref, gk_ref, q_out, kn_out, vn_out, small_sem, out_sem, x_buf, wq_buf, wk_buf, wv_buf, q_raw, q_rows, part, inbox, turn, in_sem, send_sem, recv_sem):
    steps, rows, _ = x_hbm.shape
    hd = wk_hbm.shape[1]
    heads = wq_hbm.shape[1] // hd
    pad = q_hbm.shape[1]
    me = lax.axis_index("tp")
    x_in = [pltpu.make_async_copy(x_hbm.at[t], x_buf.at[pl.ds(t * rows, rows), :], in_sem.at[t]) for t in range(steps)]
    for copy in x_in:
        copy.start()
    half = heads * hd // 2
    wk_in = pltpu.make_async_copy(wk_hbm, wk_buf, in_sem.at[3])
    wq_in = [pltpu.make_async_copy(wq_hbm.at[:, pl.ds(j * half, half)], wq_buf.at[:, pl.ds(j * half, half)], in_sem.at[4 + j]) for j in range(2)]
    wv_in = pltpu.make_async_copy(wv_hbm, wv_buf, in_sem.at[6])
    small_in = [pltpu.make_async_copy(src, dst, small_sem.at[i]) for i, (src, dst) in enumerate(
        ((len_hbm, len_ref), (freq_hbm, freq_ref), (gq_hbm, gq_ref), (gk_hbm, gk_ref)))]
    outs = [pltpu.make_async_copy(src, dst, out_sem.at[i]) for i, (src, dst) in enumerate(
        ((q_out, q_hbm), (kn_out, kn_hbm), (vn_out, vn_hbm)))]
    for copy in small_in + [wk_in, wq_in[0], wq_in[1], wv_in]:
        copy.start()

    barrier = pltpu.get_barrier_semaphore()
    for j in range(1, tp):
        pl.semaphore_signal(barrier, inc=1, device_id={"tp": lax.rem(me + j, tp)}, device_id_type=MESH)

    for copy in small_in:
        copy.wait()
    lens = jnp.transpose(jnp.broadcast_to(len_ref[...].astype(F32), (rows, rows)))[:, :hd]
    lane = lax.broadcasted_iota(jnp.int32, (rows, hd), 1)
    sign = jnp.where(lane < hd // 2, -1.0, 1.0).astype(F32)
    tables = []
    for t in range(steps):
        angle = (lens + float(t)) * freq_ref[...]
        tables.append((jnp.cos(angle), jnp.sin(angle) * sign))

    q_rows[...] = jnp.zeros_like(q_rows)
    for copy in x_in:
        copy.wait()
    wk_in.wait()
    k_raw = matmul(x_buf[...], wk_buf[...]).astype(BF16).astype(F32)
    k_sq = jnp.sum(k_raw * k_raw, axis=1, keepdims=True)
    q_sq = None
    for j in range(2):
        wq_in[j].wait()
        val = matmul(x_buf[...], wq_buf[:, j * half:(j + 1) * half]).astype(BF16).astype(F32)
        q_raw[:, j * half:(j + 1) * half] = val
        sq = jnp.sum(val * val, axis=1, keepdims=True)
        q_sq = sq if q_sq is None else q_sq + sq
    packed = jnp.zeros((rows, rows), F32)
    col = lax.broadcasted_iota(jnp.int32, (rows, rows), 1)
    for t in range(steps):
        packed = jnp.where(col == t, q_sq[t * rows:(t + 1) * rows], packed)
        packed = jnp.where(col == steps + t, k_sq[t * rows:(t + 1) * rows], packed)
    part[...] = jnp.transpose(packed)[:part.shape[0]]
    pl.semaphore_wait(barrier, tp - 1)
    copies = []
    for j in range(1, tp):
        copy = pltpu.make_async_remote_copy(
            src_ref=part, dst_ref=inbox.at[j - 1], send_sem=send_sem.at[j - 1], recv_sem=recv_sem.at[j - 1],
            device_id={"tp": lax.rem(me + j, tp)}, device_id_type=MESH)
        copy.start()
        copies.append(copy)
    wv_in.wait()
    vn_out[...] = matmul(x_buf[...], wv_buf[...]).astype(BF16).astype(F32).reshape(steps, rows, hd)
    outs[2].start()
    total = part[...]
    for j in range(1, tp):
        copies[j - 1].wait()
        total = total + inbox[j - 1]
    turn[...] = jnp.zeros_like(turn)
    turn[0:part.shape[0], :] = total
    sums = jnp.transpose(turn[...])
    gain_k = gk_ref[...].astype(F32)
    gain_q = gq_ref[...].astype(F32)
    for t in range(steps):
        cos_tab, sin_tab = tables[t]
        q_fac = lax.rsqrt(sums[:, t:t + 1] / q_width + NORM_EPS)
        k_fac = lax.rsqrt(sums[:, steps + t:steps + t + 1] / kv_width + NORM_EPS)
        val = k_raw[t * rows:(t + 1) * rows] * k_fac * gain_k
        val = val * cos_tab + pltpu.roll(val, hd // 2, axis=1) * sin_tab
        kn_out[t] = val.astype(BF16).astype(F32)
        for g in range(heads):
            val = q_raw[t * rows:(t + 1) * rows, g * hd:(g + 1) * hd] * q_fac * gain_q[g:g + 1, :]
            val = val * cos_tab + pltpu.roll(val, hd // 2, axis=1) * sin_tab
            q_rows[pl.ds(t * heads + g, rows, stride=pad), :] = val
    outs[1].start()
    q_out[...] = q_rows[...].reshape(rows, pad, hd).astype(BF16)
    outs[0].start()
    for copy in outs:
        copy.wait()


def run_qkv(tp, x_seq, cache_len, w_q, w_k, w_v, g_q, g_k):
    steps, rows, d_model = x_seq.shape
    hd = w_k.shape[1]
    width = w_q.shape[1]
    heads = width // hd
    pad = 16
    inv_freq = (ROPE_THETA ** (-(np.arange(hd // 2, dtype=np.float64) * (2.0 / hd)))).astype(np.float32)
    freq = jnp.asarray(np.concatenate([inv_freq, inv_freq])[None, :])
    return pl.pallas_call(
        functools.partial(qkv_kernel, tp, width * tp, hd * tp),
        out_shape=(jax.ShapeDtypeStruct((rows, pad, hd), BF16),
                   jax.ShapeDtypeStruct((steps, rows, hd), F32),
                   jax.ShapeDtypeStruct((steps, rows, hd), F32)),
        in_specs=[ANY_SPEC] * 8,
        out_specs=(ANY_SPEC, ANY_SPEC, ANY_SPEC),
        scratch_shapes=[
            pltpu.VMEM((1, rows), jnp.int32),
            pltpu.VMEM((1, hd), F32),
            pltpu.VMEM((heads, hd), BF16),
            pltpu.VMEM((1, hd), BF16),
            pltpu.VMEM((rows, pad, hd), BF16),
            pltpu.VMEM((steps, rows, hd), F32),
            pltpu.VMEM((steps, rows, hd), F32),
            pltpu.SemaphoreType.DMA((4,)),
            pltpu.SemaphoreType.DMA((3,)),
            pltpu.VMEM((steps * rows, d_model), BF16),
            pltpu.VMEM((d_model, width), BF16),
            pltpu.VMEM((d_model, hd), BF16),
            pltpu.VMEM((d_model, hd), BF16),
            pltpu.VMEM((steps * rows, width), F32),
            pltpu.VMEM((rows * pad, hd), F32),
            pltpu.VMEM((8, rows), F32),
            pltpu.VMEM((tp - 1, 8, rows), F32),
            pltpu.VMEM((rows, rows), F32),
            pltpu.SemaphoreType.DMA((7,)),
            pltpu.SemaphoreType.DMA((tp - 1,)),
            pltpu.SemaphoreType.DMA((tp - 1,)),
        ],
        compiler_params=pltpu.CompilerParams(collective_id=0, has_side_effects=True, vmem_limit_bytes=VMEM_LIMIT),
        name="qkv",
    )(x_seq, cache_len.reshape(1, rows), freq, w_q, w_k, w_v, g_q.reshape(heads, hd), g_k.reshape(1, hd))


SEQ_BLOCK = 8
PATCH_ROWS = 32


def attention_kernel(steps, heads, len_ref, q_hbm, kn_hbm, vn_hbm, k_hbm, v_hbm, o_hbm, k_out, v_out,
                     q_ref, kn_ref, vn_ref, o_ref, small_sem, k_buf, v_buf, mixed, in_sem, out_sem):
    rows, seq_max, hd = k_hbm.shape
    pad = q_hbm.shape[1]
    blocks = rows // SEQ_BLOCK

    def moves(blk, inward):
        sl = pl.ds(blk * SEQ_BLOCK, SEQ_BLOCK)
        if inward:
            return (pltpu.make_async_copy(k_hbm.at[sl], k_buf.at[sl], in_sem.at[0, blk]),
                    pltpu.make_async_copy(v_hbm.at[sl], v_buf.at[sl], in_sem.at[1, blk]))
        return (pltpu.make_async_copy(k_buf.at[sl], k_out.at[sl], out_sem.at[0, blk]),
                pltpu.make_async_copy(v_buf.at[sl], v_out.at[sl], out_sem.at[1, blk]))

    def start_in(blk, carry):
        for copy in moves(blk, True):
            copy.start()
        return carry

    small_in = [pltpu.make_async_copy(src, dst, small_sem.at[i]) for i, (src, dst) in enumerate(
        ((q_hbm, q_ref), (kn_hbm, kn_ref), (vn_hbm, vn_ref)))]
    o_store = pltpu.make_async_copy(o_ref, o_hbm, small_sem.at[3])
    start_in(0, 0)
    for copy in small_in:
        copy.start()
    lax.fori_loop(1, blocks, start_in, 0)
    scale = hd ** -0.5
    win_row = lax.broadcasted_iota(jnp.int32, (PATCH_ROWS, hd), 0)
    key_col = lax.broadcasted_iota(jnp.int32, (pad, seq_max), 1)
    step_row = lax.broadcasted_iota(jnp.int32, (pad, seq_max), 0) // heads
    key_off = key_col - step_row

    def body(blk, carry):
        for copy in moves(blk, True):
            copy.wait()
        lens = []
        for i in range(SEQ_BLOCK):
            b = blk * SEQ_BLOCK + i
            length = len_ref[b]
            base = pl.multiple_of(jnp.minimum((length // 16) * 16, seq_max - PATCH_ROWS), 16)
            for buf, new_ref in ((k_buf, kn_ref), (v_buf, vn_ref)):
                win = buf[b, pl.ds(base, PATCH_ROWS), :].astype(F32)
                for t in range(steps):
                    win = jnp.where(win_row == length + t - base, new_ref[t, pl.ds(b, 1), :], win)
                buf[b, pl.ds(base, PATCH_ROWS), :] = win.astype(BF16)
            lens.append(length)
        scores = []
        for i in range(SEQ_BLOCK):
            b = blk * SEQ_BLOCK + i
            s = lax.dot_general(q_ref[b], k_buf[b], (((1,), (1,)), ((), ())), preferred_element_type=F32) * scale
            scores.append(jnp.where(key_off <= lens[i], s, -jnp.inf))
        exps = []
        for i in range(SEQ_BLOCK):
            e = jnp.exp(scores[i] - jnp.max(scores[i], axis=1, keepdims=True))
            exps.append((e.astype(BF16), jnp.sum(e, axis=1, keepdims=True)))
        for i in range(SEQ_BLOCK):
            b = blk * SEQ_BLOCK + i
            out = matmul(exps[i][0], v_buf[b]) / exps[i][1]
            mixed[pl.ds(pl.multiple_of(b * pad, pad), pad), :] = out
        for copy in moves(blk, False):
            copy.start()
        return carry

    for copy in small_in:
        copy.wait()
    lax.fori_loop(0, blocks, body, 0)
    for t in range(steps):
        for g in range(heads):
            o_ref[t, :, g * hd:(g + 1) * hd] = mixed[pl.ds(t * heads + g, rows, stride=pad), :].astype(BF16)

    o_store.start()

    def finish(blk, carry):
        for copy in moves(blk, False):
            copy.wait()
        return carry

    lax.fori_loop(0, blocks, finish, 0)
    o_store.wait()


def run_attention(heads, cache_len, q_rows, k_new, v_new, k_cache, v_cache):
    rows, _, seq_max, hd = k_cache.shape
    steps = k_new.shape[0]
    pad = q_rows.shape[1]
    flat = jax.ShapeDtypeStruct((rows, seq_max, hd), BF16)
    out, k_out, v_out = pl.pallas_call(
        functools.partial(attention_kernel, steps, heads),
        out_shape=(jax.ShapeDtypeStruct((steps, rows, heads * hd), BF16), flat, flat),
        in_specs=[SMEM_SPEC] + [ANY_SPEC] * 5,
        out_specs=(ANY_SPEC, ANY_SPEC, ANY_SPEC),
        scratch_shapes=[
            pltpu.VMEM(q_rows.shape, BF16),
            pltpu.VMEM(k_new.shape, F32),
            pltpu.VMEM(v_new.shape, F32),
            pltpu.VMEM((steps, rows, heads * hd), BF16),
            pltpu.SemaphoreType.DMA((4,)),
            pltpu.VMEM((rows, seq_max, hd), BF16),
            pltpu.VMEM((rows, seq_max, hd), BF16),
            pltpu.VMEM((rows * pad, hd), F32),
            pltpu.SemaphoreType.DMA((2, rows // SEQ_BLOCK)),
            pltpu.SemaphoreType.DMA((2, rows // SEQ_BLOCK)),
        ],
        compiler_params=pltpu.CompilerParams(vmem_limit_bytes=VMEM_LIMIT),
        name="attention",
    )(cache_len, q_rows, k_new, v_new, k_cache.reshape(rows, seq_max, hd), v_cache.reshape(rows, seq_max, hd))
    return out, k_out.reshape(k_cache.shape), v_out.reshape(v_cache.shape)


QUARTERS = 4
LEFT_PIECES = tuple(range(QUARTERS // 2))
RIGHT_PIECES = tuple(range(QUARTERS // 2, QUARTERS))
PIECED = ("pair", "relay", "near", "far", "own_r", "own_l", "pass")
WHOLE = ("own_s", "sib_r", "sib_l", "sib_fr", "sib_fl")
COPIES = tuple((kind, q) for kind in PIECED for q in range(QUARTERS)) + tuple((kind, 0) for kind in WHOLE)
GATE_TILE = 256
DOWN_TILE = 512
TASKS = ("proj", "pair", "relay", "norm", "pass", "sib", "sibf", "gather", "gate", "down")
ORDER = (
    0, 1, 3, 100, 2, 101, 13, 23, 103, 10, 102, 11, 113, 12, 111, 110, 201, 200, 112, 203, 20, 22, 202, 123,
    120, 210, 213, 212, 122, 21, 211, 300, 121, 400, 402, 403, 401, 310, 501, 220, 221, 223, 500, 600, 601, 222, 700, 410,
    800, 801, 413, 411, 412, 802, 803, 511, 320, 804, 805, 806, 900, 901, 610, 510, 902, 903, 611, 904, 420, 905, 422, 150,
    906, 421, 423, 907, 710, 810, 151, 811, 812, 153, 152, 813, 814, 815, 621, 816, 620, 251, 910, 911, 912, 521, 253, 520,
    913, 250, 914, 252, 160, 915, 916, 917, 720, 820, 161, 821, 822, 163, 823, 350, 260, 162, 824, 825, 826, 920, 921, 922,
    263, 923, 924, 925, 170, 926, 171, 927, 172, 261, 173, 262, 453, 451, 270, 452, 450, 551, 550, 271, 272, 273, 360, 370,
    460, 461, 462, 463, 650, 472, 560, 470, 561, 473, 471, 651, 570, 750, 660, 571, 661, 671, 670, 760, 770,
)


def mlp_kernel(chips, x_hbm, o_hbm, wo_hbm, w1_hbm, w3_hbm, w2_hbm, ga_hbm, gm_hbm, y_out,
               o_ref, ga_ref, gm_ref, small_sem, wo, w1, w3, w2, x_own, gains, part, pair_in, relay_in, near_in, hid, act, w_sem, x_sem, y_sem, send_sem, recv_sem):
    steps, rows, d_model = x_hbm.shape
    ff = w1_hbm.shape[1]
    piece = d_model // QUARTERS
    me = lax.axis_index("tp")
    chip, core = me // 2, lax.rem(me, 2)
    nxt, prv, opp = lax.rem(chip + 1, chips), lax.rem(chip + chips - 1, chips), lax.rem(chip + 2, chips)
    right, left, sib = nxt * 2 + core, prv * 2 + core, chip * 2 + 1 - core
    n_gate, n_down = ff // GATE_TILE, d_model // DOWN_TILE

    def cols(hbm, buf, j, width, sem):
        return pltpu.make_async_copy(hbm.at[:, pl.ds(j * width, width)], buf.at[:, pl.ds(j * width, width)], w_sem.at[sem])

    wo_in = [cols(wo_hbm, wo, j, piece, j) for j in range(QUARTERS)]
    w1_in = [cols(w1_hbm, w1, j, GATE_TILE, QUARTERS + j) for j in range(n_gate)]
    w3_in = [cols(w3_hbm, w3, j, GATE_TILE, QUARTERS + n_gate + j) for j in range(n_gate)]
    w2_in = [cols(w2_hbm, w2, j, DOWN_TILE, QUARTERS + 2 * n_gate + j) for j in range(n_down)]

    def slot(c, k):
        return pl.ds(pl.multiple_of((c * 2 + k) * SLOT_ROWS, SLOT_ROWS), SLOT_ROWS)

    x_in = [pltpu.make_async_copy(x_hbm.at[t, slot(chip, core), :], x_own.at[t], x_sem.at[t]) for t in range(steps)]
    small_in = [pltpu.make_async_copy(src, dst, small_sem.at[i]) for i, (src, dst) in enumerate(
        ((o_hbm, o_ref), (ga_hbm, ga_ref), (gm_hbm, gm_ref)))]
    for copy in small_in + wo_in + x_in:
        copy.start()
    later = [copy for pair in zip(w1_in, w3_in) for copy in pair] + w2_in

    barrier = pltpu.get_barrier_semaphore()
    for other in (right, left, sib):
        pl.semaphore_signal(barrier, inc=1, device_id={"tp": other}, device_id_type=MESH)
    for copy in small_in:
        copy.wait()
    for i, ref in enumerate((ga_ref, gm_ref)):
        vals = ref[...].astype(F32)
        for j in range(vals.shape[0]):
            gains[i, :, j * vals.shape[1]:(j + 1) * vals.shape[1]] = vals[j:j + 1, :]
    pl.semaphore_wait(barrier, 3)

    def quarter(q, count=1):
        return pl.ds(q * piece, count * piece)

    def endpoints(t, kind, q):
        own, other = part.at[t, :, core], part.at[t, :, 1 - core]
        to_right = q in LEFT_PIECES
        c = quarter(q)
        if kind == "pair":
            return other.at[:, :, c], pair_in.at[t, :, :, c], sib
        if kind == "relay":
            return own.at[opp, :, c], relay_in.at[t, :, c], right if to_right else left
        if kind == "near":
            if to_right:
                return own.at[prv, :, c], near_in.at[t, 1, :, c], left
            return own.at[nxt, :, c], near_in.at[t, 0, :, c], right
        if kind == "far":
            if to_right:
                return own.at[nxt, :, c], near_in.at[t, 0, :, c], right
            return own.at[prv, :, c], near_in.at[t, 1, :, c], left
        if kind == "own_r":
            block, device = hid.at[t, slot(chip, core), c], right
        elif kind == "own_l":
            block, device = hid.at[t, slot(chip, core), c], left
        elif kind == "pass":
            block, device = (hid.at[t, slot(prv, core), c], right) if to_right else (hid.at[t, slot(nxt, core), c], left)
        elif kind == "own_s":
            block, device = hid.at[t, slot(chip, core), :], sib
        elif kind == "sib_r":
            block, device = hid.at[t, slot(prv, core), :], sib
        elif kind == "sib_l":
            block, device = hid.at[t, slot(nxt, core), :], sib
        elif kind == "sib_fr":
            block, device = hid.at[t, slot(opp, core), quarter(0, QUARTERS // 2)], sib
        else:
            block, device = hid.at[t, slot(opp, core), quarter(QUARTERS // 2, QUARTERS // 2)], sib
        return block, block, device

    def copy(ph, t, kind, q=0):
        src, dst, device = endpoints(t, kind, q)
        j = COPIES.index((kind, q))
        return pltpu.make_async_remote_copy(
            src_ref=src, dst_ref=dst, send_sem=send_sem.at[ph, t, j], recv_sem=recv_sem.at[ph, t, j],
            device_id={"tp": device}, device_id_type=MESH)

    def sent(ph, t):
        for kind, q in COPIES:
            copy(ph, t, kind, q).wait_send()

    def proj(ph, t, q):
        if t == 0:
            wo_in[q].wait()
        for n in range(q * piece, (q + 1) * piece, DOWN_TILE):
            val = matmul(o_ref[t], wo[:, n:n + DOWN_TILE]).astype(BF16)
            part[t, :, :, :, n:n + DOWN_TILE] = val.reshape(chips, 2, SLOT_ROWS, DOWN_TILE)
        copy(0, t, "pair", q).start()

    def pair_add(ph, t, q):
        copy(ph, t, "pair", q).wait_recv()
        c = slice(q * piece, (q + 1) * piece)
        for n in (opp, prv, nxt, chip):
            part[t, n, core, :, c] = (part[t, n, core, :, c].astype(F32) + pair_in[t, n, :, c].astype(F32)).astype(BF16)
        copy(ph, t, "relay", q).start()
        copy(ph, t, "near", q).start()

    def relay_add(ph, t, q):
        copy(ph, t, "relay", q).wait_recv()
        c = slice(q * piece, (q + 1) * piece)
        n = nxt if q in LEFT_PIECES else prv
        part[t, n, core, :, c] = (part[t, n, core, :, c].astype(F32) + relay_in[t, :, c].astype(F32)).astype(BF16)
        copy(ph, t, "far", q).start()

    def norm(ph, t, _):
        for q in range(QUARTERS):
            copy(ph, t, "near", q).wait_recv()
            copy(ph, t, "far", q).wait_recv()
        total = part[t, chip, core].astype(F32) + near_in[t, 0].astype(F32) + near_in[t, 1].astype(F32)
        total = total.astype(BF16).astype(F32)
        fac = lax.rsqrt(jnp.sum(total * total, axis=1, keepdims=True) / d_model + NORM_EPS)
        if ph == 0:
            x_in[t].wait()
            base = x_own[t]
        else:
            base = hid[t, slot(chip, core), :]
        hid[t, slot(chip, core), :] = (base.astype(F32) + total * fac * gains[ph]).astype(BF16)
        for first, second in ((LEFT_PIECES, RIGHT_PIECES), (RIGHT_PIECES, LEFT_PIECES)):
            for i, j in zip(first, second):
                copy(ph, t, "own_r", i).start()
                copy(ph, t, "own_l", j).start()
        copy(ph, t, "own_s").start()

    def pass_on(ph, t, q):
        copy(ph, t, "own_r" if q in LEFT_PIECES else "own_l", q).wait_recv()
        copy(ph, t, "pass", q).start()

    def pass_sib(ph, t, side):
        for q in (RIGHT_PIECES, LEFT_PIECES)[side]:
            copy(ph, t, ("own_r", "own_l")[side], q).wait_recv()
        copy(ph, t, ("sib_r", "sib_l")[side]).start()

    def far_sib(ph, t, side):
        for q in (LEFT_PIECES, RIGHT_PIECES)[side]:
            copy(ph, t, "pass", q).wait_recv()
        copy(ph, t, ("sib_fr", "sib_fl")[side]).start()

    def gather(ph, t, _):
        for kind in WHOLE:
            copy(ph, t, kind).wait_recv()
        if ph == 1:
            pltpu.make_async_copy(hid.at[t], y_out.at[t], y_sem.at[t]).start()

    def gate_up(ph, t, j):
        if t == 0:
            w1_in[j].wait()
            w3_in[j].wait()
        sl = slice(j * GATE_TILE, (j + 1) * GATE_TILE)
        gate = matmul(hid[t], w1[:, sl])
        up = matmul(hid[t], w3[:, sl])
        act[:, sl] = (gate / (1.0 + jnp.exp(-gate)) * up).astype(BF16)

    def down(ph, t, j):
        if j == 0:
            sent(0, t)
        if t == 0:
            w2_in[j].wait()
        sl = slice(j * DOWN_TILE, (j + 1) * DOWN_TILE)
        val = matmul(act[...], w2[:, sl]).astype(BF16)
        part[t, :, :, :, sl] = val.reshape(chips, 2, SLOT_ROWS, DOWN_TILE)
        if (j + 1) * DOWN_TILE % piece == 0:
            copy(1, t, "pair", (j + 1) * DOWN_TILE // piece - 1).start()

    run = (proj, pair_add, relay_add, norm, pass_on, pass_sib, far_sib, gather, gate_up, down)
    gates_from = TASKS.index("gate") * 100
    for code in ORDER:
        while later and code >= gates_from and (len(later) > n_down or later[0] is w2_in[0]):
            later.pop(0).start()
        run[code // 100](code // 50 % 2, code % 50 // 10, code % 10)
        if later:
            later.pop(0).start()
    for t in range(steps):
        sent(1, t)
        pltpu.make_async_copy(hid.at[t], y_out.at[t], y_sem.at[t]).wait()


def run_mlp(tp, x_seq, attn, w_o, w_gate, w_up, w_down, g_attn, g_mlp):
    steps, rows, d_model = x_seq.shape
    ff = w_gate.shape[1]
    chips = tp // 2
    n_sem = QUARTERS + 2 * (ff // GATE_TILE) + d_model // DOWN_TILE
    return pl.pallas_call(
        functools.partial(mlp_kernel, chips),
        out_shape=jax.ShapeDtypeStruct((steps, rows, d_model), BF16),
        in_specs=[ANY_SPEC] * 8,
        out_specs=ANY_SPEC,
        scratch_shapes=[
            pltpu.VMEM(attn.shape, BF16),
            pltpu.VMEM((d_model // 128, 128), BF16),
            pltpu.VMEM((d_model // 128, 128), BF16),
            pltpu.SemaphoreType.DMA((3,)),
            pltpu.VMEM(w_o.shape, BF16),
            pltpu.VMEM(w_gate.shape, BF16),
            pltpu.VMEM(w_up.shape, BF16),
            pltpu.VMEM(w_down.shape, BF16),
            pltpu.VMEM((steps, SLOT_ROWS, d_model), BF16),
            pltpu.VMEM((2, 1, d_model), F32),
            pltpu.VMEM((steps, chips, 2, SLOT_ROWS, d_model), BF16),
            pltpu.VMEM((steps, chips, SLOT_ROWS, d_model), BF16),
            pltpu.VMEM((steps, SLOT_ROWS, d_model), BF16),
            pltpu.VMEM((steps, 2, SLOT_ROWS, d_model), BF16),
            pltpu.VMEM((steps, rows, d_model), BF16),
            pltpu.VMEM((rows, ff), BF16),
            pltpu.SemaphoreType.DMA((n_sem,)),
            pltpu.SemaphoreType.DMA((steps,)),
            pltpu.SemaphoreType.DMA((steps,)),
            pltpu.SemaphoreType.DMA((2, steps, len(COPIES))),
            pltpu.SemaphoreType.DMA((2, steps, len(COPIES))),
        ],
        compiler_params=pltpu.CompilerParams(collective_id=1, has_side_effects=True, vmem_limit_bytes=VMEM_LIMIT),
        name="mlp",
    )(x_seq, attn, w_o, w_gate, w_up, w_down, g_attn.reshape(-1, 128), g_mlp.reshape(-1, 128))


COPY_ROWS = 64


def store_kernel(src, dst, buf, in_sem, out_sem):
    rows = src.shape[0]
    n = rows // COPY_ROWS
    sl = [pl.ds(i * COPY_ROWS, COPY_ROWS) for i in range(n)]
    ins = [pltpu.make_async_copy(src.at[sl[i]], buf.at[sl[i]], in_sem.at[i]) for i in range(n)]
    outs = [pltpu.make_async_copy(buf.at[sl[i]], dst.at[sl[i]], out_sem.at[i]) for i in range(n)]
    for i in range(n):
        ins[i].start()
    for i in range(n):
        ins[i].wait()
        outs[i].start()
    for i in range(n):
        outs[i].wait()


def run_store(y_seq):
    steps, rows, d_model = y_seq.shape
    total = steps * rows
    return pl.pallas_call(
        store_kernel,
        out_shape=jax.ShapeDtypeStruct((total, d_model), BF16),
        in_specs=[ANY_SPEC],
        out_specs=ANY_SPEC,
        scratch_shapes=[
            pltpu.VMEM((total, d_model), BF16),
            pltpu.SemaphoreType.DMA((total // COPY_ROWS,)),
            pltpu.SemaphoreType.DMA((total // COPY_ROWS,)),
        ],
        compiler_params=pltpu.CompilerParams(vmem_limit_bytes=VMEM_LIMIT),
        name="store",
    )(y_seq.reshape(total, d_model)).reshape(y_seq.shape)


def solution(mesh):
    tp = mesh.shape['tp']

    def local_run(x_seq, cache_len, k_cache, v_cache, w_q, w_k, w_v, w_o, w_gate, w_up, w_down, g_q, g_k, g_attn, g_mlp):
        heads = w_q.shape[1] // w_k.shape[1]
        q_rows, k_new, v_new = run_qkv(tp, x_seq, cache_len, w_q, w_k, w_v, g_q, g_k)
        attn, k_out, v_out = run_attention(heads, cache_len, q_rows, k_new, v_new, k_cache, v_cache)
        y_seq = run_mlp(tp, x_seq, attn, w_o, w_gate, w_up, w_down, g_attn, g_mlp)
        return run_store(y_seq), k_out, v_out

    data_spec = P(None, 'dp', None)
    cache_spec = P('dp', 'tp', None, None)
    col_spec = P(None, 'tp')
    row_spec = P('tp', None)
    arg_specs = (data_spec, P('dp'), cache_spec, cache_spec, col_spec, col_spec, col_spec, row_spec, col_spec, col_spec, row_spec, P('tp'), P('tp'), P(None), P(None))
    out_specs = (data_spec, cache_spec, cache_spec)
    return jax.shard_map(local_run, mesh=mesh, in_specs=arg_specs, out_specs=out_specs, check_vma=False)
```

```python
import functools

import jax
import jax.numpy as jnp
import numpy as np
from jax import lax
from jax.experimental import pallas as pl
from jax.experimental.pallas import tpu as pltpu
from jax.sharding import PartitionSpec as P

ROPE_THETA = 500000.0
NORM_EPS = 1e-6
F32 = jnp.float32
BF16 = jnp.bfloat16
MESH = pl.DeviceIdType.MESH
VMEM_SPEC = pl.BlockSpec(memory_space=pltpu.VMEM)
ANY_SPEC = pl.BlockSpec(memory_space=pl.ANY)
SMEM_SPEC = pl.BlockSpec(memory_space=pltpu.SMEM)
QKV_VMEM = 40 * 1024 * 1024
ATTENTION_VMEM = 24 * 1024 * 1024
MLP_VMEM = 54 * 1024 * 1024
SLOT_ROWS = 16


def in_vmem(val):
    return pltpu.with_memory_space_constraint(val, pltpu.VMEM)


def matmul(lhs, rhs):
    return jnp.dot(lhs, rhs, preferred_element_type=F32)


CACHE_PARTS = 4


def qkv_kernel(tp, q_width, kv_width, x_hbm, len_hbm, freq_hbm, wq_hbm, wk_hbm, wv_hbm, gq_hbm, gk_hbm, kc_hbm, vc_hbm,
               q_out, kn_out, vn_out, kc_out, vc_out,
               len_ref, freq_ref, gq_ref, gk_ref, small_sem, cache_sem, x_buf, wq_buf, wk_buf, wv_buf, q_raw, q_rows, part, inbox, turn, in_sem, send_sem, recv_sem):
    steps, rows, _ = x_hbm.shape
    hd = wk_hbm.shape[1]
    heads = wq_hbm.shape[1] // hd
    pad = q_out.shape[1]
    me = lax.axis_index("tp")
    x_in = [pltpu.make_async_copy(x_hbm.at[t], x_buf.at[pl.ds(t * rows, rows), :], in_sem.at[t]) for t in range(steps)]
    for copy in x_in:
        copy.start()
    half = heads * hd // 2
    wk_in = pltpu.make_async_copy(wk_hbm, wk_buf, in_sem.at[3])
    wq_in = [pltpu.make_async_copy(wq_hbm.at[:, pl.ds(j * half, half)], wq_buf.at[:, pl.ds(j * half, half)], in_sem.at[4 + j]) for j in range(2)]
    wv_in = pltpu.make_async_copy(wv_hbm, wv_buf, in_sem.at[6])
    small_in = [pltpu.make_async_copy(src, dst, small_sem.at[i]) for i, (src, dst) in enumerate(
        ((len_hbm, len_ref), (freq_hbm, freq_ref), (gq_hbm, gq_ref), (gk_hbm, gk_ref)))]
    seqs = rows // CACHE_PARTS
    cache_in = [pltpu.make_async_copy(src.at[pl.ds(i * seqs, seqs)], dst.at[pl.ds(i * seqs, seqs)], cache_sem.at[c, i])
                for i in range(CACHE_PARTS) for c, (src, dst) in enumerate(((kc_hbm, kc_out), (vc_hbm, vc_out)))]
    for copy in small_in + [wk_in, wq_in[0], wq_in[1], wv_in]:
        copy.start()

    barrier = pltpu.get_barrier_semaphore()
    for j in range(1, tp):
        pl.semaphore_signal(barrier, inc=1, device_id={"tp": lax.rem(me + j, tp)}, device_id_type=MESH)

    for copy in small_in:
        copy.wait()
    lens = jnp.transpose(jnp.broadcast_to(len_ref[...].astype(F32), (rows, rows)))[:, :hd]
    lane = lax.broadcasted_iota(jnp.int32, (rows, hd), 1)
    sign = jnp.where(lane < hd // 2, -1.0, 1.0).astype(F32)
    tables = []
    for t in range(steps):
        angle = (lens + float(t)) * freq_ref[...]
        tables.append((jnp.cos(angle), jnp.sin(angle) * sign))

    q_rows[...] = jnp.zeros_like(q_rows)
    for copy in x_in:
        copy.wait()
    wk_in.wait()
    k_raw = matmul(x_buf[...], wk_buf[...]).astype(BF16).astype(F32)
    k_sq = jnp.sum(k_raw * k_raw, axis=1, keepdims=True)
    q_sq = None
    for j in range(2):
        wq_in[j].wait()
        if j == 1:
            cache_in[0].start()
        val = matmul(x_buf[...], wq_buf[:, j * half:(j + 1) * half]).astype(BF16).astype(F32)
        q_raw[:, j * half:(j + 1) * half] = val
        sq = jnp.sum(val * val, axis=1, keepdims=True)
        q_sq = sq if q_sq is None else q_sq + sq
    packed = jnp.zeros((rows, rows), F32)
    col = lax.broadcasted_iota(jnp.int32, (rows, rows), 1)
    for t in range(steps):
        packed = jnp.where(col == t, q_sq[t * rows:(t + 1) * rows], packed)
        packed = jnp.where(col == steps + t, k_sq[t * rows:(t + 1) * rows], packed)
    part[...] = jnp.transpose(packed)[:part.shape[0]]
    pl.semaphore_wait(barrier, tp - 1)
    copies = []
    for j in range(1, tp):
        copy = pltpu.make_async_remote_copy(
            src_ref=part, dst_ref=inbox.at[j - 1], send_sem=send_sem.at[j - 1], recv_sem=recv_sem.at[j - 1],
            device_id={"tp": lax.rem(me + j, tp)}, device_id_type=MESH)
        copy.start()
        copies.append(copy)
    for copy in cache_in[1:]:
        copy.start()
    wv_in.wait()
    vn_out[...] = matmul(x_buf[...], wv_buf[...]).astype(BF16).astype(F32).reshape(steps, rows, hd)
    total = part[...]
    for j in range(1, tp):
        copies[j - 1].wait()
        total = total + inbox[j - 1]
    turn[...] = jnp.zeros_like(turn)
    turn[0:part.shape[0], :] = total
    sums = jnp.transpose(turn[...])
    gain_k = gk_ref[...].astype(F32)
    gain_q = gq_ref[...].astype(F32)
    for t in range(steps):
        cos_tab, sin_tab = tables[t]
        q_fac = lax.rsqrt(sums[:, t:t + 1] / q_width + NORM_EPS)
        k_fac = lax.rsqrt(sums[:, steps + t:steps + t + 1] / kv_width + NORM_EPS)
        val = k_raw[t * rows:(t + 1) * rows] * k_fac * gain_k
        val = val * cos_tab + pltpu.roll(val, hd // 2, axis=1) * sin_tab
        kn_out[t] = val.astype(BF16).astype(F32)
        for g in range(heads):
            val = q_raw[t * rows:(t + 1) * rows, g * hd:(g + 1) * hd] * q_fac * gain_q[g:g + 1, :]
            val = val * cos_tab + pltpu.roll(val, hd // 2, axis=1) * sin_tab
            q_rows[pl.ds(t * heads + g, rows, stride=pad), :] = val
    q_out[...] = q_rows[...].reshape(rows, pad, hd).astype(BF16)
    for copy in cache_in:
        copy.wait()


def run_qkv(tp, x_seq, cache_len, w_q, w_k, w_v, g_q, g_k, k_cache, v_cache):
    steps, rows, d_model = x_seq.shape
    hd = w_k.shape[1]
    width = w_q.shape[1]
    heads = width // hd
    pad = 16
    inv_freq = (ROPE_THETA ** (-(np.arange(hd // 2, dtype=np.float64) * (2.0 / hd)))).astype(np.float32)
    freq = jnp.asarray(np.concatenate([inv_freq, inv_freq])[None, :])
    return pl.pallas_call(
        functools.partial(qkv_kernel, tp, width * tp, hd * tp),
        out_shape=(pltpu.VMEM((rows, pad, hd), BF16),
                   pltpu.VMEM((steps, rows, hd), F32),
                   pltpu.VMEM((steps, rows, hd), F32),
                   pltpu.VMEM(k_cache.shape, BF16),
                   pltpu.VMEM(v_cache.shape, BF16)),
        in_specs=[ANY_SPEC] * 10,
        out_specs=(VMEM_SPEC,) * 5,
        scratch_shapes=[
            pltpu.VMEM((1, rows), jnp.int32),
            pltpu.VMEM((1, hd), F32),
            pltpu.VMEM((heads, hd), BF16),
            pltpu.VMEM((1, hd), BF16),
            pltpu.SemaphoreType.DMA((4,)),
            pltpu.SemaphoreType.DMA((2, CACHE_PARTS)),
            pltpu.VMEM((steps * rows, d_model), BF16),
            pltpu.VMEM((d_model, width), BF16),
            pltpu.VMEM((d_model, hd), BF16),
            pltpu.VMEM((d_model, hd), BF16),
            pltpu.VMEM((steps * rows, width), F32),
            pltpu.VMEM((rows * pad, hd), F32),
            pltpu.VMEM((8, rows), F32),
            pltpu.VMEM((tp - 1, 8, rows), F32),
            pltpu.VMEM((rows, rows), F32),
            pltpu.SemaphoreType.DMA((7,)),
            pltpu.SemaphoreType.DMA((tp - 1,)),
            pltpu.SemaphoreType.DMA((tp - 1,)),
        ],
        compiler_params=pltpu.CompilerParams(collective_id=0, has_side_effects=True, vmem_limit_bytes=QKV_VMEM),
        name="qkv",
    )(x_seq, cache_len.reshape(1, rows), freq, w_q, w_k, w_v, g_q.reshape(heads, hd), g_k.reshape(1, hd), k_cache, v_cache)


SEQ_BLOCK = 8
PATCH_ROWS = 32


def attention_kernel(steps, heads, len_ref, q_ref, kn_ref, vn_ref, k_in, v_in, wo_hbm, k_out, v_out, k_buf, v_buf, part,
                     o_ref, wo, mixed, wo_sem, out_sem):
    rows, seq_max, hd = k_buf.shape
    pad = q_ref.shape[1]
    blocks = rows // SEQ_BLOCK
    d_model = wo.shape[1]
    wo_in = pltpu.make_async_copy(wo_hbm, wo, wo_sem)
    wo_in.start()

    def moves(blk):
        sl = pl.ds(blk * SEQ_BLOCK, SEQ_BLOCK)
        return (pltpu.make_async_copy(k_buf.at[sl], k_out.at[sl], out_sem.at[0, blk]),
                pltpu.make_async_copy(v_buf.at[sl], v_out.at[sl], out_sem.at[1, blk]))

    scale = hd ** -0.5
    win_row = lax.broadcasted_iota(jnp.int32, (PATCH_ROWS, hd), 0)
    key_col = lax.broadcasted_iota(jnp.int32, (pad, seq_max), 1)
    step_row = lax.broadcasted_iota(jnp.int32, (pad, seq_max), 0) // heads
    key_off = key_col - step_row

    def body(blk, carry):
        lens = []
        for i in range(SEQ_BLOCK):
            b = blk * SEQ_BLOCK + i
            length = len_ref[b]
            base = pl.multiple_of(jnp.minimum((length // 16) * 16, seq_max - PATCH_ROWS), 16)
            for buf, new_ref in ((k_buf, kn_ref), (v_buf, vn_ref)):
                win = buf[b, pl.ds(base, PATCH_ROWS), :].astype(F32)
                for t in range(steps):
                    win = jnp.where(win_row == length + t - base, new_ref[t, pl.ds(b, 1), :], win)
                buf[b, pl.ds(base, PATCH_ROWS), :] = win.astype(BF16)
            lens.append(length)
        scores = []
        for i in range(SEQ_BLOCK):
            b = blk * SEQ_BLOCK + i
            s = lax.dot_general(q_ref[b], k_buf[b], (((1,), (1,)), ((), ())), preferred_element_type=F32) * scale
            scores.append(jnp.where(key_off <= lens[i], s, -jnp.inf))
        exps = []
        for i in range(SEQ_BLOCK):
            e = jnp.exp(scores[i] - jnp.max(scores[i], axis=1, keepdims=True))
            exps.append((e.astype(BF16), jnp.sum(e, axis=1, keepdims=True)))
        for i in range(SEQ_BLOCK):
            b = blk * SEQ_BLOCK + i
            out = matmul(exps[i][0], v_buf[b]) / exps[i][1]
            mixed[pl.ds(pl.multiple_of(b * pad, pad), pad), :] = out
        for copy in moves(blk):
            copy.start()
        return carry

    lax.fori_loop(0, blocks, body, 0)
    for t in range(steps):
        for g in range(heads):
            o_ref[t * rows:(t + 1) * rows, g * hd:(g + 1) * hd] = mixed[pl.ds(t * heads + g, rows, stride=pad), :].astype(BF16)

    wo_in.wait()
    for n in range(0, d_model, DOWN_TILE):
        val = matmul(o_ref[...], wo[:, n:n + DOWN_TILE]).astype(BF16)
        part[:, :, :, :, n:n + DOWN_TILE] = val.reshape(part.shape[:4] + (DOWN_TILE,))

    def finish(blk, carry):
        for copy in moves(blk):
            copy.wait()
        return carry

    lax.fori_loop(0, blocks, finish, 0)


def run_attention(tp, heads, cache_len, q_rows, k_new, v_new, k_cache, v_cache, w_o):
    rows, seq_max, hd = k_cache.shape
    steps = k_new.shape[0]
    pad = q_rows.shape[1]
    flat = jax.ShapeDtypeStruct(k_cache.shape, BF16)
    held = pltpu.VMEM(k_cache.shape, BF16)
    part = pltpu.VMEM((steps, tp // 2, 2, rows // tp, w_o.shape[1]), BF16)
    k_out, v_out, _, _, part = pl.pallas_call(
        functools.partial(attention_kernel, steps, heads),
        out_shape=(flat, flat, held, held, part),
        in_specs=[SMEM_SPEC] + [VMEM_SPEC] * 5 + [ANY_SPEC],
        out_specs=(ANY_SPEC, ANY_SPEC, VMEM_SPEC, VMEM_SPEC, VMEM_SPEC),
        input_output_aliases={4: 2, 5: 3},
        scratch_shapes=[
            pltpu.VMEM((steps * rows, heads * hd), BF16),
            pltpu.VMEM(w_o.shape, BF16),
            pltpu.VMEM((rows * pad, hd), F32),
            pltpu.SemaphoreType.DMA,
            pltpu.SemaphoreType.DMA((2, rows // SEQ_BLOCK)),
        ],
        compiler_params=pltpu.CompilerParams(vmem_limit_bytes=ATTENTION_VMEM),
        name="attention",
    )(cache_len, in_vmem(q_rows), in_vmem(k_new), in_vmem(v_new), in_vmem(k_cache), in_vmem(v_cache), w_o)
    return part, k_out, v_out


QUARTERS = 4
LEFT_PIECES = tuple(range(QUARTERS // 2))
RIGHT_PIECES = tuple(range(QUARTERS // 2, QUARTERS))
PIECED = ("pair", "relay", "near", "far", "own_r", "own_l", "pass")
WHOLE = ("own_s", "sib_r", "sib_l", "sib_fr", "sib_fl")
COPIES = tuple((kind, q) for kind in PIECED for q in range(QUARTERS)) + tuple((kind, 0) for kind in WHOLE)
GATE_TILE = 256
FETCHES = 1
DOWN_TILE = 512
TASKS = ("send", "pair", "relay", "norm", "pass", "sib", "sibf", "gather", "gate", "down", "fetch")
ORDER = (
    0, 1000, 1, 1001, 3, 1010, 100, 1011, 2, 1020, 101, 1021, 13, 1030, 23, 1031, 103, 1040, 10, 1041, 102, 1050, 11, 1051,
    113, 1060, 12, 1061, 111, 1100, 110, 1110, 201, 1120, 200, 1130, 112, 1140, 203, 1150, 20, 1160, 22, 1170, 202, 123, 120, 210,
    213, 212, 122, 21, 211, 300, 121, 400, 402, 403, 401, 310, 501, 220, 221, 223, 500, 600, 601, 222, 700, 410, 800, 801,
    413, 411, 412, 802, 803, 511, 320, 804, 805, 806, 900, 901, 610, 510, 902, 903, 611, 904, 420, 905, 422, 150, 906, 421,
    423, 907, 710, 810, 151, 811, 812, 153, 152, 813, 814, 815, 621, 816, 620, 251, 910, 911, 912, 521, 253, 520, 913, 250,
    914, 252, 160, 915, 916, 917, 720, 820, 161, 821, 822, 163, 823, 350, 260, 162, 824, 825, 826, 920, 921, 922, 263, 923,
    924, 925, 170, 926, 171, 927, 172, 261, 173, 262, 453, 451, 270, 452, 450, 551, 550, 271, 272, 273, 360, 370, 460, 461,
    462, 463, 650, 472, 560, 470, 561, 473, 471, 651, 570, 750, 660, 571, 661, 671, 670, 760, 770,
)


def mlp_kernel(chips, x_hbm, part_in, w1_hbm, w3_hbm, w2_hbm, ga_hbm, gm_hbm, hid, part,
               ga_ref, gm_ref, small_sem, w1, w3, w2, x_own, gains, pair_in, relay_in, near_in, act, w_sem, x_sem, send_sem, recv_sem):
    steps, rows, d_model = x_hbm.shape
    ff = w1_hbm.shape[1]
    piece = d_model // QUARTERS
    me = lax.axis_index("tp")
    chip, core = me // 2, lax.rem(me, 2)
    nxt, prv, opp = lax.rem(chip + 1, chips), lax.rem(chip + chips - 1, chips), lax.rem(chip + 2, chips)
    right, left, sib = nxt * 2 + core, prv * 2 + core, chip * 2 + 1 - core
    n_gate, n_down = ff // GATE_TILE, d_model // DOWN_TILE

    def fetches(hbm, buf, width, sem):
        depth = hbm.shape[0] // FETCHES
        return [[pltpu.make_async_copy(hbm.at[pl.ds(i * depth, depth), pl.ds(j * width, width)],
                                       buf.at[pl.ds(i * depth, depth), pl.ds(j * width, width)], w_sem.at[sem + j * FETCHES + i])
                 for i in range(FETCHES)] for j in range(hbm.shape[1] // width)]

    w1_in = fetches(w1_hbm, w1, GATE_TILE, 0)
    w3_in = fetches(w3_hbm, w3, GATE_TILE, n_gate * FETCHES)
    gate_in = [a + b for a, b in zip(w1_in, w3_in)]
    down_in = fetches(w2_hbm, w2, DOWN_TILE, 2 * n_gate * FETCHES)

    def slot(c, k):
        return pl.ds(pl.multiple_of((c * 2 + k) * SLOT_ROWS, SLOT_ROWS), SLOT_ROWS)

    x_in = [pltpu.make_async_copy(x_hbm.at[t, slot(chip, core), :], x_own.at[t], x_sem.at[t]) for t in range(steps)]
    small_in = [pltpu.make_async_copy(src, dst, small_sem.at[i]) for i, (src, dst) in enumerate(
        ((ga_hbm, ga_ref), (gm_hbm, gm_ref)))]
    for copy in small_in + x_in:
        copy.start()
    barrier = pltpu.get_barrier_semaphore()
    for other in (right, left, sib):
        pl.semaphore_signal(barrier, inc=1, device_id={"tp": other}, device_id_type=MESH)
    for copy in small_in:
        copy.wait()
    for i, ref in enumerate((ga_ref, gm_ref)):
        vals = ref[...].astype(F32)
        for j in range(vals.shape[0]):
            gains[i, :, j * vals.shape[1]:(j + 1) * vals.shape[1]] = vals[j:j + 1, :]
    pl.semaphore_wait(barrier, 3)

    def quarter(q, count=1):
        return pl.ds(q * piece, count * piece)

    def endpoints(t, kind, q):
        own, other = part.at[t, :, core], part.at[t, :, 1 - core]
        to_right = q in LEFT_PIECES
        c = quarter(q)
        if kind == "pair":
            return other.at[:, :, c], pair_in.at[t, :, :, c], sib
        if kind == "relay":
            return own.at[opp, :, c], relay_in.at[t, :, c], right if to_right else left
        if kind == "near":
            if to_right:
                return own.at[prv, :, c], near_in.at[t, 1, :, c], left
            return own.at[nxt, :, c], near_in.at[t, 0, :, c], right
        if kind == "far":
            if to_right:
                return own.at[nxt, :, c], near_in.at[t, 0, :, c], right
            return own.at[prv, :, c], near_in.at[t, 1, :, c], left
        if kind == "own_r":
            block, device = hid.at[t, slot(chip, core), c], right
        elif kind == "own_l":
            block, device = hid.at[t, slot(chip, core), c], left
        elif kind == "pass":
            block, device = (hid.at[t, slot(prv, core), c], right) if to_right else (hid.at[t, slot(nxt, core), c], left)
        elif kind == "own_s":
            block, device = hid.at[t, slot(chip, core), :], sib
        elif kind == "sib_r":
            block, device = hid.at[t, slot(prv, core), :], sib
        elif kind == "sib_l":
            block, device = hid.at[t, slot(nxt, core), :], sib
        elif kind == "sib_fr":
            block, device = hid.at[t, slot(opp, core), quarter(0, QUARTERS // 2)], sib
        else:
            block, device = hid.at[t, slot(opp, core), quarter(QUARTERS // 2, QUARTERS // 2)], sib
        return block, block, device

    def copy(ph, t, kind, q=0):
        src, dst, device = endpoints(t, kind, q)
        j = COPIES.index((kind, q))
        return pltpu.make_async_remote_copy(
            src_ref=src, dst_ref=dst, send_sem=send_sem.at[ph, t, j], recv_sem=recv_sem.at[ph, t, j],
            device_id={"tp": device}, device_id_type=MESH)

    def sent(ph, t):
        for kind, q in COPIES:
            copy(ph, t, kind, q).wait_send()

    def pair_send(ph, t, q):
        copy(0, t, "pair", q).start()

    def pair_add(ph, t, q):
        copy(ph, t, "pair", q).wait_recv()
        c = slice(q * piece, (q + 1) * piece)
        for n in (opp, prv, nxt, chip):
            part[t, n, core, :, c] = (part[t, n, core, :, c].astype(F32) + pair_in[t, n, :, c].astype(F32)).astype(BF16)
        copy(ph, t, "relay", q).start()
        copy(ph, t, "near", q).start()

    def relay_add(ph, t, q):
        copy(ph, t, "relay", q).wait_recv()
        c = slice(q * piece, (q + 1) * piece)
        n = nxt if q in LEFT_PIECES else prv
        part[t, n, core, :, c] = (part[t, n, core, :, c].astype(F32) + relay_in[t, :, c].astype(F32)).astype(BF16)
        copy(ph, t, "far", q).start()

    def norm(ph, t, _):
        for q in range(QUARTERS):
            copy(ph, t, "near", q).wait_recv()
            copy(ph, t, "far", q).wait_recv()
        total = part[t, chip, core].astype(F32) + near_in[t, 0].astype(F32) + near_in[t, 1].astype(F32)
        total = total.astype(BF16).astype(F32)
        fac = lax.rsqrt(jnp.sum(total * total, axis=1, keepdims=True) / d_model + NORM_EPS)
        if ph == 0:
            x_in[t].wait()
            base = x_own[t]
        else:
            base = hid[t, slot(chip, core), :]
        hid[t, slot(chip, core), :] = (base.astype(F32) + total * fac * gains[ph]).astype(BF16)
        for first, second in ((LEFT_PIECES, RIGHT_PIECES), (RIGHT_PIECES, LEFT_PIECES)):
            for i, j in zip(first, second):
                copy(ph, t, "own_r", i).start()
                copy(ph, t, "own_l", j).start()
        copy(ph, t, "own_s").start()

    def pass_on(ph, t, q):
        copy(ph, t, "own_r" if q in LEFT_PIECES else "own_l", q).wait_recv()
        copy(ph, t, "pass", q).start()

    def pass_sib(ph, t, side):
        for q in (RIGHT_PIECES, LEFT_PIECES)[side]:
            copy(ph, t, ("own_r", "own_l")[side], q).wait_recv()
        copy(ph, t, ("sib_r", "sib_l")[side]).start()

    def far_sib(ph, t, side):
        for q in (LEFT_PIECES, RIGHT_PIECES)[side]:
            copy(ph, t, "pass", q).wait_recv()
        copy(ph, t, ("sib_fr", "sib_fl")[side]).start()

    def gather(ph, t, _):
        for kind in WHOLE:
            copy(ph, t, kind).wait_recv()

    def gate_up(ph, t, j):
        if t == 0:
            for fetch in gate_in[j]:
                fetch.wait()
        sl = slice(j * GATE_TILE, (j + 1) * GATE_TILE)
        gate = matmul(hid[t], w1[:, sl])
        up = matmul(hid[t], w3[:, sl])
        act[:, sl] = (gate / (1.0 + jnp.exp(-gate)) * up).astype(BF16)

    def down(ph, t, j):
        if j == 0:
            sent(0, t)
        if t == 0:
            for fetch in down_in[j]:
                fetch.wait()
        sl = slice(j * DOWN_TILE, (j + 1) * DOWN_TILE)
        val = matmul(act[...], w2[:, sl]).astype(BF16)
        part[t, :, :, :, sl] = val.reshape(chips, 2, SLOT_ROWS, DOWN_TILE)
        if (j + 1) * DOWN_TILE % piece == 0:
            copy(1, t, "pair", (j + 1) * DOWN_TILE // piece - 1).start()

    run = (pair_send, pair_add, relay_add, norm, pass_on, pass_sib, far_sib, gather, gate_up, down)
    for code in ORDER:
        if code >= 1000:
            (gate_in, down_in)[code // 100 % 10][code // 10 % 10][code % 10].start()
        else:
            run[code // 100](code // 50 % 2, code % 50 // 10, code % 10)
    for t in range(steps):
        sent(1, t)


def run_mlp(tp, x_seq, part, w_gate, w_up, w_down, g_attn, g_mlp):
    steps, rows, d_model = x_seq.shape
    ff = w_gate.shape[1]
    chips = tp // 2
    n_sem = (2 * (ff // GATE_TILE) + d_model // DOWN_TILE) * FETCHES
    hid, _ = pl.pallas_call(
        functools.partial(mlp_kernel, chips),
        out_shape=(pltpu.VMEM((steps, rows, d_model), BF16), pltpu.VMEM(part.shape, BF16)),
        in_specs=[ANY_SPEC, VMEM_SPEC] + [ANY_SPEC] * 5,
        out_specs=(VMEM_SPEC, VMEM_SPEC),
        input_output_aliases={1: 1},
        scratch_shapes=[
            pltpu.VMEM((d_model // 128, 128), BF16),
            pltpu.VMEM((d_model // 128, 128), BF16),
            pltpu.SemaphoreType.DMA((2,)),
            pltpu.VMEM(w_gate.shape, BF16),
            pltpu.VMEM(w_up.shape, BF16),
            pltpu.VMEM(w_down.shape, BF16),
            pltpu.VMEM((steps, SLOT_ROWS, d_model), BF16),
            pltpu.VMEM((2, 1, d_model), F32),
            pltpu.VMEM((steps, chips, SLOT_ROWS, d_model), BF16),
            pltpu.VMEM((steps, SLOT_ROWS, d_model), BF16),
            pltpu.VMEM((steps, 2, SLOT_ROWS, d_model), BF16),
            pltpu.VMEM((rows, ff), BF16),
            pltpu.SemaphoreType.DMA((n_sem,)),
            pltpu.SemaphoreType.DMA((steps,)),
            pltpu.SemaphoreType.DMA((2, steps, len(COPIES))),
            pltpu.SemaphoreType.DMA((2, steps, len(COPIES))),
        ],
        compiler_params=pltpu.CompilerParams(collective_id=1, has_side_effects=True, vmem_limit_bytes=MLP_VMEM),
        name="mlp",
    )(x_seq, in_vmem(part), w_gate, w_up, w_down, g_attn.reshape(-1, 128), g_mlp.reshape(-1, 128))
    return hid


def store_kernel(src, dst, sem):
    steps = src.shape[0]
    copies = [pltpu.make_async_copy(src.at[t], dst.at[t], sem.at[t]) for t in range(steps)]
    for copy in copies:
        copy.start()
    for copy in copies:
        copy.wait()


def run_store(y_seq):
    return pl.pallas_call(
        store_kernel,
        out_shape=jax.ShapeDtypeStruct(y_seq.shape, BF16),
        in_specs=[VMEM_SPEC],
        out_specs=ANY_SPEC,
        scratch_shapes=[pltpu.SemaphoreType.DMA((y_seq.shape[0],))],
        compiler_params=pltpu.CompilerParams(vmem_limit_bytes=16 * 1024 * 1024),
        name="store",
    )(in_vmem(y_seq))


def solution(mesh):
    tp = mesh.shape['tp']

    def local_run(x_seq, cache_len, k_cache, v_cache, w_q, w_k, w_v, w_o, w_gate, w_up, w_down, g_q, g_k, g_attn, g_mlp):
        heads = w_q.shape[1] // w_k.shape[1]
        flat = (k_cache.shape[0],) + k_cache.shape[2:]
        q_rows, k_new, v_new, k_old, v_old = run_qkv(tp, x_seq, cache_len, w_q, w_k, w_v, g_q, g_k, k_cache.reshape(flat), v_cache.reshape(flat))
        part, k_out, v_out = run_attention(tp, heads, cache_len, q_rows, k_new, v_new, k_old, v_old, w_o)
        y_seq = run_mlp(tp, x_seq, part, w_gate, w_up, w_down, g_attn, g_mlp)
        return run_store(y_seq), k_out.reshape(k_cache.shape), v_out.reshape(v_cache.shape)

    data_spec = P(None, 'dp', None)
    cache_spec = P('dp', 'tp', None, None)
    col_spec = P(None, 'tp')
    row_spec = P('tp', None)
    arg_specs = (data_spec, P('dp'), cache_spec, cache_spec, col_spec, col_spec, col_spec, row_spec, col_spec, col_spec, row_spec, P('tp'), P('tp'), P(None), P(None))
    out_specs = (data_spec, cache_spec, cache_spec)
    return jax.shard_map(local_run, mesh=mesh, in_specs=arg_specs, out_specs=out_specs, check_vma=False)
```

```python
import functools

import jax
import jax.numpy as jnp
import numpy as np
from jax import lax
from jax.experimental import pallas as pl
from jax.experimental.pallas import tpu as pltpu
from jax.sharding import PartitionSpec as P

ROPE_THETA = 500000.0
NORM_EPS = 1e-6
F32 = jnp.float32
BF16 = jnp.bfloat16
MESH = pl.DeviceIdType.MESH
VMEM_SPEC = pl.BlockSpec(memory_space=pltpu.VMEM)
ANY_SPEC = pl.BlockSpec(memory_space=pl.ANY)
SMEM_SPEC = pl.BlockSpec(memory_space=pltpu.SMEM)
QKV_VMEM = 16 * 1024 * 1024
ATTENTION_VMEM = 24 * 1024 * 1024
MLP_VMEM = 50 * 1024 * 1024
SLOT_ROWS = 16


def in_vmem(val):
    return pltpu.with_memory_space_constraint(val, pltpu.VMEM)


def in_hbm(val):
    return pltpu.with_memory_space_constraint(val, pltpu.HBM)


def matmul(lhs, rhs):
    return jnp.dot(lhs, rhs, preferred_element_type=F32)


CACHE_PARTS = 4


def qkv_kernel(tp, q_width, kv_width, x_hbm, len_hbm, freq_hbm, wq_hbm, wk_hbm, wv_hbm, gq_hbm, gk_hbm, kc_hbm, vc_hbm,
               q_out, kn_out, vn_out, kc_out, vc_out,
               len_ref, freq_ref, gq_ref, gk_ref, small_sem, cache_sem, x_buf, wq_buf, wkv_buf, q_raw, k_raw, q_rows, part, inbox, turn, in_sem, send_sem, recv_sem):
    steps, rows, _ = x_hbm.shape
    hd = wk_hbm.shape[1]
    heads = wq_hbm.shape[1] // hd
    pad = q_out.shape[1]
    me = lax.axis_index("tp")
    x_in = [pltpu.make_async_copy(x_hbm.at[t], x_buf.at[pl.ds(t * rows, rows), :], in_sem.at[t]) for t in range(steps)]
    half = heads * hd // 2
    wk_in = pltpu.make_async_copy(wk_hbm, wkv_buf.at[:, pl.ds(0, hd)], in_sem.at[3])
    wq_in = [pltpu.make_async_copy(wq_hbm.at[:, pl.ds(j * half, half)], wq_buf.at[:, pl.ds(j * half, half)], in_sem.at[4 + j]) for j in range(2)]
    wv_in = pltpu.make_async_copy(wv_hbm, wkv_buf.at[:, pl.ds(hd, hd)], in_sem.at[6])
    small_in = [pltpu.make_async_copy(src, dst, small_sem.at[i]) for i, (src, dst) in enumerate(
        ((len_hbm, len_ref), (freq_hbm, freq_ref), (gq_hbm, gq_ref), (gk_hbm, gk_ref)))]
    seqs = rows // CACHE_PARTS
    cache_in = [pltpu.make_async_copy(src.at[pl.ds(i * seqs, seqs)], dst.at[pl.ds(i * seqs, seqs)], cache_sem.at[c, i])
                for i in range(CACHE_PARTS) for c, (src, dst) in enumerate(((kc_hbm, kc_out), (vc_hbm, vc_out)))]
    for copy in [wk_in, wv_in] + x_in + small_in + wq_in:
        copy.start()

    barrier = pltpu.get_barrier_semaphore()
    for j in range(1, tp):
        pl.semaphore_signal(barrier, inc=1, device_id={"tp": lax.rem(me + j, tp)}, device_id_type=MESH)

    for copy in small_in:
        copy.wait()
    lens = jnp.transpose(jnp.broadcast_to(len_ref[...].astype(F32), (rows, rows)))[:, :hd]
    lane = lax.broadcasted_iota(jnp.int32, (rows, hd), 1)
    sign = jnp.where(lane < hd // 2, -1.0, 1.0).astype(F32)
    tables = []
    for t in range(steps):
        angle = (lens + float(t)) * freq_ref[...]
        tables.append((jnp.cos(angle), jnp.sin(angle) * sign))

    q_rows[...] = jnp.zeros_like(q_rows)
    wk_in.wait()
    wv_in.wait()
    k_sq = []
    for t in range(steps):
        x_in[t].wait()
        val = matmul(x_buf[t * rows:(t + 1) * rows, :], wkv_buf[...]).astype(BF16).astype(F32)
        k_raw[t] = val[:, :hd]
        vn_out[t] = val[:, hd:]
        k_sq.append(jnp.sum(val[:, :hd] * val[:, :hd], axis=1, keepdims=True))
    q_sq = None
    for j in range(2):
        wq_in[j].wait()
        if j == 1:
            cache_in[0].start()
        val = matmul(x_buf[...], wq_buf[:, j * half:(j + 1) * half]).astype(BF16).astype(F32)
        q_raw[:, j * half:(j + 1) * half] = val
        sq = jnp.sum(val * val, axis=1, keepdims=True)
        q_sq = sq if q_sq is None else q_sq + sq
    packed = jnp.zeros((rows, rows), F32)
    col = lax.broadcasted_iota(jnp.int32, (rows, rows), 1)
    for t in range(steps):
        packed = jnp.where(col == t, q_sq[t * rows:(t + 1) * rows], packed)
        packed = jnp.where(col == steps + t, k_sq[t], packed)
    part[...] = jnp.transpose(packed)[:part.shape[0]]
    pl.semaphore_wait(barrier, tp - 1)
    copies = []
    for j in range(1, tp):
        copy = pltpu.make_async_remote_copy(
            src_ref=part, dst_ref=inbox.at[j - 1], send_sem=send_sem.at[j - 1], recv_sem=recv_sem.at[j - 1],
            device_id={"tp": lax.rem(me + j, tp)}, device_id_type=MESH)
        copy.start()
        copies.append(copy)
    for copy in cache_in[1:]:
        copy.start()
    total = part[...]
    for j in range(1, tp):
        copies[j - 1].wait()
        total = total + inbox[j - 1]
    turn[...] = jnp.zeros_like(turn)
    turn[0:part.shape[0], :] = total
    sums = jnp.transpose(turn[...])
    gain_k = gk_ref[...].astype(F32)
    gain_q = gq_ref[...].astype(F32)
    for t in range(steps):
        cos_tab, sin_tab = tables[t]
        q_fac = lax.rsqrt(sums[:, t:t + 1] / q_width + NORM_EPS)
        k_fac = lax.rsqrt(sums[:, steps + t:steps + t + 1] / kv_width + NORM_EPS)
        val = k_raw[t] * k_fac * gain_k
        val = val * cos_tab + pltpu.roll(val, hd // 2, axis=1) * sin_tab
        kn_out[t] = val.astype(BF16).astype(F32)
        for g in range(heads):
            val = q_raw[t * rows:(t + 1) * rows, g * hd:(g + 1) * hd] * q_fac * gain_q[g:g + 1, :]
            val = val * cos_tab + pltpu.roll(val, hd // 2, axis=1) * sin_tab
            q_rows[pl.ds(t * heads + g, rows, stride=pad), :] = val
    q_out[...] = q_rows[...].reshape(rows, pad, hd).astype(BF16)
    for copy in cache_in:
        copy.wait()


def run_qkv(tp, x_seq, cache_len, w_q, w_k, w_v, g_q, g_k, k_cache, v_cache):
    steps, rows, d_model = x_seq.shape
    hd = w_k.shape[1]
    width = w_q.shape[1]
    heads = width // hd
    pad = 16
    inv_freq = (ROPE_THETA ** (-(np.arange(hd // 2, dtype=np.float64) * (2.0 / hd)))).astype(np.float32)
    freq = jnp.asarray(np.concatenate([inv_freq, inv_freq])[None, :])
    return pl.pallas_call(
        functools.partial(qkv_kernel, tp, width * tp, hd * tp),
        out_shape=(pltpu.VMEM((rows, pad, hd), BF16),
                   pltpu.VMEM((steps, rows, hd), F32),
                   pltpu.VMEM((steps, rows, hd), F32),
                   pltpu.VMEM(k_cache.shape, BF16),
                   pltpu.VMEM(v_cache.shape, BF16)),
        in_specs=[ANY_SPEC] * 10,
        out_specs=(VMEM_SPEC,) * 5,
        scratch_shapes=[
            pltpu.VMEM((1, rows), jnp.int32),
            pltpu.VMEM((1, hd), F32),
            pltpu.VMEM((heads, hd), BF16),
            pltpu.VMEM((1, hd), BF16),
            pltpu.SemaphoreType.DMA((4,)),
            pltpu.SemaphoreType.DMA((2, CACHE_PARTS)),
            pltpu.VMEM((steps * rows, d_model), BF16),
            pltpu.VMEM((d_model, width), BF16),
            pltpu.VMEM((d_model, 2 * hd), BF16),
            pltpu.VMEM((steps * rows, width), F32),
            pltpu.VMEM((steps, rows, hd), F32),
            pltpu.VMEM((rows * pad, hd), F32),
            pltpu.VMEM((8, rows), F32),
            pltpu.VMEM((tp - 1, 8, rows), F32),
            pltpu.VMEM((rows, rows), F32),
            pltpu.SemaphoreType.DMA((7,)),
            pltpu.SemaphoreType.DMA((tp - 1,)),
            pltpu.SemaphoreType.DMA((tp - 1,)),
        ],
        compiler_params=pltpu.CompilerParams(collective_id=0, has_side_effects=True, vmem_limit_bytes=QKV_VMEM),
        name="qkv",
    )(*[in_hbm(val) for val in (x_seq, cache_len.reshape(1, rows), freq, w_q, w_k, w_v, g_q.reshape(heads, hd), g_k.reshape(1, hd), k_cache, v_cache)])


SEQ_BLOCK = 8
PATCH_ROWS = 32


def attention_kernel(steps, heads, len_ref, q_ref, kn_ref, vn_ref, k_in, v_in, wo_hbm, k_out, v_out, part,
                     k_buf, v_buf, o_ref, wo, mixed, wo_sem, out_sem):
    rows, seq_max, hd = k_buf.shape
    pad = q_ref.shape[1]
    blocks = rows // SEQ_BLOCK
    d_model = wo.shape[1]
    wo_in = pltpu.make_async_copy(wo_hbm, wo, wo_sem)
    wo_in.start()

    def moves(blk):
        sl = pl.ds(blk * SEQ_BLOCK, SEQ_BLOCK)
        return (pltpu.make_async_copy(k_buf.at[sl], k_out.at[sl], out_sem.at[0, blk]),
                pltpu.make_async_copy(v_buf.at[sl], v_out.at[sl], out_sem.at[1, blk]))

    scale = hd ** -0.5
    win_row = lax.broadcasted_iota(jnp.int32, (PATCH_ROWS, hd), 0)
    key_col = lax.broadcasted_iota(jnp.int32, (pad, seq_max), 1)
    step_row = lax.broadcasted_iota(jnp.int32, (pad, seq_max), 0) // heads
    key_off = key_col - step_row

    def body(blk, carry):
        block = pl.ds(blk * SEQ_BLOCK, SEQ_BLOCK)
        k_buf[block] = k_in[block]
        v_buf[block] = v_in[block]
        lens = []
        for i in range(SEQ_BLOCK):
            b = blk * SEQ_BLOCK + i
            length = len_ref[b]
            base = pl.multiple_of(jnp.minimum((length // 16) * 16, seq_max - PATCH_ROWS), 16)
            for buf, new_ref in ((k_buf, kn_ref), (v_buf, vn_ref)):
                win = buf[b, pl.ds(base, PATCH_ROWS), :].astype(F32)
                for t in range(steps):
                    win = jnp.where(win_row == length + t - base, new_ref[t, pl.ds(b, 1), :], win)
                buf[b, pl.ds(base, PATCH_ROWS), :] = win.astype(BF16)
            lens.append(length)
        scores = []
        for i in range(SEQ_BLOCK):
            b = blk * SEQ_BLOCK + i
            s = lax.dot_general(q_ref[b], k_buf[b], (((1,), (1,)), ((), ())), preferred_element_type=F32) * scale
            scores.append(jnp.where(key_off <= lens[i], s, -jnp.inf))
        exps = []
        for i in range(SEQ_BLOCK):
            e = jnp.exp(scores[i] - jnp.max(scores[i], axis=1, keepdims=True))
            exps.append((e.astype(BF16), jnp.sum(e, axis=1, keepdims=True)))
        for i in range(SEQ_BLOCK):
            b = blk * SEQ_BLOCK + i
            out = matmul(exps[i][0], v_buf[b]) / exps[i][1]
            mixed[pl.ds(pl.multiple_of(b * pad, pad), pad), :] = out
        for copy in moves(blk):
            copy.start()
        return carry

    lax.fori_loop(0, blocks, body, 0)
    for t in range(steps):
        for g in range(heads):
            o_ref[t * rows:(t + 1) * rows, g * hd:(g + 1) * hd] = mixed[pl.ds(t * heads + g, rows, stride=pad), :].astype(BF16)

    wo_in.wait()
    for n in range(0, d_model, DOWN_TILE):
        val = matmul(o_ref[...], wo[:, n:n + DOWN_TILE]).astype(BF16)
        part[:, :, :, :, n:n + DOWN_TILE] = val.reshape(part.shape[:4] + (DOWN_TILE,))

    def finish(blk, carry):
        for copy in moves(blk):
            copy.wait()
        return carry

    lax.fori_loop(0, blocks, finish, 0)


def run_attention(tp, heads, cache_len, q_rows, k_new, v_new, k_cache, v_cache, w_o):
    rows, seq_max, hd = k_cache.shape
    steps = k_new.shape[0]
    pad = q_rows.shape[1]
    flat = jax.ShapeDtypeStruct(k_cache.shape, BF16)
    part = pltpu.VMEM((steps, tp // 2, 2, rows // tp, w_o.shape[1]), BF16)
    k_out, v_out, part = pl.pallas_call(
        functools.partial(attention_kernel, steps, heads),
        out_shape=(flat, flat, part),
        in_specs=[SMEM_SPEC] + [VMEM_SPEC] * 5 + [ANY_SPEC],
        out_specs=(ANY_SPEC, ANY_SPEC, VMEM_SPEC),
        scratch_shapes=[
            pltpu.VMEM(k_cache.shape, BF16),
            pltpu.VMEM(v_cache.shape, BF16),
            pltpu.VMEM((steps * rows, heads * hd), BF16),
            pltpu.VMEM(w_o.shape, BF16),
            pltpu.VMEM((rows * pad, hd), F32),
            pltpu.SemaphoreType.DMA,
            pltpu.SemaphoreType.DMA((2, rows // SEQ_BLOCK)),
        ],
        compiler_params=pltpu.CompilerParams(vmem_limit_bytes=ATTENTION_VMEM),
        name="attention",
    )(cache_len, in_vmem(q_rows), in_vmem(k_new), in_vmem(v_new), in_vmem(k_cache), in_vmem(v_cache), in_hbm(w_o))
    return part, k_out, v_out


QUARTERS = 4
LEFT_PIECES = tuple(range(QUARTERS // 2))
RIGHT_PIECES = tuple(range(QUARTERS // 2, QUARTERS))
PIECED = ("pair", "relay", "near", "far", "own_r", "own_l", "pass")
WHOLE = ("own_s", "sib_r", "sib_l", "sib_fr", "sib_fl")
COPIES = tuple((kind, q) for kind in PIECED for q in range(QUARTERS)) + tuple((kind, 0) for kind in WHOLE)
GATE_TILE = 256
FETCHES = 1
DOWN_TILE = 512
TASKS = ("send", "pair", "relay", "norm", "pass", "sib", "sibf", "gather", "gate", "down", "fetch")
ORDER = (
    2, 21, 1, 3, 1060, 23, 11, 0, 102, 13, 1150, 103, 1160, 12, 100, 101, 1051, 10, 1041, 112, 110, 1110, 113, 202,
    1011, 20, 111, 200, 1100, 203, 201, 123, 212, 22, 121, 120, 211, 1021, 210, 1140, 213, 300, 122, 1130, 1000, 1030, 400, 402,
    401, 403, 1040, 310, 221, 220, 1050, 1170, 223, 1120, 1020, 222, 501, 500, 1001, 600, 601, 1010, 412, 410, 1061, 1031, 700, 800,
    801, 802, 411, 413, 803, 804, 320, 805, 511, 806, 900, 901, 510, 902, 610, 611, 903, 904, 150, 905, 906, 710, 422, 151,
    907, 810, 420, 421, 811, 153, 812, 152, 520, 423, 813, 814, 251, 250, 521, 815, 816, 910, 911, 620, 912, 913, 253, 252,
    914, 160, 621, 915, 916, 161, 917, 720, 820, 821, 162, 822, 163, 823, 350, 824, 825, 826, 920, 921, 262, 922, 923, 261,
    924, 170, 925, 926, 171, 927, 260, 172, 173, 263, 452, 451, 270, 453, 450, 272, 271, 273, 360, 370, 460, 551, 650, 463,
    462, 651, 461, 550, 470, 472, 473, 750, 471, 570, 661, 660, 571, 560, 561, 670, 671, 760, 770,
)


def mlp_kernel(chips, x_hbm, part_in, w1_hbm, w3_hbm, w2_hbm, ga_hbm, gm_hbm, hid, part,
               ga_ref, gm_ref, small_sem, w1, w3, w2, x_own, gains, pair_in, relay_in, near_in, act, w_sem, x_sem, send_sem, recv_sem):
    steps, rows, d_model = x_hbm.shape
    ff = w1_hbm.shape[1]
    piece = d_model // QUARTERS
    me = lax.axis_index("tp")
    chip, core = me // 2, lax.rem(me, 2)
    nxt, prv, opp = lax.rem(chip + 1, chips), lax.rem(chip + chips - 1, chips), lax.rem(chip + 2, chips)
    right, left, sib = nxt * 2 + core, prv * 2 + core, chip * 2 + 1 - core
    n_gate, n_down = ff // GATE_TILE, d_model // DOWN_TILE

    def fetches(hbm, buf, width, sem):
        depth = hbm.shape[0] // FETCHES
        return [[pltpu.make_async_copy(hbm.at[pl.ds(i * depth, depth), pl.ds(j * width, width)],
                                       buf.at[pl.ds(i * depth, depth), pl.ds(j * width, width)], w_sem.at[sem + j * FETCHES + i])
                 for i in range(FETCHES)] for j in range(hbm.shape[1] // width)]

    w1_in = fetches(w1_hbm, w1, GATE_TILE, 0)
    w3_in = fetches(w3_hbm, w3, GATE_TILE, n_gate * FETCHES)
    gate_in = [a + b for a, b in zip(w1_in, w3_in)]
    down_in = fetches(w2_hbm, w2, DOWN_TILE, 2 * n_gate * FETCHES)

    def slot(c, k):
        return pl.ds(pl.multiple_of((c * 2 + k) * SLOT_ROWS, SLOT_ROWS), SLOT_ROWS)

    x_in = [pltpu.make_async_copy(x_hbm.at[t, slot(chip, core), :], x_own.at[t], x_sem.at[t]) for t in range(steps)]
    small_in = [pltpu.make_async_copy(src, dst, small_sem.at[i]) for i, (src, dst) in enumerate(
        ((ga_hbm, ga_ref), (gm_hbm, gm_ref)))]
    for copy in small_in + x_in:
        copy.start()
    barrier = pltpu.get_barrier_semaphore()
    for other in (right, left, sib):
        pl.semaphore_signal(barrier, inc=1, device_id={"tp": other}, device_id_type=MESH)
    for copy in small_in:
        copy.wait()
    for i, ref in enumerate((ga_ref, gm_ref)):
        vals = ref[...].astype(F32)
        for j in range(vals.shape[0]):
            gains[i, :, j * vals.shape[1]:(j + 1) * vals.shape[1]] = vals[j:j + 1, :]
    pl.semaphore_wait(barrier, 3)

    def quarter(q, count=1):
        return pl.ds(q * piece, count * piece)

    def endpoints(t, kind, q):
        own, other = part.at[t, :, core], part.at[t, :, 1 - core]
        to_right = q in LEFT_PIECES
        c = quarter(q)
        if kind == "pair":
            return other.at[:, :, c], pair_in.at[t, :, :, c], sib
        if kind == "relay":
            return own.at[opp, :, c], relay_in.at[t, :, c], right if to_right else left
        if kind == "near":
            if to_right:
                return own.at[prv, :, c], near_in.at[t, 1, :, c], left
            return own.at[nxt, :, c], near_in.at[t, 0, :, c], right
        if kind == "far":
            if to_right:
                return own.at[nxt, :, c], near_in.at[t, 0, :, c], right
            return own.at[prv, :, c], near_in.at[t, 1, :, c], left
        if kind == "own_r":
            block, device = hid.at[t, slot(chip, core), c], right
        elif kind == "own_l":
            block, device = hid.at[t, slot(chip, core), c], left
        elif kind == "pass":
            block, device = (hid.at[t, slot(prv, core), c], right) if to_right else (hid.at[t, slot(nxt, core), c], left)
        elif kind == "own_s":
            block, device = hid.at[t, slot(chip, core), :], sib
        elif kind == "sib_r":
            block, device = hid.at[t, slot(prv, core), :], sib
        elif kind == "sib_l":
            block, device = hid.at[t, slot(nxt, core), :], sib
        elif kind == "sib_fr":
            block, device = hid.at[t, slot(opp, core), quarter(0, QUARTERS // 2)], sib
        else:
            block, device = hid.at[t, slot(opp, core), quarter(QUARTERS // 2, QUARTERS // 2)], sib
        return block, block, device

    def copy(ph, t, kind, q=0):
        src, dst, device = endpoints(t, kind, q)
        j = COPIES.index((kind, q))
        return pltpu.make_async_remote_copy(
            src_ref=src, dst_ref=dst, send_sem=send_sem.at[ph, t, j], recv_sem=recv_sem.at[ph, t, j],
            device_id={"tp": device}, device_id_type=MESH)

    def sent(ph, t):
        for kind, q in COPIES:
            copy(ph, t, kind, q).wait_send()

    def pair_send(ph, t, q):
        copy(0, t, "pair", q).start()

    def pair_add(ph, t, q):
        copy(ph, t, "pair", q).wait_recv()
        c = slice(q * piece, (q + 1) * piece)
        for n in (opp, prv, nxt, chip):
            part[t, n, core, :, c] = (part[t, n, core, :, c].astype(F32) + pair_in[t, n, :, c].astype(F32)).astype(BF16)
        copy(ph, t, "relay", q).start()
        copy(ph, t, "near", q).start()

    def relay_add(ph, t, q):
        copy(ph, t, "relay", q).wait_recv()
        c = slice(q * piece, (q + 1) * piece)
        n = nxt if q in LEFT_PIECES else prv
        part[t, n, core, :, c] = (part[t, n, core, :, c].astype(F32) + relay_in[t, :, c].astype(F32)).astype(BF16)
        copy(ph, t, "far", q).start()

    def norm(ph, t, _):
        for q in range(QUARTERS):
            copy(ph, t, "near", q).wait_recv()
            copy(ph, t, "far", q).wait_recv()
        total = part[t, chip, core].astype(F32) + near_in[t, 0].astype(F32) + near_in[t, 1].astype(F32)
        total = total.astype(BF16).astype(F32)
        fac = lax.rsqrt(jnp.sum(total * total, axis=1, keepdims=True) / d_model + NORM_EPS)
        if ph == 0:
            x_in[t].wait()
            base = x_own[t]
        else:
            base = hid[t, slot(chip, core), :]
        hid[t, slot(chip, core), :] = (base.astype(F32) + total * fac * gains[ph]).astype(BF16)
        for first, second in ((LEFT_PIECES, RIGHT_PIECES), (RIGHT_PIECES, LEFT_PIECES)):
            for i, j in zip(first, second):
                copy(ph, t, "own_r", i).start()
                copy(ph, t, "own_l", j).start()
        copy(ph, t, "own_s").start()

    def pass_on(ph, t, q):
        copy(ph, t, "own_r" if q in LEFT_PIECES else "own_l", q).wait_recv()
        copy(ph, t, "pass", q).start()

    def pass_sib(ph, t, side):
        for q in (RIGHT_PIECES, LEFT_PIECES)[side]:
            copy(ph, t, ("own_r", "own_l")[side], q).wait_recv()
        copy(ph, t, ("sib_r", "sib_l")[side]).start()

    def far_sib(ph, t, side):
        for q in (LEFT_PIECES, RIGHT_PIECES)[side]:
            copy(ph, t, "pass", q).wait_recv()
        copy(ph, t, ("sib_fr", "sib_fl")[side]).start()

    def gather(ph, t, _):
        for kind in WHOLE:
            copy(ph, t, kind).wait_recv()

    def gate_up(ph, t, j):
        if t == 0:
            for fetch in gate_in[j]:
                fetch.wait()
        sl = slice(j * GATE_TILE, (j + 1) * GATE_TILE)
        gate = matmul(hid[t], w1[:, sl])
        up = matmul(hid[t], w3[:, sl])
        act[:, sl] = (gate / (1.0 + jnp.exp(-gate)) * up).astype(BF16)

    def down(ph, t, j):
        if j == 0:
            sent(0, t)
        if t == 0:
            for fetch in down_in[j]:
                fetch.wait()
        sl = slice(j * DOWN_TILE, (j + 1) * DOWN_TILE)
        val = matmul(act[...], w2[:, sl]).astype(BF16)
        part[t, :, :, :, sl] = val.reshape(chips, 2, SLOT_ROWS, DOWN_TILE)
        if (j + 1) * DOWN_TILE % piece == 0:
            copy(1, t, "pair", (j + 1) * DOWN_TILE // piece - 1).start()

    run = (pair_send, pair_add, relay_add, norm, pass_on, pass_sib, far_sib, gather, gate_up, down)
    for code in ORDER:
        if code >= 1000:
            (gate_in, down_in)[code // 100 % 10][code // 10 % 10][code % 10].start()
        else:
            run[code // 100](code // 50 % 2, code % 50 // 10, code % 10)
    for t in range(steps):
        sent(1, t)


def run_mlp(tp, x_seq, part, w_gate, w_up, w_down, g_attn, g_mlp):
    steps, rows, d_model = x_seq.shape
    ff = w_gate.shape[1]
    chips = tp // 2
    n_sem = (2 * (ff // GATE_TILE) + d_model // DOWN_TILE) * FETCHES
    hid, _ = pl.pallas_call(
        functools.partial(mlp_kernel, chips),
        out_shape=(pltpu.VMEM((steps, rows, d_model), BF16), pltpu.VMEM(part.shape, BF16)),
        in_specs=[ANY_SPEC, VMEM_SPEC] + [ANY_SPEC] * 5,
        out_specs=(VMEM_SPEC, VMEM_SPEC),
        input_output_aliases={1: 1},
        scratch_shapes=[
            pltpu.VMEM((d_model // 128, 128), BF16),
            pltpu.VMEM((d_model // 128, 128), BF16),
            pltpu.SemaphoreType.DMA((2,)),
            pltpu.VMEM(w_gate.shape, BF16),
            pltpu.VMEM(w_up.shape, BF16),
            pltpu.VMEM(w_down.shape, BF16),
            pltpu.VMEM((steps, SLOT_ROWS, d_model), BF16),
            pltpu.VMEM((2, 1, d_model), F32),
            pltpu.VMEM((steps, chips, SLOT_ROWS, d_model), BF16),
            pltpu.VMEM((steps, SLOT_ROWS, d_model), BF16),
            pltpu.VMEM((steps, 2, SLOT_ROWS, d_model), BF16),
            pltpu.VMEM((rows, ff), BF16),
            pltpu.SemaphoreType.DMA((n_sem,)),
            pltpu.SemaphoreType.DMA((steps,)),
            pltpu.SemaphoreType.DMA((2, steps, len(COPIES))),
            pltpu.SemaphoreType.DMA((2, steps, len(COPIES))),
        ],
        compiler_params=pltpu.CompilerParams(collective_id=1, has_side_effects=True, vmem_limit_bytes=MLP_VMEM),
        name="mlp",
    )(in_hbm(x_seq), in_vmem(part), in_hbm(w_gate), in_hbm(w_up), in_hbm(w_down), g_attn.reshape(-1, 128), g_mlp.reshape(-1, 128))
    return hid


def store_kernel(src, dst, sem):
    steps = src.shape[0]
    copies = [pltpu.make_async_copy(src.at[t], dst.at[t], sem.at[t]) for t in range(steps)]
    for copy in copies:
        copy.start()
    for copy in copies:
        copy.wait()


def run_store(y_seq):
    return pl.pallas_call(
        store_kernel,
        out_shape=jax.ShapeDtypeStruct(y_seq.shape, BF16),
        in_specs=[VMEM_SPEC],
        out_specs=ANY_SPEC,
        scratch_shapes=[pltpu.SemaphoreType.DMA((y_seq.shape[0],))],
        compiler_params=pltpu.CompilerParams(vmem_limit_bytes=16 * 1024 * 1024),
        name="store",
    )(in_vmem(y_seq))


def solution(mesh):
    tp = mesh.shape['tp']

    def local_run(x_seq, cache_len, k_cache, v_cache, w_q, w_k, w_v, w_o, w_gate, w_up, w_down, g_q, g_k, g_attn, g_mlp):
        heads = w_q.shape[1] // w_k.shape[1]
        flat = (k_cache.shape[0],) + k_cache.shape[2:]
        q_rows, k_new, v_new, k_old, v_old = run_qkv(tp, x_seq, cache_len, w_q, w_k, w_v, g_q, g_k, k_cache.reshape(flat), v_cache.reshape(flat))
        part, k_out, v_out = run_attention(tp, heads, cache_len, q_rows, k_new, v_new, k_old, v_old, w_o)
        y_seq = run_mlp(tp, x_seq, part, w_gate, w_up, w_down, g_attn, g_mlp)
        return run_store(y_seq), k_out.reshape(k_cache.shape), v_out.reshape(v_cache.shape)

    data_spec = P(None, 'dp', None)
    cache_spec = P('dp', 'tp', None, None)
    col_spec = P(None, 'tp')
    row_spec = P('tp', None)
    arg_specs = (data_spec, P('dp'), cache_spec, cache_spec, col_spec, col_spec, col_spec, row_spec, col_spec, col_spec, row_spec, P('tp'), P('tp'), P(None), P(None))
    out_specs = (data_spec, cache_spec, cache_spec)
    return jax.shard_map(local_run, mesh=mesh, in_specs=arg_specs, out_specs=out_specs, check_vma=False)
```

```python
import functools

import jax
import jax.numpy as jnp
import numpy as np
from jax import lax
from jax.experimental import pallas as pl
from jax.experimental.pallas import tpu as pltpu
from jax.sharding import PartitionSpec as P

ROPE_THETA = 500000.0
NORM_EPS = 1e-6
F32 = jnp.float32
BF16 = jnp.bfloat16
MESH = pl.DeviceIdType.MESH
VMEM_SPEC = pl.BlockSpec(memory_space=pltpu.VMEM)
ANY_SPEC = pl.BlockSpec(memory_space=pl.ANY)
SMEM_SPEC = pl.BlockSpec(memory_space=pltpu.SMEM)
QKV_VMEM = 16 * 1024 * 1024
ATTENTION_VMEM = 24 * 1024 * 1024
MLP_VMEM = 50 * 1024 * 1024
SLOT_ROWS = 16


def in_vmem(val):
    return pltpu.with_memory_space_constraint(val, pltpu.VMEM)


def in_hbm(val):
    return pltpu.with_memory_space_constraint(val, pltpu.HBM)


def matmul(lhs, rhs):
    return jnp.dot(lhs, rhs, preferred_element_type=F32)


CACHE_PARTS = 4


def qkv_kernel(tp, q_width, kv_width, x_hbm, len_hbm, freq_hbm, wq_hbm, wk_hbm, wv_hbm, gq_hbm, gk_hbm, kc_hbm, vc_hbm,
               q_out, kn_out, vn_out, kc_out, vc_out,
               len_ref, freq_ref, gq_ref, gk_ref, small_sem, cache_sem, x_buf, wq_buf, wk_buf, wv_buf, q_raw, k_raw, q_rows, part, inbox, turn, in_sem, send_sem, recv_sem):
    steps, rows, _ = x_hbm.shape
    hd = wk_hbm.shape[1]
    heads = wq_hbm.shape[1] // hd
    pad = q_out.shape[1]
    me = lax.axis_index("tp")
    x_in = [pltpu.make_async_copy(x_hbm.at[t], x_buf.at[pl.ds(t * rows, rows), :], in_sem.at[t]) for t in range(steps)]
    half = heads * hd // 2
    wk_in = pltpu.make_async_copy(wk_hbm, wk_buf, in_sem.at[3])
    wq_in = pltpu.make_async_copy(wq_hbm, wq_buf, in_sem.at[5])
    wv_in = pltpu.make_async_copy(wv_hbm, wv_buf, in_sem.at[4])
    small_in = [pltpu.make_async_copy(src, dst, small_sem.at[i]) for i, (src, dst) in enumerate(
        ((len_hbm, len_ref), (freq_hbm, freq_ref), (gq_hbm, gq_ref), (gk_hbm, gk_ref)))]
    seqs = rows // CACHE_PARTS
    cache_in = [pltpu.make_async_copy(src.at[pl.ds(i * seqs, seqs)], dst.at[pl.ds(i * seqs, seqs)], cache_sem.at[c, i])
                for i in range(CACHE_PARTS) for c, (src, dst) in enumerate(((kc_hbm, kc_out), (vc_hbm, vc_out)))]
    for copy in [wk_in, wv_in] + x_in + small_in + [wq_in]:
        copy.start()

    barrier = pltpu.get_barrier_semaphore()
    for j in range(1, tp):
        pl.semaphore_signal(barrier, inc=1, device_id={"tp": lax.rem(me + j, tp)}, device_id_type=MESH)

    for copy in small_in:
        copy.wait()
    lens = jnp.transpose(jnp.broadcast_to(len_ref[...].astype(F32), (rows, rows)))[:, :hd]
    lane = lax.broadcasted_iota(jnp.int32, (rows, hd), 1)
    sign = jnp.where(lane < hd // 2, -1.0, 1.0).astype(F32)
    tables = []
    for t in range(steps):
        angle = (lens + float(t)) * freq_ref[...]
        tables.append((jnp.cos(angle), jnp.sin(angle) * sign))

    q_rows[...] = jnp.zeros_like(q_rows)
    wk_in.wait()
    wv_in.wait()
    w_kv = jnp.concatenate([wk_buf[...], wv_buf[...]], axis=1)
    k_sq = []
    for t in range(steps):
        x_in[t].wait()
        val = matmul(x_buf[t * rows:(t + 1) * rows, :], w_kv).astype(BF16).astype(F32)
        k_raw[t] = val[:, :hd]
        vn_out[t] = val[:, hd:]
        k_sq.append(jnp.sum(val[:, :hd] * val[:, :hd], axis=1, keepdims=True))
    q_sq = None
    for j in range(2):
        if j == 0:
            wq_in.wait()
            cache_in[0].start()
        val = matmul(x_buf[...], wq_buf[:, j * half:(j + 1) * half]).astype(BF16).astype(F32)
        q_raw[:, j * half:(j + 1) * half] = val
        sq = jnp.sum(val * val, axis=1, keepdims=True)
        q_sq = sq if q_sq is None else q_sq + sq
    packed = jnp.zeros((rows, rows), F32)
    col = lax.broadcasted_iota(jnp.int32, (rows, rows), 1)
    for t in range(steps):
        packed = jnp.where(col == t, q_sq[t * rows:(t + 1) * rows], packed)
        packed = jnp.where(col == steps + t, k_sq[t], packed)
    part[...] = jnp.transpose(packed)[:part.shape[0]]
    pl.semaphore_wait(barrier, tp - 1)
    copies = []
    for j in range(1, tp):
        copy = pltpu.make_async_remote_copy(
            src_ref=part, dst_ref=inbox.at[j - 1], send_sem=send_sem.at[j - 1], recv_sem=recv_sem.at[j - 1],
            device_id={"tp": lax.rem(me + j, tp)}, device_id_type=MESH)
        copy.start()
        copies.append(copy)
    for copy in cache_in[1:]:
        copy.start()
    total = part[...]
    for j in range(1, tp):
        copies[j - 1].wait()
        total = total + inbox[j - 1]
    turn[...] = jnp.zeros_like(turn)
    turn[0:part.shape[0], :] = total
    sums = jnp.transpose(turn[...])
    gain_k = gk_ref[...].astype(F32)
    gain_q = gq_ref[...].astype(F32)
    for t in range(steps):
        cos_tab, sin_tab = tables[t]
        q_fac = lax.rsqrt(sums[:, t:t + 1] / q_width + NORM_EPS)
        k_fac = lax.rsqrt(sums[:, steps + t:steps + t + 1] / kv_width + NORM_EPS)
        val = k_raw[t] * k_fac * gain_k
        val = val * cos_tab + pltpu.roll(val, hd // 2, axis=1) * sin_tab
        kn_out[t] = val.astype(BF16).astype(F32)
        for g in range(heads):
            val = q_raw[t * rows:(t + 1) * rows, g * hd:(g + 1) * hd] * q_fac * gain_q[g:g + 1, :]
            val = val * cos_tab + pltpu.roll(val, hd // 2, axis=1) * sin_tab
            q_rows[pl.ds(t * heads + g, rows, stride=pad), :] = val
    q_out[...] = q_rows[...].reshape(rows, pad, hd).astype(BF16)
    for copy in cache_in:
        copy.wait()


def run_qkv(tp, x_seq, cache_len, w_q, w_k, w_v, g_q, g_k, k_cache, v_cache):
    steps, rows, d_model = x_seq.shape
    hd = w_k.shape[1]
    width = w_q.shape[1]
    heads = width // hd
    pad = 16
    inv_freq = (ROPE_THETA ** (-(np.arange(hd // 2, dtype=np.float64) * (2.0 / hd)))).astype(np.float32)
    freq = jnp.asarray(np.concatenate([inv_freq, inv_freq])[None, :])
    return pl.pallas_call(
        functools.partial(qkv_kernel, tp, width * tp, hd * tp),
        out_shape=(pltpu.VMEM((rows, pad, hd), BF16),
                   pltpu.VMEM((steps, rows, hd), F32),
                   pltpu.VMEM((steps, rows, hd), F32),
                   pltpu.VMEM(k_cache.shape, BF16),
                   pltpu.VMEM(v_cache.shape, BF16)),
        in_specs=[ANY_SPEC] * 10,
        out_specs=(VMEM_SPEC,) * 5,
        scratch_shapes=[
            pltpu.VMEM((1, rows), jnp.int32),
            pltpu.VMEM((1, hd), F32),
            pltpu.VMEM((heads, hd), BF16),
            pltpu.VMEM((1, hd), BF16),
            pltpu.SemaphoreType.DMA((4,)),
            pltpu.SemaphoreType.DMA((2, CACHE_PARTS)),
            pltpu.VMEM((steps * rows, d_model), BF16),
            pltpu.VMEM((d_model, width), BF16),
            pltpu.VMEM((d_model, hd), BF16),
            pltpu.VMEM((d_model, hd), BF16),
            pltpu.VMEM((steps * rows, width), F32),
            pltpu.VMEM((steps, rows, hd), F32),
            pltpu.VMEM((rows * pad, hd), F32),
            pltpu.VMEM((8, rows), F32),
            pltpu.VMEM((tp - 1, 8, rows), F32),
            pltpu.VMEM((rows, rows), F32),
            pltpu.SemaphoreType.DMA((7,)),
            pltpu.SemaphoreType.DMA((tp - 1,)),
            pltpu.SemaphoreType.DMA((tp - 1,)),
        ],
        compiler_params=pltpu.CompilerParams(collective_id=0, has_side_effects=True, vmem_limit_bytes=QKV_VMEM),
        name="qkv",
    )(*[in_hbm(val) for val in (x_seq, cache_len.reshape(1, rows), freq, w_q, w_k, w_v, g_q.reshape(heads, hd), g_k.reshape(1, hd), k_cache, v_cache)])


SEQ_BLOCK = 8
PATCH_ROWS = 32


def attention_kernel(steps, heads, len_ref, q_ref, kn_ref, vn_ref, k_in, v_in, wo_hbm, k_out, v_out, part,
                     k_buf, v_buf, o_ref, wo, mixed, wo_sem, out_sem):
    rows, seq_max, hd = k_buf.shape
    pad = q_ref.shape[1]
    blocks = rows // SEQ_BLOCK
    d_model = wo.shape[1]
    wo_in = pltpu.make_async_copy(wo_hbm, wo, wo_sem)
    wo_in.start()

    def moves(blk):
        sl = pl.ds(blk * SEQ_BLOCK, SEQ_BLOCK)
        return (pltpu.make_async_copy(k_buf.at[sl], k_out.at[sl], out_sem.at[0, blk]),
                pltpu.make_async_copy(v_buf.at[sl], v_out.at[sl], out_sem.at[1, blk]))

    scale = hd ** -0.5
    win_row = lax.broadcasted_iota(jnp.int32, (PATCH_ROWS, hd), 0)
    key_col = lax.broadcasted_iota(jnp.int32, (pad, seq_max), 1)
    step_row = lax.broadcasted_iota(jnp.int32, (pad, seq_max), 0) // heads
    key_off = key_col - step_row

    def body(blk, carry):
        block = pl.ds(blk * SEQ_BLOCK, SEQ_BLOCK)
        k_buf[block] = k_in[block]
        v_buf[block] = v_in[block]
        lens = []
        for i in range(SEQ_BLOCK):
            b = blk * SEQ_BLOCK + i
            length = len_ref[b]
            base = pl.multiple_of(jnp.minimum((length // 16) * 16, seq_max - PATCH_ROWS), 16)
            for buf, new_ref in ((k_buf, kn_ref), (v_buf, vn_ref)):
                win = buf[b, pl.ds(base, PATCH_ROWS), :].astype(F32)
                for t in range(steps):
                    win = jnp.where(win_row == length + t - base, new_ref[t, pl.ds(b, 1), :], win)
                buf[b, pl.ds(base, PATCH_ROWS), :] = win.astype(BF16)
            lens.append(length)
        scores = []
        for i in range(SEQ_BLOCK):
            b = blk * SEQ_BLOCK + i
            s = lax.dot_general(q_ref[b], k_buf[b], (((1,), (1,)), ((), ())), preferred_element_type=F32) * scale
            scores.append(jnp.where(key_off <= lens[i], s, -jnp.inf))
        exps = []
        for i in range(SEQ_BLOCK):
            e = jnp.exp(scores[i] - jnp.max(scores[i], axis=1, keepdims=True))
            exps.append((e.astype(BF16), jnp.sum(e, axis=1, keepdims=True)))
        for i in range(SEQ_BLOCK):
            b = blk * SEQ_BLOCK + i
            out = matmul(exps[i][0], v_buf[b]) / exps[i][1]
            mixed[pl.ds(pl.multiple_of(b * pad, pad), pad), :] = out
        for copy in moves(blk):
            copy.start()
        return carry

    lax.fori_loop(0, blocks, body, 0)
    for t in range(steps):
        for g in range(heads):
            o_ref[t * rows:(t + 1) * rows, g * hd:(g + 1) * hd] = mixed[pl.ds(t * heads + g, rows, stride=pad), :].astype(BF16)

    wo_in.wait()
    for n in range(0, d_model, DOWN_TILE):
        val = matmul(o_ref[...], wo[:, n:n + DOWN_TILE]).astype(BF16)
        part[:, :, :, :, n:n + DOWN_TILE] = val.reshape(part.shape[:4] + (DOWN_TILE,))

    def finish(blk, carry):
        for copy in moves(blk):
            copy.wait()
        return carry

    lax.fori_loop(0, blocks, finish, 0)


def run_attention(tp, heads, cache_len, q_rows, k_new, v_new, k_cache, v_cache, w_o):
    rows, seq_max, hd = k_cache.shape
    steps = k_new.shape[0]
    pad = q_rows.shape[1]
    flat = jax.ShapeDtypeStruct(k_cache.shape, BF16)
    part = pltpu.VMEM((steps, tp // 2, 2, rows // tp, w_o.shape[1]), BF16)
    k_out, v_out, part = pl.pallas_call(
        functools.partial(attention_kernel, steps, heads),
        out_shape=(flat, flat, part),
        in_specs=[SMEM_SPEC] + [VMEM_SPEC] * 5 + [ANY_SPEC],
        out_specs=(ANY_SPEC, ANY_SPEC, VMEM_SPEC),
        scratch_shapes=[
            pltpu.VMEM(k_cache.shape, BF16),
            pltpu.VMEM(v_cache.shape, BF16),
            pltpu.VMEM((steps * rows, heads * hd), BF16),
            pltpu.VMEM(w_o.shape, BF16),
            pltpu.VMEM((rows * pad, hd), F32),
            pltpu.SemaphoreType.DMA,
            pltpu.SemaphoreType.DMA((2, rows // SEQ_BLOCK)),
        ],
        compiler_params=pltpu.CompilerParams(vmem_limit_bytes=ATTENTION_VMEM),
        name="attention",
    )(cache_len, in_vmem(q_rows), in_vmem(k_new), in_vmem(v_new), in_vmem(k_cache), in_vmem(v_cache), in_hbm(w_o))
    return part, k_out, v_out


QUARTERS = 4
LEFT_PIECES = tuple(range(QUARTERS // 2))
RIGHT_PIECES = tuple(range(QUARTERS // 2, QUARTERS))
PIECED = ("pair", "relay", "near", "far", "own_r", "own_l", "pass")
WHOLE = ("own_s", "sib_r", "sib_l", "sib_fr", "sib_fl")
COPIES = tuple((kind, q) for kind in PIECED for q in range(QUARTERS)) + tuple((kind, 0) for kind in WHOLE)
GATE_TILE = 256
FETCHES = 8
DOWN_TILE = 512
TASKS = ("send", "pair", "relay", "norm", "pass", "sib", "sibf", "gather", "gate", "down", "fetch")
ORDER = (
    1105, 2, 3, 1, 22, 0, 1101, 102, 101, 11, 10, 1011, 13, 103, 100, 122, 1107, 111, 1007, 1003, 1106, 1004, 12, 113,
    21, 1012, 201, 202, 1006, 203, 200, 110, 23, 1015, 112, 20, 1008, 120, 211, 123, 1100, 213, 1010, 300, 1102, 1000, 121, 210,
    1104, 1005, 212, 1009, 402, 400, 1013, 403, 401, 1103, 220, 222, 1002, 500, 501, 1014, 221, 223, 310, 1001, 601, 600, 700, 800,
    801, 802, 410, 412, 413, 411, 803, 320, 804, 805, 510, 806, 900, 511, 901, 902, 903, 904, 610, 611, 905, 150, 906, 907,
    422, 423, 710, 151, 420, 421, 810, 152, 153, 811, 812, 520, 813, 814, 815, 251, 816, 250, 910, 911, 912, 521, 913, 253,
    621, 620, 914, 252, 160, 915, 916, 917, 720, 161, 820, 821, 162, 163, 822, 823, 350, 824, 825, 826, 920, 921, 922, 263,
    923, 260, 924, 170, 925, 926, 171, 927, 450, 172, 261, 173, 262, 452, 451, 270, 453, 271, 272, 273, 360, 370, 463, 650,
    651, 550, 460, 461, 462, 470, 472, 471, 561, 551, 473, 570, 750, 560, 571, 660, 661, 760, 670, 671, 770,
)


def mlp_kernel(chips, x_hbm, part_in, w1_hbm, w3_hbm, w2_hbm, ga_hbm, gm_hbm, hid, part,
               ga_ref, gm_ref, small_sem, w1, w3, w2, x_own, gains, pair_in, relay_in, near_in, act, w_sem, x_sem, send_sem, recv_sem):
    steps, rows, d_model = x_hbm.shape
    ff = w1_hbm.shape[1]
    piece = d_model // QUARTERS
    me = lax.axis_index("tp")
    chip, core = me // 2, lax.rem(me, 2)
    nxt, prv, opp = lax.rem(chip + 1, chips), lax.rem(chip + chips - 1, chips), lax.rem(chip + 2, chips)
    right, left, sib = nxt * 2 + core, prv * 2 + core, chip * 2 + 1 - core
    n_gate, n_down = ff // GATE_TILE, d_model // DOWN_TILE

    def fetches(hbm, buf, sem):
        depth = hbm.shape[0] // FETCHES
        blocks = [pl.ds(i * depth, depth) for i in range(FETCHES)]
        return [pltpu.make_async_copy(hbm.at[blocks[i]], buf.at[blocks[i]], w_sem.at[sem, i]) for i in range(FETCHES)]

    gate_in = [copy for pair in zip(fetches(w1_hbm, w1, 0), fetches(w3_hbm, w3, 1)) for copy in pair]
    down_in = fetches(w2_hbm, w2, 2)

    def slot(c, k):
        return pl.ds(pl.multiple_of((c * 2 + k) * SLOT_ROWS, SLOT_ROWS), SLOT_ROWS)

    x_in = [pltpu.make_async_copy(x_hbm.at[t, slot(chip, core), :], x_own.at[t], x_sem.at[t]) for t in range(steps)]
    small_in = [pltpu.make_async_copy(src, dst, small_sem.at[i]) for i, (src, dst) in enumerate(
        ((ga_hbm, ga_ref), (gm_hbm, gm_ref)))]
    for copy in small_in + x_in:
        copy.start()
    barrier = pltpu.get_barrier_semaphore()
    for other in (right, left, sib):
        pl.semaphore_signal(barrier, inc=1, device_id={"tp": other}, device_id_type=MESH)
    for copy in small_in:
        copy.wait()
    for i, ref in enumerate((ga_ref, gm_ref)):
        vals = ref[...].astype(F32)
        for j in range(vals.shape[0]):
            gains[i, :, j * vals.shape[1]:(j + 1) * vals.shape[1]] = vals[j:j + 1, :]
    pl.semaphore_wait(barrier, 3)

    def quarter(q, count=1):
        return pl.ds(q * piece, count * piece)

    def endpoints(t, kind, q):
        own, other = part.at[t, :, core], part.at[t, :, 1 - core]
        to_right = q in LEFT_PIECES
        c = quarter(q)
        if kind == "pair":
            return other.at[:, :, c], pair_in.at[t, :, :, c], sib
        if kind == "relay":
            return own.at[opp, :, c], relay_in.at[t, :, c], right if to_right else left
        if kind == "near":
            if to_right:
                return own.at[prv, :, c], near_in.at[t, 1, :, c], left
            return own.at[nxt, :, c], near_in.at[t, 0, :, c], right
        if kind == "far":
            if to_right:
                return own.at[nxt, :, c], near_in.at[t, 0, :, c], right
            return own.at[prv, :, c], near_in.at[t, 1, :, c], left
        if kind == "own_r":
            block, device = hid.at[t, slot(chip, core), c], right
        elif kind == "own_l":
            block, device = hid.at[t, slot(chip, core), c], left
        elif kind == "pass":
            block, device = (hid.at[t, slot(prv, core), c], right) if to_right else (hid.at[t, slot(nxt, core), c], left)
        elif kind == "own_s":
            block, device = hid.at[t, slot(chip, core), :], sib
        elif kind == "sib_r":
            block, device = hid.at[t, slot(prv, core), :], sib
        elif kind == "sib_l":
            block, device = hid.at[t, slot(nxt, core), :], sib
        elif kind == "sib_fr":
            block, device = hid.at[t, slot(opp, core), quarter(0, QUARTERS // 2)], sib
        else:
            block, device = hid.at[t, slot(opp, core), quarter(QUARTERS // 2, QUARTERS // 2)], sib
        return block, block, device

    def copy(ph, t, kind, q=0):
        src, dst, device = endpoints(t, kind, q)
        j = COPIES.index((kind, q))
        return pltpu.make_async_remote_copy(
            src_ref=src, dst_ref=dst, send_sem=send_sem.at[ph, t, j], recv_sem=recv_sem.at[ph, t, j],
            device_id={"tp": device}, device_id_type=MESH)

    def sent(ph, t):
        for kind, q in COPIES:
            copy(ph, t, kind, q).wait_send()

    def pair_send(ph, t, q):
        copy(0, t, "pair", q).start()

    def pair_add(ph, t, q):
        copy(ph, t, "pair", q).wait_recv()
        c = slice(q * piece, (q + 1) * piece)
        for n in (opp, prv, nxt, chip):
            part[t, n, core, :, c] = (part[t, n, core, :, c].astype(F32) + pair_in[t, n, :, c].astype(F32)).astype(BF16)
        copy(ph, t, "relay", q).start()
        copy(ph, t, "near", q).start()

    def relay_add(ph, t, q):
        copy(ph, t, "relay", q).wait_recv()
        c = slice(q * piece, (q + 1) * piece)
        n = nxt if q in LEFT_PIECES else prv
        part[t, n, core, :, c] = (part[t, n, core, :, c].astype(F32) + relay_in[t, :, c].astype(F32)).astype(BF16)
        copy(ph, t, "far", q).start()

    def norm(ph, t, _):
        for q in range(QUARTERS):
            copy(ph, t, "near", q).wait_recv()
            copy(ph, t, "far", q).wait_recv()
        total = part[t, chip, core].astype(F32) + near_in[t, 0].astype(F32) + near_in[t, 1].astype(F32)
        total = total.astype(BF16).astype(F32)
        fac = lax.rsqrt(jnp.sum(total * total, axis=1, keepdims=True) / d_model + NORM_EPS)
        if ph == 0:
            x_in[t].wait()
            base = x_own[t]
        else:
            base = hid[t, slot(chip, core), :]
        hid[t, slot(chip, core), :] = (base.astype(F32) + total * fac * gains[ph]).astype(BF16)
        for first, second in ((LEFT_PIECES, RIGHT_PIECES), (RIGHT_PIECES, LEFT_PIECES)):
            for i, j in zip(first, second):
                copy(ph, t, "own_r", i).start()
                copy(ph, t, "own_l", j).start()
        copy(ph, t, "own_s").start()

    def pass_on(ph, t, q):
        copy(ph, t, "own_r" if q in LEFT_PIECES else "own_l", q).wait_recv()
        copy(ph, t, "pass", q).start()

    def pass_sib(ph, t, side):
        for q in (RIGHT_PIECES, LEFT_PIECES)[side]:
            copy(ph, t, ("own_r", "own_l")[side], q).wait_recv()
        copy(ph, t, ("sib_r", "sib_l")[side]).start()

    def far_sib(ph, t, side):
        for q in (LEFT_PIECES, RIGHT_PIECES)[side]:
            copy(ph, t, "pass", q).wait_recv()
        copy(ph, t, ("sib_fr", "sib_fl")[side]).start()

    def gather(ph, t, _):
        for kind in WHOLE:
            copy(ph, t, kind).wait_recv()

    def gate_up(ph, t, j):
        if t == 0 and j == 0:
            for fetch in gate_in:
                fetch.wait()
        sl = slice(j * GATE_TILE, (j + 1) * GATE_TILE)
        gate = matmul(hid[t], w1[:, sl])
        up = matmul(hid[t], w3[:, sl])
        act[:, sl] = (gate / (1.0 + jnp.exp(-gate)) * up).astype(BF16)

    def down(ph, t, j):
        if j == 0:
            sent(0, t)
        if t == 0 and j == 0:
            for fetch in down_in:
                fetch.wait()
        sl = slice(j * DOWN_TILE, (j + 1) * DOWN_TILE)
        val = matmul(act[...], w2[:, sl]).astype(BF16)
        part[t, :, :, :, sl] = val.reshape(chips, 2, SLOT_ROWS, DOWN_TILE)
        if (j + 1) * DOWN_TILE % piece == 0:
            copy(1, t, "pair", (j + 1) * DOWN_TILE // piece - 1).start()

    run = (pair_send, pair_add, relay_add, norm, pass_on, pass_sib, far_sib, gather, gate_up, down)
    for code in ORDER:
        if code >= 1000:
            (gate_in, down_in)[code // 100 % 10][code % 100].start()
        else:
            run[code // 100](code // 50 % 2, code % 50 // 10, code % 10)
    for t in range(steps):
        sent(1, t)


def run_mlp(tp, x_seq, part, w_gate, w_up, w_down, g_attn, g_mlp):
    steps, rows, d_model = x_seq.shape
    ff = w_gate.shape[1]
    chips = tp // 2
    hid, _ = pl.pallas_call(
        functools.partial(mlp_kernel, chips),
        out_shape=(pltpu.VMEM((steps, rows, d_model), BF16), pltpu.VMEM(part.shape, BF16)),
        in_specs=[ANY_SPEC, VMEM_SPEC] + [ANY_SPEC] * 5,
        out_specs=(VMEM_SPEC, VMEM_SPEC),
        input_output_aliases={1: 1},
        scratch_shapes=[
            pltpu.VMEM((d_model // 128, 128), BF16),
            pltpu.VMEM((d_model // 128, 128), BF16),
            pltpu.SemaphoreType.DMA((2,)),
            pltpu.VMEM(w_gate.shape, BF16),
            pltpu.VMEM(w_up.shape, BF16),
            pltpu.VMEM(w_down.shape, BF16),
            pltpu.VMEM((steps, SLOT_ROWS, d_model), BF16),
            pltpu.VMEM((2, 1, d_model), F32),
            pltpu.VMEM((steps, chips, SLOT_ROWS, d_model), BF16),
            pltpu.VMEM((steps, SLOT_ROWS, d_model), BF16),
            pltpu.VMEM((steps, 2, SLOT_ROWS, d_model), BF16),
            pltpu.VMEM((rows, ff), BF16),
            pltpu.SemaphoreType.DMA((3, FETCHES)),
            pltpu.SemaphoreType.DMA((steps,)),
            pltpu.SemaphoreType.DMA((2, steps, len(COPIES))),
            pltpu.SemaphoreType.DMA((2, steps, len(COPIES))),
        ],
        compiler_params=pltpu.CompilerParams(collective_id=1, has_side_effects=True, vmem_limit_bytes=MLP_VMEM),
        name="mlp",
    )(in_hbm(x_seq), in_vmem(part), in_hbm(w_gate), in_hbm(w_up), in_hbm(w_down), g_attn.reshape(-1, 128), g_mlp.reshape(-1, 128))
    return hid


def store_kernel(src, dst, sem):
    steps = src.shape[0]
    copies = [pltpu.make_async_copy(src.at[t], dst.at[t], sem.at[t]) for t in range(steps)]
    for copy in copies:
        copy.start()
    for copy in copies:
        copy.wait()


def run_store(y_seq):
    return pl.pallas_call(
        store_kernel,
        out_shape=jax.ShapeDtypeStruct(y_seq.shape, BF16),
        in_specs=[VMEM_SPEC],
        out_specs=ANY_SPEC,
        scratch_shapes=[pltpu.SemaphoreType.DMA((y_seq.shape[0],))],
        compiler_params=pltpu.CompilerParams(vmem_limit_bytes=16 * 1024 * 1024),
        name="store",
    )(in_vmem(y_seq))


def solution(mesh):
    tp = mesh.shape['tp']

    def local_run(x_seq, cache_len, k_cache, v_cache, w_q, w_k, w_v, w_o, w_gate, w_up, w_down, g_q, g_k, g_attn, g_mlp):
        heads = w_q.shape[1] // w_k.shape[1]
        flat = (k_cache.shape[0],) + k_cache.shape[2:]
        q_rows, k_new, v_new, k_old, v_old = run_qkv(tp, x_seq, cache_len, w_q, w_k, w_v, g_q, g_k, k_cache.reshape(flat), v_cache.reshape(flat))
        part, k_out, v_out = run_attention(tp, heads, cache_len, q_rows, k_new, v_new, k_old, v_old, w_o)
        y_seq = run_mlp(tp, x_seq, part, w_gate, w_up, w_down, g_attn, g_mlp)
        return run_store(y_seq), k_out.reshape(k_cache.shape), v_out.reshape(v_cache.shape)

    data_spec = P(None, 'dp', None)
    cache_spec = P('dp', 'tp', None, None)
    col_spec = P(None, 'tp')
    row_spec = P('tp', None)
    arg_specs = (data_spec, P('dp'), cache_spec, cache_spec, col_spec, col_spec, col_spec, row_spec, col_spec, col_spec, row_spec, P('tp'), P('tp'), P(None), P(None))
    out_specs = (data_spec, cache_spec, cache_spec)
    return jax.shard_map(local_run, mesh=mesh, in_specs=arg_specs, out_specs=out_specs, check_vma=False)
```

```python
import functools

import jax
import jax.numpy as jnp
import numpy as np
from jax import lax
from jax.experimental import pallas as pl
from jax.experimental.pallas import tpu as pltpu
from jax.sharding import PartitionSpec as P

ROPE_THETA = 500000.0
NORM_EPS = 1e-6
F32 = jnp.float32
BF16 = jnp.bfloat16
MESH = pl.DeviceIdType.MESH
VMEM_SPEC = pl.BlockSpec(memory_space=pltpu.VMEM)
ANY_SPEC = pl.BlockSpec(memory_space=pl.ANY)
SMEM_SPEC = pl.BlockSpec(memory_space=pltpu.SMEM)
QKV_VMEM = 16 * 1024 * 1024
ATTENTION_VMEM = 24 * 1024 * 1024
MLP_VMEM = 50 * 1024 * 1024
SLOT_ROWS = 16


def in_vmem(val):
    return pltpu.with_memory_space_constraint(val, pltpu.VMEM)


def in_hbm(val):
    return pltpu.with_memory_space_constraint(val, pltpu.HBM)


def matmul(lhs, rhs):
    return jnp.dot(lhs, rhs, preferred_element_type=F32)


CACHE_PARTS = 4


def qkv_kernel(tp, q_width, kv_width, x_hbm, len_hbm, freq_hbm, wq_hbm, wk_hbm, wv_hbm, gq_hbm, gk_hbm, kc_hbm, vc_hbm,
               q_out, kn_out, vn_out, kc_out, vc_out,
               len_ref, freq_ref, gq_ref, gk_ref, small_sem, cache_sem, x_buf, wq_buf, wk_buf, wv_buf, q_raw, k_raw, q_rows, part, inbox, turn, in_sem, send_sem, recv_sem):
    steps, rows, _ = x_hbm.shape
    hd = wk_hbm.shape[1]
    heads = wq_hbm.shape[1] // hd
    pad = q_out.shape[1]
    me = lax.axis_index("tp")
    x_in = [pltpu.make_async_copy(x_hbm.at[t], x_buf.at[pl.ds(t * rows, rows), :], in_sem.at[t]) for t in range(steps)]
    half = heads * hd // 2
    wk_in = pltpu.make_async_copy(wk_hbm, wk_buf, in_sem.at[3])
    wq_in = pltpu.make_async_copy(wq_hbm, wq_buf, in_sem.at[5])
    wv_in = pltpu.make_async_copy(wv_hbm, wv_buf, in_sem.at[4])
    small_in = [pltpu.make_async_copy(src, dst, small_sem.at[i]) for i, (src, dst) in enumerate(
        ((len_hbm, len_ref), (freq_hbm, freq_ref), (gq_hbm, gq_ref), (gk_hbm, gk_ref)))]
    seqs = rows // CACHE_PARTS
    cache_in = [pltpu.make_async_copy(src.at[pl.ds(i * seqs, seqs)], dst.at[pl.ds(i * seqs, seqs)], cache_sem.at[c, i])
                for i in range(CACHE_PARTS) for c, (src, dst) in enumerate(((kc_hbm, kc_out), (vc_hbm, vc_out)))]
    for copy in [wk_in, wv_in] + x_in + small_in + [wq_in]:
        copy.start()

    barrier = pltpu.get_barrier_semaphore()
    for j in range(1, tp):
        pl.semaphore_signal(barrier, inc=1, device_id={"tp": lax.rem(me + j, tp)}, device_id_type=MESH)

    for copy in small_in:
        copy.wait()
    lens = jnp.transpose(jnp.broadcast_to(len_ref[...].astype(F32), (rows, rows)))[:, :hd]
    lane = lax.broadcasted_iota(jnp.int32, (rows, hd), 1)
    sign = jnp.where(lane < hd // 2, -1.0, 1.0).astype(F32)
    tables = []
    for t in range(steps):
        angle = (lens + float(t)) * freq_ref[...]
        tables.append((jnp.cos(angle), jnp.sin(angle) * sign))

    q_rows[...] = jnp.zeros_like(q_rows)
    wk_in.wait()
    wv_in.wait()
    w_kv = jnp.concatenate([wk_buf[...], wv_buf[...]], axis=1)
    k_sq = []
    for t in range(steps):
        x_in[t].wait()
        val = matmul(x_buf[t * rows:(t + 1) * rows, :], w_kv).astype(BF16).astype(F32)
        k_raw[t] = val[:, :hd]
        vn_out[t] = val[:, hd:]
        k_sq.append(jnp.sum(val[:, :hd] * val[:, :hd], axis=1, keepdims=True))
    q_sq = None
    for j in range(2):
        if j == 0:
            wq_in.wait()
            for copy in cache_in[:CACHE_PARTS]:
                copy.start()
        val = matmul(x_buf[...], wq_buf[:, j * half:(j + 1) * half]).astype(BF16).astype(F32)
        q_raw[:, j * half:(j + 1) * half] = val
        sq = jnp.sum(val * val, axis=1, keepdims=True)
        q_sq = sq if q_sq is None else q_sq + sq
    packed = jnp.zeros((rows, rows), F32)
    col = lax.broadcasted_iota(jnp.int32, (rows, rows), 1)
    for t in range(steps):
        packed = jnp.where(col == t, q_sq[t * rows:(t + 1) * rows], packed)
        packed = jnp.where(col == steps + t, k_sq[t], packed)
    part[...] = jnp.transpose(packed)[:part.shape[0]]
    pl.semaphore_wait(barrier, tp - 1)
    copies = []
    for j in range(1, tp):
        copy = pltpu.make_async_remote_copy(
            src_ref=part, dst_ref=inbox.at[j - 1], send_sem=send_sem.at[j - 1], recv_sem=recv_sem.at[j - 1],
            device_id={"tp": lax.rem(me + j, tp)}, device_id_type=MESH)
        copy.start()
        copies.append(copy)
    for copy in cache_in[CACHE_PARTS:]:
        copy.start()
    total = part[...]
    for j in range(1, tp):
        copies[j - 1].wait()
        total = total + inbox[j - 1]
    turn[...] = jnp.zeros_like(turn)
    turn[0:part.shape[0], :] = total
    sums = jnp.transpose(turn[...])
    gain_k = gk_ref[...].astype(F32)
    gain_q = gq_ref[...].astype(F32)
    for t in range(steps):
        cos_tab, sin_tab = tables[t]
        q_fac = lax.rsqrt(sums[:, t:t + 1] / q_width + NORM_EPS)
        k_fac = lax.rsqrt(sums[:, steps + t:steps + t + 1] / kv_width + NORM_EPS)
        val = k_raw[t] * k_fac * gain_k
        val = val * cos_tab + pltpu.roll(val, hd // 2, axis=1) * sin_tab
        kn_out[t] = val.astype(BF16).astype(F32)
        for g in range(heads):
            val = q_raw[t * rows:(t + 1) * rows, g * hd:(g + 1) * hd] * q_fac * gain_q[g:g + 1, :]
            val = val * cos_tab + pltpu.roll(val, hd // 2, axis=1) * sin_tab
            q_rows[pl.ds(t * heads + g, rows, stride=pad), :] = val
    q_out[...] = q_rows[...].reshape(rows, pad, hd).astype(BF16)
    for copy in cache_in:
        copy.wait()


def run_qkv(tp, x_seq, cache_len, w_q, w_k, w_v, g_q, g_k, k_cache, v_cache):
    steps, rows, d_model = x_seq.shape
    hd = w_k.shape[1]
    width = w_q.shape[1]
    heads = width // hd
    pad = 16
    inv_freq = (ROPE_THETA ** (-(np.arange(hd // 2, dtype=np.float64) * (2.0 / hd)))).astype(np.float32)
    freq = jnp.asarray(np.concatenate([inv_freq, inv_freq])[None, :])
    return pl.pallas_call(
        functools.partial(qkv_kernel, tp, width * tp, hd * tp),
        out_shape=(pltpu.VMEM((rows, pad, hd), BF16),
                   pltpu.VMEM((steps, rows, hd), F32),
                   pltpu.VMEM((steps, rows, hd), F32),
                   pltpu.VMEM(k_cache.shape, BF16),
                   pltpu.VMEM(v_cache.shape, BF16)),
        in_specs=[ANY_SPEC] * 10,
        out_specs=(VMEM_SPEC,) * 5,
        scratch_shapes=[
            pltpu.VMEM((1, rows), jnp.int32),
            pltpu.VMEM((1, hd), F32),
            pltpu.VMEM((heads, hd), BF16),
            pltpu.VMEM((1, hd), BF16),
            pltpu.SemaphoreType.DMA((4,)),
            pltpu.SemaphoreType.DMA((2, CACHE_PARTS)),
            pltpu.VMEM((steps * rows, d_model), BF16),
            pltpu.VMEM((d_model, width), BF16),
            pltpu.VMEM((d_model, hd), BF16),
            pltpu.VMEM((d_model, hd), BF16),
            pltpu.VMEM((steps * rows, width), F32),
            pltpu.VMEM((steps, rows, hd), F32),
            pltpu.VMEM((rows * pad, hd), F32),
            pltpu.VMEM((8, rows), F32),
            pltpu.VMEM((tp - 1, 8, rows), F32),
            pltpu.VMEM((rows, rows), F32),
            pltpu.SemaphoreType.DMA((7,)),
            pltpu.SemaphoreType.DMA((tp - 1,)),
            pltpu.SemaphoreType.DMA((tp - 1,)),
        ],
        compiler_params=pltpu.CompilerParams(collective_id=0, has_side_effects=True, vmem_limit_bytes=QKV_VMEM),
        name="qkv",
    )(*[in_hbm(val) for val in (x_seq, cache_len.reshape(1, rows), freq, w_q, w_k, w_v, g_q.reshape(heads, hd), g_k.reshape(1, hd), k_cache, v_cache)])


SEQ_BLOCK = 8
PATCH_ROWS = 32


def attention_kernel(steps, heads, len_ref, q_ref, kn_ref, vn_ref, k_in, v_in, wo_hbm, k_out, v_out, part,
                     k_buf, v_buf, o_ref, wo, mixed, wo_sem, out_sem):
    rows, seq_max, hd = k_buf.shape
    pad = q_ref.shape[1]
    blocks = rows // SEQ_BLOCK
    d_model = wo.shape[1]
    wo_in = pltpu.make_async_copy(wo_hbm, wo, wo_sem)
    wo_in.start()

    def moves(blk):
        sl = pl.ds(blk * SEQ_BLOCK, SEQ_BLOCK)
        return (pltpu.make_async_copy(k_buf.at[sl], k_out.at[sl], out_sem.at[0, blk]),
                pltpu.make_async_copy(v_buf.at[sl], v_out.at[sl], out_sem.at[1, blk]))

    scale = hd ** -0.5
    win_row = lax.broadcasted_iota(jnp.int32, (PATCH_ROWS, hd), 0)
    key_col = lax.broadcasted_iota(jnp.int32, (pad, seq_max), 1)
    step_row = lax.broadcasted_iota(jnp.int32, (pad, seq_max), 0) // heads
    key_off = key_col - step_row

    def body(blk, carry):
        block = pl.ds(blk * SEQ_BLOCK, SEQ_BLOCK)
        k_buf[block] = k_in[block]
        v_buf[block] = v_in[block]
        lens = []
        for i in range(SEQ_BLOCK):
            b = blk * SEQ_BLOCK + i
            length = len_ref[b]
            base = pl.multiple_of(jnp.minimum((length // 16) * 16, seq_max - PATCH_ROWS), 16)
            for buf, new_ref in ((k_buf, kn_ref), (v_buf, vn_ref)):
                win = buf[b, pl.ds(base, PATCH_ROWS), :].astype(F32)
                for t in range(steps):
                    win = jnp.where(win_row == length + t - base, new_ref[t, pl.ds(b, 1), :], win)
                buf[b, pl.ds(base, PATCH_ROWS), :] = win.astype(BF16)
            lens.append(length)
        scores = []
        for i in range(SEQ_BLOCK):
            b = blk * SEQ_BLOCK + i
            s = lax.dot_general(q_ref[b], k_buf[b], (((1,), (1,)), ((), ())), preferred_element_type=F32) * scale
            scores.append(jnp.where(key_off <= lens[i], s, -jnp.inf))
        exps = []
        for i in range(SEQ_BLOCK):
            e = jnp.exp(scores[i] - jnp.max(scores[i], axis=1, keepdims=True))
            exps.append((e.astype(BF16), jnp.sum(e, axis=1, keepdims=True)))
        for i in range(SEQ_BLOCK):
            b = blk * SEQ_BLOCK + i
            out = matmul(exps[i][0], v_buf[b]) / exps[i][1]
            mixed[pl.ds(pl.multiple_of(b * pad, pad), pad), :] = out
        for copy in moves(blk):
            copy.start()
        return carry

    lax.fori_loop(0, blocks, body, 0)
    for t in range(steps):
        for g in range(heads):
            o_ref[t * rows:(t + 1) * rows, g * hd:(g + 1) * hd] = mixed[pl.ds(t * heads + g, rows, stride=pad), :].astype(BF16)

    wo_in.wait()
    for n in range(0, d_model, DOWN_TILE):
        val = matmul(o_ref[...], wo[:, n:n + DOWN_TILE]).astype(BF16)
        part[:, :, :, :, n:n + DOWN_TILE] = val.reshape(part.shape[:4] + (DOWN_TILE,))

    def finish(blk, carry):
        for copy in moves(blk):
            copy.wait()
        return carry

    lax.fori_loop(0, blocks, finish, 0)


def run_attention(tp, heads, cache_len, q_rows, k_new, v_new, k_cache, v_cache, w_o):
    rows, seq_max, hd = k_cache.shape
    steps = k_new.shape[0]
    pad = q_rows.shape[1]
    flat = jax.ShapeDtypeStruct(k_cache.shape, BF16)
    part = pltpu.VMEM((steps, tp // 2, 2, rows // tp, w_o.shape[1]), BF16)
    k_out, v_out, part = pl.pallas_call(
        functools.partial(attention_kernel, steps, heads),
        out_shape=(flat, flat, part),
        in_specs=[SMEM_SPEC] + [VMEM_SPEC] * 5 + [ANY_SPEC],
        out_specs=(ANY_SPEC, ANY_SPEC, VMEM_SPEC),
        scratch_shapes=[
            pltpu.VMEM(k_cache.shape, BF16),
            pltpu.VMEM(v_cache.shape, BF16),
            pltpu.VMEM((steps * rows, heads * hd), BF16),
            pltpu.VMEM(w_o.shape, BF16),
            pltpu.VMEM((rows * pad, hd), F32),
            pltpu.SemaphoreType.DMA,
            pltpu.SemaphoreType.DMA((2, rows // SEQ_BLOCK)),
        ],
        compiler_params=pltpu.CompilerParams(vmem_limit_bytes=ATTENTION_VMEM),
        name="attention",
    )(cache_len, in_vmem(q_rows), in_vmem(k_new), in_vmem(v_new), in_vmem(k_cache), in_vmem(v_cache), in_hbm(w_o))
    return part, k_out, v_out


QUARTERS = 4
LEFT_PIECES = tuple(range(QUARTERS // 2))
RIGHT_PIECES = tuple(range(QUARTERS // 2, QUARTERS))
PIECED = ("pair", "relay", "near", "far", "own_r", "own_l", "pass")
WHOLE = ("own_s", "sib_r", "sib_l", "sib_fr", "sib_fl")
COPIES = tuple((kind, q) for kind in PIECED for q in range(QUARTERS)) + tuple((kind, 0) for kind in WHOLE)
GATE_TILE = 256
FETCHES = 8
DOWN_TILE = 512
TASKS = ("send", "pair", "relay", "norm", "pass", "sib", "sibf", "gather", "gate", "down", "fetch")
ORDER = (
    1105, 2, 3, 1, 22, 0, 1101, 102, 101, 11, 10, 1011, 13, 103, 100, 122, 1107, 111, 1007, 1003, 1106, 1004, 12, 113,
    21, 1012, 201, 202, 1006, 203, 200, 110, 23, 1015, 112, 20, 1008, 120, 211, 123, 1100, 213, 1010, 300, 1102, 1000, 121, 210,
    1104, 1005, 212, 1009, 402, 400, 1013, 403, 401, 1103, 220, 222, 1002, 500, 501, 1014, 221, 223, 310, 1001, 601, 600, 700, 800,
    801, 802, 410, 412, 413, 411, 803, 320, 804, 805, 510, 806, 900, 511, 901, 902, 903, 904, 610, 611, 905, 150, 906, 907,
    422, 423, 710, 151, 420, 421, 810, 152, 153, 811, 812, 520, 813, 814, 815, 251, 816, 250, 910, 911, 912, 521, 913, 253,
    621, 620, 914, 252, 160, 915, 916, 917, 720, 161, 820, 821, 162, 163, 822, 823, 350, 824, 825, 826, 920, 921, 922, 263,
    923, 260, 924, 170, 925, 926, 171, 927, 450, 172, 261, 173, 262, 452, 451, 270, 453, 271, 272, 273, 360, 370, 463, 650,
    651, 550, 460, 461, 462, 470, 472, 471, 561, 551, 473, 570, 750, 560, 571, 660, 661, 760, 670, 671, 770,
)


def mlp_kernel(chips, x_hbm, part_in, w1_hbm, w3_hbm, w2_hbm, ga_hbm, gm_hbm, hid, part,
               ga_ref, gm_ref, small_sem, w1, w3, w2, x_own, gains, pair_in, relay_in, near_in, act, w_sem, x_sem, send_sem, recv_sem):
    steps, rows, d_model = x_hbm.shape
    ff = w1_hbm.shape[1]
    piece = d_model // QUARTERS
    me = lax.axis_index("tp")
    chip, core = me // 2, lax.rem(me, 2)
    nxt, prv, opp = lax.rem(chip + 1, chips), lax.rem(chip + chips - 1, chips), lax.rem(chip + 2, chips)
    right, left, sib = nxt * 2 + core, prv * 2 + core, chip * 2 + 1 - core
    n_gate, n_down = ff // GATE_TILE, d_model // DOWN_TILE

    def fetches(hbm, buf, sem):
        depth = hbm.shape[0] // FETCHES
        blocks = [pl.ds(i * depth, depth) for i in range(FETCHES)]
        return [pltpu.make_async_copy(hbm.at[blocks[i]], buf.at[blocks[i]], w_sem.at[sem, i]) for i in range(FETCHES)]

    gate_in = [copy for pair in zip(fetches(w1_hbm, w1, 0), fetches(w3_hbm, w3, 1)) for copy in pair]
    down_in = fetches(w2_hbm, w2, 2)

    def slot(c, k):
        return pl.ds(pl.multiple_of((c * 2 + k) * SLOT_ROWS, SLOT_ROWS), SLOT_ROWS)

    x_in = [pltpu.make_async_copy(x_hbm.at[t, slot(chip, core), :], x_own.at[t], x_sem.at[t]) for t in range(steps)]
    small_in = [pltpu.make_async_copy(src, dst, small_sem.at[i]) for i, (src, dst) in enumerate(
        ((ga_hbm, ga_ref), (gm_hbm, gm_ref)))]
    for copy in small_in + x_in:
        copy.start()
    barrier = pltpu.get_barrier_semaphore()
    for other in (right, left, sib):
        pl.semaphore_signal(barrier, inc=1, device_id={"tp": other}, device_id_type=MESH)
    for copy in small_in:
        copy.wait()
    for i, ref in enumerate((ga_ref, gm_ref)):
        vals = ref[...].astype(F32)
        for j in range(vals.shape[0]):
            gains[i, :, j * vals.shape[1]:(j + 1) * vals.shape[1]] = vals[j:j + 1, :]
    pl.semaphore_wait(barrier, 3)

    def quarter(q, count=1):
        return pl.ds(q * piece, count * piece)

    def endpoints(t, kind, q):
        own, other = part.at[t, :, core], part.at[t, :, 1 - core]
        to_right = q in LEFT_PIECES
        c = quarter(q)
        if kind == "pair":
            return other.at[:, :, c], pair_in.at[t, :, :, c], sib
        if kind == "relay":
            return own.at[opp, :, c], relay_in.at[t, :, c], right if to_right else left
        if kind == "near":
            if to_right:
                return own.at[prv, :, c], near_in.at[t, 1, :, c], left
            return own.at[nxt, :, c], near_in.at[t, 0, :, c], right
        if kind == "far":
            if to_right:
                return own.at[nxt, :, c], near_in.at[t, 0, :, c], right
            return own.at[prv, :, c], near_in.at[t, 1, :, c], left
        if kind == "own_r":
            block, device = hid.at[t, slot(chip, core), c], right
        elif kind == "own_l":
            block, device = hid.at[t, slot(chip, core), c], left
        elif kind == "pass":
            block, device = (hid.at[t, slot(prv, core), c], right) if to_right else (hid.at[t, slot(nxt, core), c], left)
        elif kind == "own_s":
            block, device = hid.at[t, slot(chip, core), :], sib
        elif kind == "sib_r":
            block, device = hid.at[t, slot(prv, core), :], sib
        elif kind == "sib_l":
            block, device = hid.at[t, slot(nxt, core), :], sib
        elif kind == "sib_fr":
            block, device = hid.at[t, slot(opp, core), quarter(0, QUARTERS // 2)], sib
        else:
            block, device = hid.at[t, slot(opp, core), quarter(QUARTERS // 2, QUARTERS // 2)], sib
        return block, block, device

    def copy(ph, t, kind, q=0):
        src, dst, device = endpoints(t, kind, q)
        j = COPIES.index((kind, q))
        return pltpu.make_async_remote_copy(
            src_ref=src, dst_ref=dst, send_sem=send_sem.at[ph, t, j], recv_sem=recv_sem.at[ph, t, j],
            device_id={"tp": device}, device_id_type=MESH)

    def sent(ph, t):
        for kind, q in COPIES:
            copy(ph, t, kind, q).wait_send()

    def pair_send(ph, t, q):
        copy(0, t, "pair", q).start()

    def pair_add(ph, t, q):
        copy(ph, t, "pair", q).wait_recv()
        c = slice(q * piece, (q + 1) * piece)
        for n in (opp, prv, nxt, chip):
            part[t, n, core, :, c] = (part[t, n, core, :, c].astype(F32) + pair_in[t, n, :, c].astype(F32)).astype(BF16)
        copy(ph, t, "relay", q).start()
        copy(ph, t, "near", q).start()

    def relay_add(ph, t, q):
        copy(ph, t, "relay", q).wait_recv()
        c = slice(q * piece, (q + 1) * piece)
        n = nxt if q in LEFT_PIECES else prv
        part[t, n, core, :, c] = (part[t, n, core, :, c].astype(F32) + relay_in[t, :, c].astype(F32)).astype(BF16)
        copy(ph, t, "far", q).start()

    def norm(ph, t, _):
        for q in range(QUARTERS):
            copy(ph, t, "near", q).wait_recv()
            copy(ph, t, "far", q).wait_recv()
        total = part[t, chip, core].astype(F32) + near_in[t, 0].astype(F32) + near_in[t, 1].astype(F32)
        total = total.astype(BF16).astype(F32)
        fac = lax.rsqrt(jnp.sum(total * total, axis=1, keepdims=True) / d_model + NORM_EPS)
        if ph == 0:
            x_in[t].wait()
            base = x_own[t]
        else:
            base = hid[t, slot(chip, core), :]
        hid[t, slot(chip, core), :] = (base.astype(F32) + total * fac * gains[ph]).astype(BF16)
        for first, second in ((LEFT_PIECES, RIGHT_PIECES), (RIGHT_PIECES, LEFT_PIECES)):
            for i, j in zip(first, second):
                copy(ph, t, "own_r", i).start()
                copy(ph, t, "own_l", j).start()
        copy(ph, t, "own_s").start()

    def pass_on(ph, t, q):
        copy(ph, t, "own_r" if q in LEFT_PIECES else "own_l", q).wait_recv()
        copy(ph, t, "pass", q).start()

    def pass_sib(ph, t, side):
        for q in (RIGHT_PIECES, LEFT_PIECES)[side]:
            copy(ph, t, ("own_r", "own_l")[side], q).wait_recv()
        copy(ph, t, ("sib_r", "sib_l")[side]).start()

    def far_sib(ph, t, side):
        for q in (LEFT_PIECES, RIGHT_PIECES)[side]:
            copy(ph, t, "pass", q).wait_recv()
        copy(ph, t, ("sib_fr", "sib_fl")[side]).start()

    def gather(ph, t, _):
        for kind in WHOLE:
            copy(ph, t, kind).wait_recv()

    def gate_up(ph, t, j):
        if t == 0 and j == 0:
            for fetch in gate_in:
                fetch.wait()
        sl = slice(j * GATE_TILE, (j + 1) * GATE_TILE)
        gate = matmul(hid[t], w1[:, sl])
        up = matmul(hid[t], w3[:, sl])
        act[:, sl] = (gate / (1.0 + jnp.exp(-gate)) * up).astype(BF16)

    def down(ph, t, j):
        if j == 0:
            sent(0, t)
        if t == 0 and j == 0:
            for fetch in down_in:
                fetch.wait()
        sl = slice(j * DOWN_TILE, (j + 1) * DOWN_TILE)
        val = matmul(act[...], w2[:, sl]).astype(BF16)
        part[t, :, :, :, sl] = val.reshape(chips, 2, SLOT_ROWS, DOWN_TILE)
        if (j + 1) * DOWN_TILE % piece == 0:
            copy(1, t, "pair", (j + 1) * DOWN_TILE // piece - 1).start()

    run = (pair_send, pair_add, relay_add, norm, pass_on, pass_sib, far_sib, gather, gate_up, down)
    for code in ORDER:
        if code >= 1000:
            (gate_in, down_in)[code // 100 % 10][code % 100].start()
        else:
            run[code // 100](code // 50 % 2, code % 50 // 10, code % 10)
    for t in range(steps):
        sent(1, t)


def run_mlp(tp, x_seq, part, w_gate, w_up, w_down, g_attn, g_mlp):
    steps, rows, d_model = x_seq.shape
    ff = w_gate.shape[1]
    chips = tp // 2
    hid, _ = pl.pallas_call(
        functools.partial(mlp_kernel, chips),
        out_shape=(pltpu.VMEM((steps, rows, d_model), BF16), pltpu.VMEM(part.shape, BF16)),
        in_specs=[ANY_SPEC, VMEM_SPEC] + [ANY_SPEC] * 5,
        out_specs=(VMEM_SPEC, VMEM_SPEC),
        input_output_aliases={1: 1},
        scratch_shapes=[
            pltpu.VMEM((d_model // 128, 128), BF16),
            pltpu.VMEM((d_model // 128, 128), BF16),
            pltpu.SemaphoreType.DMA((2,)),
            pltpu.VMEM(w_gate.shape, BF16),
            pltpu.VMEM(w_up.shape, BF16),
            pltpu.VMEM(w_down.shape, BF16),
            pltpu.VMEM((steps, SLOT_ROWS, d_model), BF16),
            pltpu.VMEM((2, 1, d_model), F32),
            pltpu.VMEM((steps, chips, SLOT_ROWS, d_model), BF16),
            pltpu.VMEM((steps, SLOT_ROWS, d_model), BF16),
            pltpu.VMEM((steps, 2, SLOT_ROWS, d_model), BF16),
            pltpu.VMEM((rows, ff), BF16),
            pltpu.SemaphoreType.DMA((3, FETCHES)),
            pltpu.SemaphoreType.DMA((steps,)),
            pltpu.SemaphoreType.DMA((2, steps, len(COPIES))),
            pltpu.SemaphoreType.DMA((2, steps, len(COPIES))),
        ],
        compiler_params=pltpu.CompilerParams(collective_id=1, has_side_effects=True, vmem_limit_bytes=MLP_VMEM),
        name="mlp",
    )(in_hbm(x_seq), in_vmem(part), in_hbm(w_gate), in_hbm(w_up), in_hbm(w_down), g_attn.reshape(-1, 128), g_mlp.reshape(-1, 128))
    return hid


def store_kernel(src, dst, sem):
    steps = src.shape[0]
    copies = [pltpu.make_async_copy(src.at[t], dst.at[t], sem.at[t]) for t in range(steps)]
    for copy in copies:
        copy.start()
    for copy in copies:
        copy.wait()


def run_store(y_seq):
    return pl.pallas_call(
        store_kernel,
        out_shape=jax.ShapeDtypeStruct(y_seq.shape, BF16),
        in_specs=[VMEM_SPEC],
        out_specs=ANY_SPEC,
        scratch_shapes=[pltpu.SemaphoreType.DMA((y_seq.shape[0],))],
        compiler_params=pltpu.CompilerParams(vmem_limit_bytes=16 * 1024 * 1024),
        name="store",
    )(in_vmem(y_seq))


def solution(mesh):
    tp = mesh.shape['tp']

    def local_run(x_seq, cache_len, k_cache, v_cache, w_q, w_k, w_v, w_o, w_gate, w_up, w_down, g_q, g_k, g_attn, g_mlp):
        heads = w_q.shape[1] // w_k.shape[1]
        flat = (k_cache.shape[0],) + k_cache.shape[2:]
        q_rows, k_new, v_new, k_old, v_old = run_qkv(tp, x_seq, cache_len, w_q, w_k, w_v, g_q, g_k, k_cache.reshape(flat), v_cache.reshape(flat))
        part, k_out, v_out = run_attention(tp, heads, cache_len, q_rows, k_new, v_new, k_old, v_old, w_o)
        y_seq = run_mlp(tp, x_seq, part, w_gate, w_up, w_down, g_attn, g_mlp)
        return run_store(y_seq), k_out.reshape(k_cache.shape), v_out.reshape(v_cache.shape)

    data_spec = P(None, 'dp', None)
    cache_spec = P('dp', 'tp', None, None)
    col_spec = P(None, 'tp')
    row_spec = P('tp', None)
    arg_specs = (data_spec, P('dp'), cache_spec, cache_spec, col_spec, col_spec, col_spec, row_spec, col_spec, col_spec, row_spec, P('tp'), P('tp'), P(None), P(None))
    out_specs = (data_spec, cache_spec, cache_spec)
    return jax.shard_map(local_run, mesh=mesh, in_specs=arg_specs, out_specs=out_specs, check_vma=False)
```
